128 devices in a mesh: head: 8 (over z_lo, x), blk: 16 (over z_hi, y, core).
Axes of the slice: x: 4, y: 4, z: 4 (z_hi: 2, z_lo: 2; z = z_hi * 2 + z_lo), core: 2. Of those that a mesh axis runs over, the one named last changes fastest.
Arguments:
- hidden_in: bfloat16 [8192, 4096], P(('blk', 'head')), may hold values from -6 to 6
- queries: bfloat16 [8192, 2048], P(('blk', 'head')), may hold values from -26 to 26
- key_states: bfloat16 [8192, 1024], P(('blk', 'head')), may hold values from -5 to 5
- value_states: bfloat16 [8192, 1024], P(('blk', 'head')), may hold values from -6 to 6
- out_weight: bfloat16 [2048, 4096], P('head'), may hold values from -0.125 to 0.125
- norm_gain: float32 [4096], replicated, may hold values from 0.1 to 1.9
- gate_weight: bfloat16 [4096, 7168], P(None, 'head'), may hold values from -0.09375 to 0.09375
- up_weight: bfloat16 [4096, 7168], P(None, 'head'), may hold values from -0.09375 to 0.09375
- down_weight: bfloat16 [7168, 4096], P('head'), may hold values from -0.0625 to 0.0625
Outputs:
- layer_out: bfloat16 [8192, 4096], P(('blk', 'head'))
The draws below stay inside these ranges and needn't reach their ends.
All inputs are finite; a program needn't handle non-finite values.
Results may differ from the reference program's by a relative error of at most 0.018.
Values may be sent and summed in bfloat16 or wider, within the bound.
A program may use at most 192 MiB of HBM per device.

```python
import jax
import jax.numpy as jnp
from jax import lax

D = 4096
HEADS = 16
KV_HEADS = 8
HEAD_DIM = 128
FF = 7168
TOK_BLK = 512
SEQ = 8192


def paired_draw(seed_key):
    anchor = jax.random.fold_in(seed_key, 7)
    stream_keys = jax.random.fold_in(anchor, 1)
    stream_query = jax.random.fold_in(anchor, 2)
    key_width = KV_HEADS * HEAD_DIM
    query_width = HEADS * HEAD_DIM
    key_drawn = jnp.clip(jax.random.normal(stream_keys, (SEQ, key_width), jnp.float32), -5.0, 5.0)
    query_drawn = jnp.clip(2.5 * jax.random.normal(stream_query, (SEQ, query_width), jnp.float32), -15.0, 15.0)
    return (query_drawn, key_drawn)


def draw_queries(key, part):
    return paired_draw(key)[0].astype(jnp.bfloat16)


def draw_key_states(key, part):
    return paired_draw(key)[1].astype(jnp.bfloat16)


def levels(rng, extent, pieces, least, top_value):
    loudness = 1.0
    for axis_at, blocks in pieces:
        heights = jax.random.uniform(jax.random.fold_in(jax.random.fold_in(rng, 6), axis_at), (blocks,), jnp.float32, least / len(pieces), top_value / len(pieces))
        loudness = loudness * jnp.repeat(jnp.exp(heights), extent[axis_at] // blocks).reshape((-1,) + (1,) * (len(extent) - 1 - axis_at))
    return loudness


def normal_values(key, extent, width, reach, pieces=(), held_as=jnp.bfloat16):
    drawn = jax.random.normal(key, extent, jnp.float32) * width
    if len(pieces) > 0:
        drawn = levels(key, extent, pieces, -0.22, 0.18) * drawn
    return jnp.clip(drawn, min=-reach, max=reach).astype(held_as)


def setup_inputs(seed: int = 0) -> dict:
    splits = jax.random.split(jax.random.key(seed), 10)
    return {
        "hidden_in": normal_values(splits[0], (SEQ, D), 1.0, 6.0, ((0, 128),)),
        "queries": draw_queries(jax.random.fold_in(splits[9], 71), 0),
        "key_states": draw_key_states(jax.random.fold_in(splits[9], 71), 0),
        "value_states": normal_values(splits[3], (SEQ, KV_HEADS * HEAD_DIM), 1.0, 6.0, ((0, 128),)),
        "out_weight": normal_values(splits[4], (HEADS * HEAD_DIM, D), (HEADS * HEAD_DIM) ** -0.5, 0.125, ((0, 8),)),
        "norm_gain": jnp.clip(1.0 + 0.18 * jax.random.normal(splits[5], (D,), jnp.float32), 0.1, 1.9),
        "gate_weight": normal_values(splits[6], (D, FF), D ** -0.5, 0.09375, ((1, 8),)),
        "up_weight": normal_values(splits[7], (D, FF), D ** -0.5, 0.09375, ((1, 8),)),
        "down_weight": normal_values(splits[8], (FF, D), FF ** -0.5, 0.0625, ((0, 8),)),
    }


def attend_group(query_group, key_group, value_group):
    score_scale = HEAD_DIM ** (-0.5)
    positions = jnp.arange(SEQ, dtype=jnp.int32)

    def one_block(block_index):
        first_row = block_index * TOK_BLK
        query_block = lax.dynamic_slice_in_dim(query_group, first_row, TOK_BLK, 1)
        scores = jnp.einsum('rqd,kd->rqk', query_block, key_group) * score_scale
        query_pos = first_row + jnp.arange(TOK_BLK, dtype=jnp.int32)
        visible = positions[None, :] <= query_pos[:, None]
        row_peak = lax.optimization_barrier(jnp.max(jnp.where(visible, scores, -jnp.inf), axis=-1))
        exp_scores = jnp.where(visible, jnp.exp(scores - row_peak[..., None]), 0.0)
        row_total = lax.optimization_barrier(jnp.sum(exp_scores, axis=-1))
        rounded = lax.optimization_barrier(exp_scores.astype(jnp.bfloat16)).astype(jnp.float32)
        numerator = jnp.einsum('rqk,kd->rqd', rounded, value_group)
        return (numerator / row_total[..., None]).astype(jnp.bfloat16)
    return lax.map(one_block, jnp.arange(SEQ // TOK_BLK, dtype=jnp.int32))

def attend_tuple(groups):
    return attend_group(groups[0], groups[1], groups[2])

def reference(hidden_in, queries, key_states, value_states, out_weight, norm_gain, gate_weight, up_weight, down_weight):
    group_ratio = HEADS // KV_HEADS
    query_all = queries.astype(jnp.float32).reshape(SEQ, KV_HEADS, group_ratio, HEAD_DIM).transpose(1, 2, 0, 3)
    key_all = key_states.astype(jnp.float32).reshape(SEQ, KV_HEADS, HEAD_DIM).transpose(1, 0, 2)
    value_all = value_states.astype(jnp.float32).reshape(SEQ, KV_HEADS, HEAD_DIM).transpose(1, 0, 2)
    attended = lax.map(attend_tuple, (query_all, key_all, value_all))
    attended = attended.transpose(1, 3, 0, 2, 4).reshape(SEQ, HEADS * HEAD_DIM)
    projected = jnp.dot(attended, out_weight, preferred_element_type=jnp.float32)
    residual = (hidden_in.astype(jnp.float32) + projected).astype(jnp.bfloat16)
    widened = residual.astype(jnp.float32)
    mean_square = lax.optimization_barrier(jnp.mean(widened * widened, axis=-1, keepdims=True))
    normed = (widened * lax.rsqrt(mean_square + 1e-05) * norm_gain.astype(jnp.float32)).astype(jnp.bfloat16)
    gate_part = jnp.dot(normed, gate_weight, preferred_element_type=jnp.float32)
    up_part = jnp.dot(normed, up_weight, preferred_element_type=jnp.float32)
    inner_act = (jax.nn.silu(gate_part) * up_part).astype(jnp.bfloat16)
    mlp_out = jnp.dot(inner_act, down_weight, preferred_element_type=jnp.float32)
    return (residual.astype(jnp.float32) + mlp_out).astype(jnp.bfloat16)
```

```python
import jax
import jax.numpy as jnp
from jax import lax
from jax.experimental import pallas as pl
from jax.experimental.pallas import tpu as pltpu
from jax.sharding import PartitionSpec as P

HEADS = 16
KV_HEADS = 8
HEAD_DIM = 128
MESH = pl.DeviceIdType.MESH
F32 = jnp.float32
BF16 = jnp.bfloat16

negative_fill = -1e30


class Place:
    def __init__(self):
        self.head = lax.axis_index("head")
        self.blk = lax.axis_index("blk")
        self.x = lax.rem(self.head, 4)
        self.zl = self.head // 4
        self.zh = self.blk // 8
        self.yc = lax.rem(self.blk, 8)
        self.z = self.zh * 2 + self.zl
        self.xs = [lax.rem(self.x + k, 4) for k in range(4)]
        self.right = self.at_x(self.xs[1])
        self.left = self.at_x(self.xs[3])
        self.above = self.at_z(1)
        self.below = self.at_z(3)

    def at_x(self, x):
        return (self.zl * 4 + x, self.blk)

    def at_z(self, step):
        z = lax.rem(self.z + step, 4)
        return (lax.rem(z, 2) * 4 + self.x, (z // 2) * 8 + self.yc)

    def here(self, k):
        return self.zl * 4 + self.xs[k]

    def other(self, k):
        return (1 - self.zl) * 4 + self.xs[k]


def remote(src, dst, send_sem, recv_sem, device):
    return pltpu.make_async_remote_copy(
        src_ref=src, dst_ref=dst, send_sem=send_sem, recv_sem=recv_sem,
        device_id=device, device_id_type=MESH,
    )


def gather_rows(p, buf, send_sem, recv, steps, compute):
    def send(h, s, half, to_half, kind, device):
        remote(buf.at[h, s, half], buf.at[h, s, to_half], send_sem, recv.at[kind, s], device).start()

    def wait(h, s, half, kind):
        remote(buf.at[h, s, half], buf.at[h, s, half], send_sem, recv.at[kind, s], p.right).wait_recv()

    me, left, right, far = p.here(0), p.here(3), p.here(1), p.here(2)
    for s in range(steps):
        send(me, s, 0, 0, 0, p.right)
        send(me, s, 1, 1, 4, p.left)
        send(me, s, 0, 1, 6, p.above)
        send(me, s, 1, 0, 10, p.below)
    for s in range(steps):
        send(me, s, 1, 1, 1, p.right)
        send(me, s, 0, 0, 3, p.left)
    compute(me, True)
    for s in range(steps):
        wait(left, s, 0, 0)
        send(left, s, 0, 0, 2, p.right)
        send(left, s, 0, 1, 7, p.above)
        wait(right, s, 1, 4)
        send(right, s, 1, 1, 5, p.left)
        send(right, s, 1, 0, 12, p.below)
    for s in range(steps):
        wait(p.other(0), s, 1, 6)
        wait(p.other(0), s, 0, 10)
    compute(p.other(0), False)
    for s in range(steps):
        wait(left, s, 1, 1)
        send(left, s, 1, 0, 11, p.below)
        wait(right, s, 0, 3)
        send(right, s, 0, 1, 8, p.above)
    compute(left, False)
    compute(right, False)
    for s in range(steps):
        wait(far, s, 0, 2)
        send(far, s, 0, 1, 9, p.above)
        wait(far, s, 1, 5)
        send(far, s, 1, 0, 13, p.below)
    compute(far, False)
    for k, up, down in ((3, 7, 11), (1, 8, 12), (2, 9, 13)):
        for s in range(steps):
            wait(p.other(k), s, 1, up)
            wait(p.other(k), s, 0, down)
        compute(p.other(k), False)
    pltpu.make_async_copy(buf.at[0:7], buf.at[0:7], send_sem).wait()


NS1 = 2
NS2 = 4
NC = 8
CW = 512
FFL = 896


def block_kernel(
    att, hid, gain, wo_hbm, gate_hbm, up_hbm, down_hbm, out,
    abuf, rbuf, wo, wgu, wd, oacc, acc, xg, sq, inner,
    zs, zr, keep, m1s, m1r, m2s, m2r,
    wsem, s1, r1, s2, r2, s3, zsem, m1sem, m2sem,
):
    p = Place()
    barrier = pltpu.get_barrier_semaphore()
    for device in (p.right, p.left, p.above, p.below):
        pl.semaphore_signal(barrier, inc=1, device_id=device, device_id_type=MESH)

    order = [p.here(0), p.other(0), p.here(3), p.here(1), p.here(2), p.other(3), p.other(1), p.other(2)]
    wo_copy = pltpu.make_async_copy(wo_hbm, wo, wsem.at[16])
    wd_copy = pltpu.make_async_copy(down_hbm, wd, wsem.at[17])

    def gate_copy(h):
        rows = pl.ds(pl.multiple_of(h * 512, 512), 512)
        return pltpu.make_async_copy(gate_hbm.at[rows], wgu.at[rows, 0:FFL], wsem.at[h])

    def up_copy(h):
        rows = pl.ds(pl.multiple_of(h * 512, 512), 512)
        return pltpu.make_async_copy(up_hbm.at[rows], wgu.at[rows, FFL : 2 * FFL], wsem.at[8 + h])

    wo_copy.start()
    for h in order:
        gate_copy(h).start()
        up_copy(h).start()
    wd_copy.start()

    me = p.here(0)
    c1 = 256 // NS1
    for s in range(NS1):
        for half in range(2):
            abuf[me, s, half] = att[half * 256 : (half + 1) * 256, s * c1 : (s + 1) * c1]
    pl.semaphore_wait(barrier, 4)

    def project(h, first):
        if first:
            wo_copy.wait()
        a = jnp.concatenate([abuf[h, s].reshape(512, c1) for s in range(NS1)], axis=1)
        rows = pl.ds(pl.multiple_of(h * 256, 256), 256)
        for n in range(2):
            cols = slice(n * 256, (n + 1) * 256)
            part = jnp.dot(a, wo[rows, cols], preferred_element_type=F32)
            if first:
                oacc[:, cols] = hid[:, cols].astype(F32) + part
            else:
                oacc[:, cols] += part

    gather_rows(p, abuf, s1, r1, NS1, project)

    c2 = 512 // NS2
    for s in range(NS2):
        for half in range(2):
            rbuf[me, s, half] = oacc[half * 256 : (half + 1) * 256, s * c2 : (s + 1) * c2].astype(BF16)

    def expand(h, first):
        gate_copy(h).wait()
        up_copy(h).wait()
        total = None
        for s in range(NS2):
            r = rbuf[h, s].reshape(512, c2).astype(F32)
            g = gain[pl.ds(h * NS2 + s, 1), :]
            xg[:, s * c2 : (s + 1) * c2] = (r * g).astype(BF16)
            total = r * r if total is None else total + r * r
        if first:
            sq[...] = total
        else:
            sq[...] += total
        rows = pl.ds(pl.multiple_of(h * 512, 512), 512)

        def tile(n, _):
            cols = pl.ds(pl.multiple_of(n * 256, 256), 256)
            part = jnp.dot(xg[...], wgu[rows, cols], preferred_element_type=F32)
            if first:
                acc[:, cols] = part
            else:
                acc[:, cols] += part
            return 0

        lax.fori_loop(0, 7, tile, 0)

    gather_rows(p, rbuf, s2, r2, NS2, expand)

    scale = lax.rsqrt(jnp.sum(sq[...], axis=1, keepdims=True) * (1.0 / 4096.0) + 1e-5)
    sq[...] = jnp.broadcast_to(scale, (512, 128))

    def activate(j, _):
        at = pl.multiple_of(j * 128, 128)
        u = acc[:, pl.ds(at, 128)] * sq[...]
        v = acc[:, pl.ds(pl.multiple_of(at + FFL, 128), 128)] * sq[...]
        inner[:, pl.ds(at, 128)] = (u / (1.0 + jnp.exp(-u)) * v).astype(BF16)
        return 0

    lax.fori_loop(0, 7, activate, 0)

    def z_copy(c, side):
        device = p.above if side == 0 else p.below
        return remote(zs.at[c, side], zr.at[c, 1 - side], s3, zsem.at[1 - side, c], device)

    def z_wait(c, side):
        remote(zr.at[c, side], zr.at[c, side], s3, zsem.at[side, c], p.right).wait_recv()

    def reduce_down(c, _):
        for n in range(2):
            at = slice(n * 256, (n + 1) * 256)
            cols = pl.ds(pl.multiple_of(c * CW + n * 256, 256), 256)
            part = jnp.dot(inner[...], wd[:, cols], preferred_element_type=F32)
            keep[c, 0, :, at] = part[0:128]
            zs[c, 0, :, at] = part[128:256].astype(BF16)
            zs[c, 1, :, at] = part[256:384].astype(BF16)
            keep[c, 1, :, at] = part[384:512]
        z_copy(c, 0).start()
        z_copy(c, 1).start()
        return 0

    wd_copy.wait()
    lax.fori_loop(0, NC, reduce_down, 0)

    def slot(k):
        return pl.ds(pl.multiple_of(p.xs[k] * 32, 32), 32)

    def m1_copy(c, side):
        device = p.right if side == 0 else p.left
        return remote(m1s.at[c, side], m1r.at[c, side], s3, m1sem.at[side, c], device)

    def m2_copy(c, side):
        device = p.right if side == 0 else p.left
        return remote(m2s.at[c, side], m2r.at[c, side], s3, m2sem.at[side, c], device)

    def finish(t, _):
        @pl.when(t < NC)
        def _():
            c = t
            for side in range(2):
                z_wait(c, side)
                keep[c, side] += zr[c, side].astype(F32)
                m1s[c, side] = keep[c, side, slot(2), :].astype(BF16)
                m1_copy(c, side).start()

        @pl.when((t >= 1) & (t < NC + 1))
        def _():
            c = t - 1
            for side in range(2):
                m1_copy(c, side).wait_recv()
                k = 1 if side == 0 else 3
                for part in range(2):
                    q = keep[c, part, slot(k), :]
                    if part == side:
                        q = q + m1r[c, side].astype(F32)
                    m2s[c, side, part] = q.astype(BF16)
                m2_copy(c, side).start()

        @pl.when(t >= 2)
        def _():
            c = t - 2
            for side in range(2):
                m2_copy(c, side).wait_recv()
            for part in range(2):
                q = keep[c, part, slot(0), :] + m2r[c, 0, part].astype(F32) + m2r[c, 1, part].astype(F32)
                rows = pl.ds(pl.multiple_of(part * 128 + p.x * 32, 32), 32)
                for s in range(NS2):
                    r = rbuf[c, s, part, rows, :].astype(F32)
                    cols = pl.ds(pl.multiple_of(c * CW + s * c2, c2), c2)
                    out[part * 32 : (part + 1) * 32, cols] = (r + q[:, s * c2 : (s + 1) * c2]).astype(BF16)

        return 0

    lax.fori_loop(0, NC + 2, finish, 0)
    pltpu.make_async_copy(zs, zs, s3).wait()
    pltpu.make_async_copy(m1s, m1s, s3).wait()
    pltpu.make_async_copy(m2s, m2s, s3).wait()


def feed_forward(att, hid, wo, gain, gate, up, down):
    vmem = pl.BlockSpec(memory_space=pltpu.VMEM)
    hbm = pl.BlockSpec(memory_space=pl.ANY)
    dma = pltpu.SemaphoreType.DMA
    return pl.pallas_call(
        block_kernel,
        out_shape=jax.ShapeDtypeStruct((64, 4096), BF16),
        in_specs=[vmem, vmem, vmem, hbm, hbm, hbm, hbm],
        out_specs=vmem,
        scratch_shapes=[
            pltpu.VMEM((8, NS1, 2, 256, 256 // NS1), BF16),
            pltpu.VMEM((8, NS2, 2, 256, 512 // NS2), BF16),
            pltpu.VMEM((2048, 512), BF16),
            pltpu.VMEM((4096, 2 * FFL), BF16),
            pltpu.VMEM((FFL, 4096), BF16),
            pltpu.VMEM((512, 512), F32),
            pltpu.VMEM((512, 2 * FFL), F32),
            pltpu.VMEM((512, 512), BF16),
            pltpu.VMEM((512, 128), F32),
            pltpu.VMEM((512, FFL), BF16),
            pltpu.VMEM((NC, 2, 128, CW), BF16),
            pltpu.VMEM((NC, 2, 128, CW), BF16),
            pltpu.VMEM((NC, 2, 128, CW), F32),
            pltpu.VMEM((NC, 2, 32, CW), BF16),
            pltpu.VMEM((NC, 2, 32, CW), BF16),
            pltpu.VMEM((NC, 2, 2, 32, CW), BF16),
            pltpu.VMEM((NC, 2, 2, 32, CW), BF16),
            dma((18,)),
            dma,
            dma((14, NS1)),
            dma,
            dma((14, NS2)),
            dma,
            dma((2, NC)),
            dma((2, NC)),
            dma((2, NC)),
        ],
        compiler_params=pltpu.CompilerParams(
            collective_id=1, has_side_effects=True, vmem_limit_bytes=62 * 1024 * 1024
        ),
        cost_estimate=pl.CostEstimate(flops=12_500_000_000, bytes_accessed=24_000_000, transcendentals=0),
        name="feed_forward",
    )(att, hid, gain, wo, gate, up, down)


def sent_together(arrays, axis, dim, along):
    ends, at = ([], 0)
    for a in arrays[:-1]:
        at += a.shape[along]
        ends.append(at)
    both = jnp.concatenate(arrays, axis=along)
    return tuple(jnp.split(lax.all_gather(both, axis, axis=dim, tiled=True), ends, axis=along))


def absorb_rows(query_groups, query_pos, key_block, value_block, key_pos):
    key_count = key_block.shape[0]
    group_count = query_groups.shape[1]
    head_size = query_groups.shape[3]
    key_heads = key_block.reshape(key_count, group_count, head_size)
    value_heads = value_block.reshape(key_count, group_count, head_size)
    scores = jnp.einsum(
        "qgrd,kgd->grqk", query_groups, key_heads, preferred_element_type=jnp.float32
    ) * head_size ** (-0.5)
    visible = key_pos[None, :] <= query_pos[:, None]
    new_peak = jnp.max(jnp.where(visible, scores, negative_fill), axis=-1)
    exp_scores = jnp.where(visible, jnp.exp(scores - new_peak[..., None]), 0.0)
    new_total = jnp.sum(exp_scores, axis=-1)
    products = jnp.einsum(
        "grqk,kgd->grqd",
        exp_scores.astype(jnp.bfloat16),
        value_heads,
        preferred_element_type=jnp.float32,
    )
    return new_total, products


def regroup(rows):
    width = rows.shape[1]
    zl = lax.axis_index("head") // 4
    parts = rows.reshape(2, 4, 2, 32, width)
    own = jnp.where(zl == 0, parts[0], parts[1])
    other = jnp.where(zl == 0, parts[1], parts[0])
    gives = jnp.where(zl == 0, other[:, 0], other[:, 1]).reshape(128, width)
    keeps = jnp.where(zl == 0, other[:, 1], other[:, 0]).reshape(128, width)
    gets = lax.ppermute(gives, "blk", [(b, (b + 8) % 16) for b in range(16)])
    upper = jnp.where(zl == 0, keeps, gets)
    lower = jnp.where(zl == 0, gets, keeps)
    return jnp.concatenate([own[:, 0].reshape(128, width), upper, lower, own[:, 1].reshape(128, width)], axis=0)


def local(
    hidden_in,
    queries,
    key_states,
    value_states,
    out_weight,
    norm_gain,
    gate_weight,
    up_weight,
    down_weight,
):
    own_block = lax.axis_index("blk")
    query_local, key_local, value_local = (
        lax.all_to_all(queries, "head", split_axis=1, concat_axis=0, tiled=True),
        lax.all_to_all(key_states, "head", split_axis=1, concat_axis=0, tiled=True),
        lax.all_to_all(value_states, "head", split_axis=1, concat_axis=0, tiled=True),
    )
    hidden_local = lax.all_to_all(hidden_in, "head", split_axis=1, concat_axis=0, tiled=True)
    wo = lax.all_to_all(out_weight, "head", split_axis=1, concat_axis=0, tiled=True)
    block_rows = query_local.shape[0]
    query_width = query_local.shape[1]
    key_width = key_local.shape[1]
    group_count = key_width // HEAD_DIM
    group_ratio = HEADS // KV_HEADS
    local_index = jnp.arange(block_rows, dtype=jnp.int32)
    query_pos = own_block * block_rows + local_index
    query_groups = query_local.reshape(block_rows, group_count, group_ratio, HEAD_DIM)
    key_block, value_block = sent_together((key_local, value_local), "blk", 0, 1)
    key_pos = jnp.arange(key_block.shape[0], dtype=jnp.int32)
    row_total, weighted = absorb_rows(query_groups, query_pos, key_block, value_block, key_pos)
    attended = (
        (weighted / row_total[..., None])
        .transpose(2, 0, 1, 3)
        .reshape(block_rows, query_width)
        .astype(jnp.bfloat16)
    )
    att = regroup(attended)
    hid = regroup(hidden_local)
    return feed_forward(att, hid, wo, norm_gain.reshape(4 * 8, 128), gate_weight, up_weight, down_weight)


def solution(mesh):
    return jax.shard_map(
        local,
        mesh=mesh,
        in_specs=(
            P(("blk", "head"), None),
            P(("blk", "head"), None),
            P(("blk", "head"), None),
            P(("blk", "head"), None),
            P("head", None),
            P(),
            P(None, "head"),
            P(None, "head"),
            P("head", None),
        ),
        out_specs=P(("blk", "head"), None),
        check_vma=False,
    )
```

```python
import jax
import jax.numpy as jnp
from jax import lax
from jax.experimental import pallas as pl
from jax.experimental.pallas import tpu as pltpu
from jax.sharding import PartitionSpec as P

HEAD_DIM = 128
MESH = pl.DeviceIdType.MESH
F32 = jnp.float32
BF16 = jnp.bfloat16

negative_fill = -1e30


class Place:
    def __init__(self):
        self.head = lax.axis_index("head")
        self.blk = lax.axis_index("blk")
        self.x = lax.rem(self.head, 4)
        self.zl = self.head // 4
        self.zh = self.blk // 8
        self.yc = lax.rem(self.blk, 8)
        self.z = self.zh * 2 + self.zl
        self.xs = [lax.rem(self.x + k, 4) for k in range(4)]
        self.right = self.at_x(self.xs[1])
        self.left = self.at_x(self.xs[3])
        self.above = self.at_z(1)
        self.below = self.at_z(3)

        self.y = self.yc // 2
        self.core = lax.rem(self.blk, 2)
        self.chip = self.blk // 2
        self.up = self.at_y(1)
        self.down = self.at_y(3)
        self.partner = (self.head, self.blk + 1 - 2 * self.core)
        self.across = (self.head, (1 - self.zh) * 8 + self.yc)

    def at_y(self, step):
        return (self.head, self.zh * 8 + lax.rem(self.y + step, 4) * 2 + self.core)

    def plane(self, step, k):
        z = lax.rem(self.z + step, 4)
        return (lax.rem(z, 2) * 4 + self.xs[k], (z // 2) * 8 + self.yc)

    def chip_at(self, dz, k):
        return lax.rem(self.zh + dz, 2) * 4 + lax.rem(self.y + k, 4)

    def at_x(self, x):
        return (self.zl * 4 + x, self.blk)

    def at_z(self, step):
        z = lax.rem(self.z + step, 4)
        return (lax.rem(z, 2) * 4 + self.x, (z // 2) * 8 + self.yc)

    def here(self, k):
        return self.zl * 4 + self.xs[k]

    def other(self, k):
        return (1 - self.zl) * 4 + self.xs[k]


def remote(src, dst, send_sem, recv_sem, device):
    return pltpu.make_async_remote_copy(
        src_ref=src, dst_ref=dst, send_sem=send_sem, recv_sem=recv_sem,
        device_id=device, device_id_type=MESH,
    )


def gather_rows(p, buf, send_sem, recv, steps, compute):
    def send(h, s, half, to_half, kind, device):
        remote(buf.at[h, s, half], buf.at[h, s, to_half], send_sem, recv.at[kind, s], device).start()

    def wait(h, s, half, kind):
        remote(buf.at[h, s, half], buf.at[h, s, half], send_sem, recv.at[kind, s], p.right).wait_recv()

    me, left, right, far = p.here(0), p.here(3), p.here(1), p.here(2)
    for s in range(steps):
        send(me, s, 0, 0, 0, p.right)
        send(me, s, 1, 1, 4, p.left)
        send(me, s, 0, 1, 6, p.above)
        send(me, s, 1, 0, 10, p.below)
    for s in range(steps):
        send(me, s, 1, 1, 1, p.right)
        send(me, s, 0, 0, 3, p.left)
    compute(me, True)
    for s in range(steps):
        wait(left, s, 0, 0)
        send(left, s, 0, 0, 2, p.right)
        send(left, s, 0, 1, 7, p.above)
        wait(right, s, 1, 4)
        send(right, s, 1, 1, 5, p.left)
        send(right, s, 1, 0, 12, p.below)
    for s in range(steps):
        wait(p.other(0), s, 1, 6)
        wait(p.other(0), s, 0, 10)
    compute(p.other(0), False)
    for s in range(steps):
        wait(left, s, 1, 1)
        send(left, s, 1, 0, 11, p.below)
        wait(right, s, 0, 3)
        send(right, s, 0, 1, 8, p.above)
    compute(left, False)
    compute(right, False)
    for s in range(steps):
        wait(far, s, 0, 2)
        send(far, s, 0, 1, 9, p.above)
        wait(far, s, 1, 5)
        send(far, s, 1, 0, 13, p.below)
    compute(far, False)
    for k, up, down in ((3, 7, 11), (1, 8, 12), (2, 9, 13)):
        for s in range(steps):
            wait(p.other(k), s, 1, up)
            wait(p.other(k), s, 0, down)
        compute(p.other(k), False)
    pltpu.make_async_copy(buf.at[0:7], buf.at[0:7], send_sem).wait()


def columns(h, width):
    return pl.ds(pl.multiple_of(h * width, width), width)


SCALE = HEAD_DIM ** (-0.5) * 1.4426950408889634


def attend_blocks(
    p, q, k, v, hid_in, wo_hbm, kv, qbuf, hid, wo, qs, oa, peak, abuf,
    sk, kv1, q1, h1, w1, w2, ysem, zrecv, csem, wown,
):
    own = p.blk
    mine = pl.ds(pl.multiple_of(p.x * 32, 32), 32)

    def rows_of(g):
        return pl.ds(pl.multiple_of(g * 128 + p.x * 32, 32), 32)

    kv_rows = pl.ds(pl.multiple_of(p.head * 64, 64), 64)

    def send_kv(device):
        h = device[0]
        remote(k.at[:, columns(h, 128)], kv.at[own, kv_rows, 0:128], sk, kv1, device).start()
        remote(v.at[:, columns(h, 128)], kv.at[own, kv_rows, 128:256], sk, kv1, device).start()

    def send_rows(src, dst, sem, width, part, g, device):
        at = columns(device[0], width)
        remote(src.at[part * 32 : (part + 1) * 32, at], dst.at[rows_of(g), :], sk, sem, device).start()

    near = 1 - 2 * p.zl + 4
    for kx in range(4):
        send_kv(p.plane(near, kx))
        if kx:
            send_kv(p.plane(0, kx))
    for kx in range(4):
        send_rows(q, qbuf, q1, 256, 0, 2, p.plane(1, kx))
        send_rows(q, qbuf, q1, 256, 1, 1, p.plane(3, kx))
        if kx:
            send_rows(q, qbuf, q1, 256, 0, 0, p.plane(0, kx))
            send_rows(q, qbuf, q1, 256, 1, 3, p.plane(0, kx))

    def block(dz, kk, other=False):
        core = 1 - p.core if other else p.core
        return p.chip_at(dz, kk) * 2 + core

    def piece(dz, kk, part):
        return kv.at[block(dz, kk), part * 256 : (part + 1) * 256, 0:256]

    def send_piece(dz, kk, part, sem, device):
        remote(piece(dz, kk, part), piece(dz, kk, part), sk, sem, device).start()

    def wait_piece(dz, kk, part, sem):
        remote(piece(dz, kk, part), piece(dz, kk, part), sk, sem, p.up).wait_recv()

    def share(dz, kk, sem):
        ref = kv.at[block(dz, kk), :, 0:256]
        remote(ref, ref, sk, sem, p.partner).start()

    def wait_shared(dz, kk, sem):
        ref = kv.at[block(dz, kk, True), :, 0:256]
        remote(ref, ref, sk, sem, p.partner).wait_recv()

    def send_both(dz):
        i = 3 * dz
        send_piece(dz, 0, 0, ysem.at[0, i], p.up)
        send_piece(dz, 0, 1, ysem.at[1, i + 1], p.down)
        send_piece(dz, 0, 1, ysem.at[0, i + 1], p.up)
        send_piece(dz, 0, 0, ysem.at[1, i], p.down)

    def forward(dz):
        i = 3 * dz
        wait_piece(dz, 3, 0, ysem.at[0, i])
        send_piece(dz, 3, 0, ysem.at[0, i + 2], p.up)
        wait_piece(dz, 1, 1, ysem.at[1, i + 1])
        send_piece(dz, 1, 1, ysem.at[1, i + 2], p.down)

    def near_done(dz):
        i = 3 * dz
        wait_piece(dz, 3, 1, ysem.at[0, i + 1])
        share(dz, 3, csem.at[4 * dz + 3])
        wait_piece(dz, 1, 0, ysem.at[1, i])
        share(dz, 1, csem.at[4 * dz + 1])

    def far_done(dz):
        i = 3 * dz
        wait_piece(dz, 2, 0, ysem.at[0, i + 2])
        wait_piece(dz, 2, 1, ysem.at[1, i + 2])
        share(dz, 2, csem.at[4 * dz + 2])

    ref = kv.at[own, 0:448, 0:256]
    remote(ref, ref, sk, kv1, p.up).wait_recv()
    send_both(0)
    for part in range(2):
        send_piece(0, 0, part, zrecv.at[part], p.across)
    share(0, 0, csem.at[0])
    for kx in range(4):
        send_rows(hid_in, hid, h1, 512, 0, 2, p.plane(1, kx))
        send_rows(hid_in, hid, h1, 512, 1, 1, p.plane(3, kx))
        if kx:
            send_rows(hid_in, hid, h1, 512, 0, 0, p.plane(0, kx))
            send_rows(hid_in, hid, h1, 512, 1, 3, p.plane(0, kx))

    ref = qbuf.at[0:448]
    remote(ref, ref, sk, q1, p.up).wait_recv()
    same = 1 + p.zl
    for r in range(2):
        cols = slice(r * 128, (r + 1) * 128)
        qs[r * 384 : r * 384 + 128] = qbuf[0:128, cols]
        qs[r * 384 + 128 : r * 384 + 256] = qbuf[pl.ds(pl.multiple_of(same * 128, 128), 128), cols]
        qs[r * 384 + 256 : r * 384 + 384] = qbuf[384:512, cols]
        qs[768 + r * 128 : 896 + r * 128] = qbuf[pl.ds(pl.multiple_of((3 - same) * 128, 128), 128), cols]
    oa[...] = jnp.zeros_like(oa)
    peak[...] = jnp.full_like(peak, negative_fill)

    def absorb(start, count, chip, row_pos):
        rows = pl.ds(start, count)
        keys = kv[pl.ds(chip * 2, 2), :, 0:128].reshape(1024, 128)
        s = lax.dot_general(qs[rows], keys, (((1,), (1,)), ((), ())), preferred_element_type=F32)
        if row_pos is not None:
            i = lax.broadcasted_iota(jnp.int32, (count, 1), 0)
            key_pos = chip * 1024 + lax.broadcasted_iota(jnp.int32, (count, 1024), 1)
            s = jnp.where(key_pos <= row_pos(i), s, negative_fill)
        old = peak[rows]
        new = jnp.maximum(old, jnp.max(s, axis=1, keepdims=True))
        peak[rows] = new
        w = jnp.exp2((s - new[:, 0:1]) * SCALE).astype(BF16)
        shrink = jnp.exp2((old - new) * SCALE)
        values = kv[pl.ds(chip * 2, 2), :, 128:384].reshape(1024, 256)
        part = jnp.dot(w, values, preferred_element_type=F32)
        oa[rows, 0:128] = oa[rows, 0:128] * shrink + part[:, 0:128]
        oa[rows, 128:256] = oa[rows, 128:256] * shrink + part[:, 128:256]

    def spread(i):
        return ((i & 96) << 1) + (i & 31)

    def pos_a(i):
        seg = i >> 7
        shift = jnp.where(seg == 1, (1 - p.zl) * 288, p.zl * 256 + (seg >> 1) * 32)
        return own * 512 + spread(i & 127) + shift

    chip_b = (1 - p.zh) * 4 + p.y

    def pos_b(i):
        return (chip_b * 2 + p.core) * 512 + spread(i & 127) + (1 - p.zl) * 256 + p.zl * 32

    def absorb_a(chip, masked):
        def one(r, _):
            absorb(pl.multiple_of(r * 384, 128), 384, chip, pos_a if masked else None)
            return 0

        lax.fori_loop(0, 2, one, 0)

    def absorb_b(chip, masked):
        absorb(768, 256, chip, pos_b if masked else None)

    def seen(chip):
        @pl.when(chip < p.chip)
        def _():
            absorb_a(chip, False)

        @pl.when(chip < chip_b)
        def _():
            absorb_b(chip, False)

    wait_shared(0, 0, csem.at[0])
    absorb_a(p.chip, True)

    @pl.when(p.chip < chip_b)
    def _():
        absorb_b(p.chip, False)

    forward(0)
    near_done(0)
    for part in range(2):
        wait_piece(1, 0, part, zrecv.at[part])
    send_both(1)
    share(1, 0, csem.at[4])
    half = pl.ds(pl.multiple_of(p.core * 128, 128), 128)
    for kx in range(4):
        if kx:
            device = p.plane(0, kx)
            remote(
                wo_hbm.at[half, columns(device[0], 512)], wo.at[p.head, p.core], sk, w1, device
            ).start()
        for part in range(2):
            device = p.plane(1 + 2 * part, kx)
            rows = pl.ds(pl.multiple_of(p.core * 128 + part * 64, 64), 64)
            remote(
                wo_hbm.at[rows, columns(device[0], 512)],
                wo.at[p.head, p.core, part * 64 : (part + 1) * 64], sk, w1, device,
            ).start()
    wait_shared(0, 3, csem.at[3])
    wait_shared(0, 1, csem.at[1])

    def near_step(t, _):
        seen(p.chip_at(0, 3 - 2 * t))
        return 0

    lax.fori_loop(0, 2, near_step, 0)
    far_done(0)
    forward(1)
    wait_shared(1, 0, csem.at[4])
    chip = p.chip_at(1, 0)

    @pl.when(chip < p.chip)
    def _():
        absorb_a(chip, False)

    absorb_b(chip, True)
    near_done(1)
    wait_shared(0, 2, csem.at[2])
    wait_shared(1, 3, csem.at[7])
    wait_shared(1, 1, csem.at[5])

    def late_step(t, _):
        @pl.when(t == 3)
        def _():
            far_done(1)
            wait_shared(1, 2, csem.at[6])

        seen(p.chip_at(jnp.minimum(t, 1), 2 + t - 3 * (t // 2)))
        return 0

    lax.fori_loop(0, 4, late_step, 0)

    wown.wait()
    ref = wo.at[0:7, 0]
    remote(ref, ref, sk, w1, p.up).wait_recv()
    ref = wo.at[:, p.core]
    remote(ref, ref, sk, w2, p.partner).start()

    for r in range(2):
        a = (oa[r * 384 : (r + 1) * 384, 0:128] / oa[r * 384 : (r + 1) * 384, 128:256]).astype(BF16)
        abuf[p.head, r, 0, 0:128] = a[0:128]
        abuf[p.head, r, p.zl, pl.ds(pl.multiple_of((1 - p.zl) * 128, 128), 128)] = a[128:256]
        abuf[p.head, r, 1, 128:256] = a[256:384]
        b = (oa[768 + r * 128 : 896 + r * 128, 0:128] / oa[768 + r * 128 : 896 + r * 128, 128:256]).astype(BF16)
        abuf[p.head, r, 1 - p.zl, pl.ds(pl.multiple_of(p.zl * 128, 128), 128)] = b

    ref = hid.at[0:448]
    remote(ref, ref, sk, h1, p.up).wait_recv()
    ref = wo.at[:, 1 - p.core]
    remote(ref, ref, sk, w2, p.partner).wait_recv()

    for ref in (
        qbuf.at[0:448], hid.at[0:448], kv.at[own, 0:448, 0:256], kv.at[0:15, :, 0:256], wo.at[0:7, 0], wo.at[:, p.core],
    ):
        pltpu.make_async_copy(ref, ref, sk).wait()


NS1 = 2
NS2 = 4
NC = 8
CW = 512
FFL = 896


def block_kernel(
    q, k, v, hid_in, gain, wo_hbm, gate_hbm, up_hbm, down_hbm, out,
    kv, qbuf, qs, oa, peak,
    abuf, rbuf, hid, wo, wgu, wd, oacc, acc, xg, sq, inner,
    zs, zr, keep, m1s, m1r, m2s, m2r,
    wsem, sk, kv1, q1, h1, w1, w2, ysem, zrecv, csem,
    s1, r1, s2, r2, s3, zsem, m1sem, m2sem,
):
    p = Place()
    barrier = pltpu.get_barrier_semaphore()
    peers = [p.plane(0, kx) for kx in (1, 2, 3)]
    peers += [p.plane(step, kx) for step in (1, 3) for kx in range(4)]
    peers += [p.up, p.down, p.across, p.partner]
    for device in peers:
        pl.semaphore_signal(barrier, inc=1, device_id=device, device_id_type=MESH)

    order = [p.here(0), p.other(0), p.here(3), p.here(1), p.here(2), p.other(3), p.other(1), p.other(2)]
    half = pl.ds(pl.multiple_of(p.core * 128, 128), 128)
    wo_copy = pltpu.make_async_copy(
        wo_hbm.at[half, columns(p.head, 512)], wo.at[p.head, p.core], wsem.at[16]
    )
    wd_copy = pltpu.make_async_copy(down_hbm, wd, wsem.at[17])

    def gate_copy(h):
        rows = pl.ds(pl.multiple_of(h * 512, 512), 512)
        return pltpu.make_async_copy(gate_hbm.at[rows], wgu.at[rows, 0:FFL], wsem.at[h])

    def up_copy(h):
        rows = pl.ds(pl.multiple_of(h * 512, 512), 512)
        return pltpu.make_async_copy(up_hbm.at[rows], wgu.at[rows, FFL : 2 * FFL], wsem.at[8 + h])

    wo_copy.start()
    for h in order:
        gate_copy(h).start()
        up_copy(h).start()
    wd_copy.start()

    me = p.here(0)
    c1 = 256 // NS1
    kv[:, :, 256:384] = jnp.ones((16, 512, 128), BF16)
    kv_rows = pl.ds(pl.multiple_of(p.head * 64, 64), 64)
    kv[p.blk, kv_rows, 0:128] = k[:, columns(p.head, 128)]
    kv[p.blk, kv_rows, 128:256] = v[:, columns(p.head, 128)]
    for part in range(2):
        rows = pl.ds(pl.multiple_of(part * 384 + p.x * 32, 32), 32)
        qbuf[rows, :] = q[part * 32 : (part + 1) * 32, columns(p.head, 256)]
        hid[rows, :] = hid_in[part * 32 : (part + 1) * 32, columns(p.head, 512)]
    pl.semaphore_wait(barrier, len(peers))
    attend_blocks(
        p, q, k, v, hid_in, wo_hbm, kv, qbuf, hid, wo, qs, oa, peak, abuf,
        sk, kv1, q1, h1, w1, w2, ysem, zrecv, csem, wo_copy,
    )

    def project(h, first):
        a = jnp.concatenate([abuf[h, s].reshape(512, c1) for s in range(NS1)], axis=1)
        w = wo[h].reshape(256, 512)
        for n in range(2):
            cols = slice(n * 256, (n + 1) * 256)
            part = jnp.dot(a, w[:, cols], preferred_element_type=F32)
            if first:
                oacc[:, cols] = hid[:, cols].astype(F32) + part
            else:
                oacc[:, cols] += part

    gather_rows(p, abuf, s1, r1, NS1, project)

    c2 = 512 // NS2
    for s in range(NS2):
        for half in range(2):
            rbuf[me, s, half] = oacc[half * 256 : (half + 1) * 256, s * c2 : (s + 1) * c2].astype(BF16)

    def expand(h, first):
        gate_copy(h).wait()
        up_copy(h).wait()
        total = None
        for s in range(NS2):
            r = rbuf[h, s].reshape(512, c2).astype(F32)
            g = gain[pl.ds(h * NS2 + s, 1), :]
            xg[:, s * c2 : (s + 1) * c2] = (r * g).astype(BF16)
            total = r * r if total is None else total + r * r
        if first:
            sq[...] = total
        else:
            sq[...] += total
        rows = pl.ds(pl.multiple_of(h * 512, 512), 512)

        def tile(n, _):
            cols = pl.ds(pl.multiple_of(n * 256, 256), 256)
            part = jnp.dot(xg[...], wgu[rows, cols], preferred_element_type=F32)
            if first:
                acc[:, cols] = part
            else:
                acc[:, cols] += part
            return 0

        lax.fori_loop(0, 7, tile, 0)

    gather_rows(p, rbuf, s2, r2, NS2, expand)

    scale = lax.rsqrt(jnp.sum(sq[...], axis=1, keepdims=True) * (1.0 / 4096.0) + 1e-5)
    sq[...] = jnp.broadcast_to(scale, (512, 128))

    def activate(j, _):
        at = pl.multiple_of(j * 128, 128)
        u = acc[:, pl.ds(at, 128)] * sq[...]
        v = acc[:, pl.ds(pl.multiple_of(at + FFL, 128), 128)] * sq[...]
        inner[:, pl.ds(at, 128)] = (u / (1.0 + jnp.exp(-u)) * v).astype(BF16)
        return 0

    lax.fori_loop(0, 7, activate, 0)

    def z_copy(c, side):
        device = p.above if side == 0 else p.below
        return remote(zs.at[c, side], zr.at[c, 1 - side], s3, zsem.at[1 - side, c], device)

    def z_wait(c, side):
        remote(zr.at[c, side], zr.at[c, side], s3, zsem.at[side, c], p.right).wait_recv()

    def reduce_down(c, _):
        for n in range(2):
            at = slice(n * 256, (n + 1) * 256)
            cols = pl.ds(pl.multiple_of(c * CW + n * 256, 256), 256)
            part = jnp.dot(inner[...], wd[:, cols], preferred_element_type=F32)
            keep[c, 0, :, at] = part[0:128]
            zs[c, 0, :, at] = part[128:256].astype(BF16)
            zs[c, 1, :, at] = part[256:384].astype(BF16)
            keep[c, 1, :, at] = part[384:512]
        z_copy(c, 0).start()
        z_copy(c, 1).start()
        return 0

    wd_copy.wait()
    lax.fori_loop(0, NC, reduce_down, 0)

    def slot(k):
        return pl.ds(pl.multiple_of(p.xs[k] * 32, 32), 32)

    def m1_copy(c, side):
        device = p.right if side == 0 else p.left
        return remote(m1s.at[c, side], m1r.at[c, side], s3, m1sem.at[side, c], device)

    def m2_copy(c, side):
        device = p.right if side == 0 else p.left
        return remote(m2s.at[c, side], m2r.at[c, side], s3, m2sem.at[side, c], device)

    def finish(t, _):
        @pl.when(t < NC)
        def _():
            c = t
            for side in range(2):
                z_wait(c, side)
                keep[c, side] += zr[c, side].astype(F32)
                m1s[c, side] = keep[c, side, slot(2), :].astype(BF16)
                m1_copy(c, side).start()

        @pl.when((t >= 1) & (t < NC + 1))
        def _():
            c = t - 1
            for side in range(2):
                m1_copy(c, side).wait_recv()
                k = 1 if side == 0 else 3
                for part in range(2):
                    q = keep[c, part, slot(k), :]
                    if part == side:
                        q = q + m1r[c, side].astype(F32)
                    m2s[c, side, part] = q.astype(BF16)
                m2_copy(c, side).start()

        @pl.when(t >= 2)
        def _():
            c = t - 2
            for side in range(2):
                m2_copy(c, side).wait_recv()
            for part in range(2):
                q = keep[c, part, slot(0), :] + m2r[c, 0, part].astype(F32) + m2r[c, 1, part].astype(F32)
                rows = pl.ds(pl.multiple_of(part * 128 + p.x * 32, 32), 32)
                for s in range(NS2):
                    r = rbuf[c, s, part, rows, :].astype(F32)
                    cols = pl.ds(pl.multiple_of(c * CW + s * c2, c2), c2)
                    out[part * 32 : (part + 1) * 32, cols] = (r + q[:, s * c2 : (s + 1) * c2]).astype(BF16)

        return 0

    lax.fori_loop(0, NC + 2, finish, 0)
    pltpu.make_async_copy(zs, zs, s3).wait()
    pltpu.make_async_copy(m1s, m1s, s3).wait()
    pltpu.make_async_copy(m2s, m2s, s3).wait()


def layer(q, k, v, hidden, gain, wo, gate, up, down):
    vmem = pl.BlockSpec(memory_space=pltpu.VMEM)
    hbm = pl.BlockSpec(memory_space=pl.ANY)
    dma = pltpu.SemaphoreType.DMA
    return pl.pallas_call(
        block_kernel,
        out_shape=jax.ShapeDtypeStruct((64, 4096), BF16),
        in_specs=[vmem, vmem, vmem, vmem, vmem, hbm, hbm, hbm, hbm],
        out_specs=vmem,
        scratch_shapes=[
            pltpu.VMEM((16, 512, 384), BF16),
            pltpu.VMEM((512, 256), BF16),
            pltpu.VMEM((1024, 128), BF16),
            pltpu.VMEM((1024, 256), F32),
            pltpu.VMEM((1024, 128), F32),
            pltpu.VMEM((8, NS1, 2, 256, 256 // NS1), BF16),
            pltpu.VMEM((8, NS2, 2, 256, 512 // NS2), BF16),
            pltpu.VMEM((512, 512), BF16),
            pltpu.VMEM((8, 2, 128, 512), BF16),
            pltpu.VMEM((4096, 2 * FFL), BF16),
            pltpu.VMEM((FFL, 4096), BF16),
            pltpu.VMEM((512, 512), F32),
            pltpu.VMEM((512, 2 * FFL), F32),
            pltpu.VMEM((512, 512), BF16),
            pltpu.VMEM((512, 128), F32),
            pltpu.VMEM((512, FFL), BF16),
            pltpu.VMEM((NC, 2, 128, CW), BF16),
            pltpu.VMEM((NC, 2, 128, CW), BF16),
            pltpu.VMEM((NC, 2, 128, CW), F32),
            pltpu.VMEM((NC, 2, 32, CW), BF16),
            pltpu.VMEM((NC, 2, 32, CW), BF16),
            pltpu.VMEM((NC, 2, 2, 32, CW), BF16),
            pltpu.VMEM((NC, 2, 2, 32, CW), BF16),
            dma((18,)),
            dma,
            dma,
            dma,
            dma,
            dma,
            dma,
            dma((2, 6)),
            dma((2,)),
            dma((8,)),
            dma,
            dma((14, NS1)),
            dma,
            dma((14, NS2)),
            dma,
            dma((2, NC)),
            dma((2, NC)),
            dma((2, NC)),
        ],
        compiler_params=pltpu.CompilerParams(
            collective_id=1, has_side_effects=True, vmem_limit_bytes=62 * 1024 * 1024
        ),
        cost_estimate=pl.CostEstimate(flops=16_500_000_000, bytes_accessed=24_000_000, transcendentals=0),
        name="layer",
    )(q, k, v, hidden, gain, wo, gate, up, down)


def local(
    hidden_in,
    queries,
    key_states,
    value_states,
    out_weight,
    norm_gain,
    gate_weight,
    up_weight,
    down_weight,
):
    return layer(
        queries, key_states, value_states, hidden_in, norm_gain.reshape(32, 128),
        out_weight, gate_weight, up_weight, down_weight,
    )


def solution(mesh):
    return jax.shard_map(
        local,
        mesh=mesh,
        in_specs=(
            P(("blk", "head"), None),
            P(("blk", "head"), None),
            P(("blk", "head"), None),
            P(("blk", "head"), None),
            P("head", None),
            P(),
            P(None, "head"),
            P(None, "head"),
            P("head", None),
        ),
        out_specs=P(("blk", "head"), None),
        check_vma=False,
    )
```

```python
import jax
import jax.numpy as jnp
from jax import lax
from jax.experimental import pallas as pl
from jax.experimental.pallas import tpu as pltpu
from jax.sharding import PartitionSpec as P

HEAD_DIM = 128
MESH = pl.DeviceIdType.MESH
F32 = jnp.float32
BF16 = jnp.bfloat16

negative_fill = -1e30


class Place:
    def __init__(self):
        self.head = lax.axis_index("head")
        self.blk = lax.axis_index("blk")
        self.x = lax.rem(self.head, 4)
        self.zl = self.head // 4
        self.zh = self.blk // 8
        self.yc = lax.rem(self.blk, 8)
        self.z = self.zh * 2 + self.zl
        self.xs = [lax.rem(self.x + k, 4) for k in range(4)]
        self.right = self.at_x(self.xs[1])
        self.left = self.at_x(self.xs[3])
        self.above = self.at_z(1)
        self.below = self.at_z(3)

        self.y = self.yc // 2
        self.core = lax.rem(self.blk, 2)
        self.chip = self.blk // 2
        self.up = self.at_y(1)
        self.down = self.at_y(3)
        self.partner = (self.head, self.blk + 1 - 2 * self.core)
        self.across = (self.head, (1 - self.zh) * 8 + self.yc)

    def at_y(self, step):
        return (self.head, self.zh * 8 + lax.rem(self.y + step, 4) * 2 + self.core)

    def plane(self, step, k):
        z = lax.rem(self.z + step, 4)
        return (lax.rem(z, 2) * 4 + self.xs[k], (z // 2) * 8 + self.yc)

    def chip_at(self, dz, k):
        return lax.rem(self.zh + dz, 2) * 4 + lax.rem(self.y + k, 4)

    def at_x(self, x):
        return (self.zl * 4 + x, self.blk)

    def at_z(self, step):
        z = lax.rem(self.z + step, 4)
        return (lax.rem(z, 2) * 4 + self.x, (z // 2) * 8 + self.yc)

    def here(self, k):
        return self.zl * 4 + self.xs[k]

    def other(self, k):
        return (1 - self.zl) * 4 + self.xs[k]


def remote(src, dst, send_sem, recv_sem, device):
    return pltpu.make_async_remote_copy(
        src_ref=src, dst_ref=dst, send_sem=send_sem, recv_sem=recv_sem,
        device_id=device, device_id_type=MESH,
    )


def gather_rows(p, buf, send_sem, recv, steps, compute):
    def send(h, s, half, to_half, kind, device):
        remote(buf.at[h, s, half], buf.at[h, s, to_half], send_sem, recv.at[kind, s], device).start()

    def wait(h, s, half, kind):
        remote(buf.at[h, s, half], buf.at[h, s, half], send_sem, recv.at[kind, s], p.right).wait_recv()

    me, left, right, far = p.here(0), p.here(3), p.here(1), p.here(2)
    for s in range(steps):
        send(me, s, 0, 0, 0, p.right)
        send(me, s, 1, 1, 4, p.left)
        send(me, s, 0, 1, 6, p.above)
        send(me, s, 1, 0, 10, p.below)
    for s in range(steps):
        send(me, s, 1, 1, 1, p.right)
        send(me, s, 0, 0, 3, p.left)
    compute(me, True)
    for s in range(steps):
        wait(left, s, 0, 0)
        send(left, s, 0, 0, 2, p.right)
        send(left, s, 0, 1, 7, p.above)
        wait(right, s, 1, 4)
        send(right, s, 1, 1, 5, p.left)
        send(right, s, 1, 0, 12, p.below)
    for s in range(steps):
        wait(p.other(0), s, 1, 6)
        wait(p.other(0), s, 0, 10)
    compute(p.other(0), False)
    for s in range(steps):
        wait(left, s, 1, 1)
        send(left, s, 1, 0, 11, p.below)
        wait(right, s, 0, 3)
        send(right, s, 0, 1, 8, p.above)
    compute(left, False)
    compute(right, False)
    for s in range(steps):
        wait(far, s, 0, 2)
        send(far, s, 0, 1, 9, p.above)
        wait(far, s, 1, 5)
        send(far, s, 1, 0, 13, p.below)
    compute(far, False)
    for k, up, down in ((3, 7, 11), (1, 8, 12), (2, 9, 13)):
        for s in range(steps):
            wait(p.other(k), s, 1, up)
            wait(p.other(k), s, 0, down)
        compute(p.other(k), False)
    pltpu.make_async_copy(buf.at[0:7], buf.at[0:7], send_sem).wait()


def columns(h, width):
    return pl.ds(pl.multiple_of(h * width, width), width)


SCALE = HEAD_DIM ** (-0.5) * 1.4426950408889634


def attend_blocks(
    p, q, k, v, hid_in, wo_hbm, kv, qbuf, hid, wo, qs, oa, peak, abuf,
    sk, kv1, q1, h1, w1, w2, ysem, zrecv, csem, wown,
):
    own = p.blk
    mine = pl.ds(pl.multiple_of(p.x * 32, 32), 32)

    def rows_of(g):
        return pl.ds(pl.multiple_of(g * 128 + p.x * 32, 32), 32)

    kv_rows = pl.ds(pl.multiple_of(p.head * 64, 64), 64)

    def send_kv(device, sem):
        h = device[0]
        remote(k.at[:, columns(h, 128)], kv.at[own, kv_rows, 0:128], sk, sem, device).start()
        remote(v.at[:, columns(h, 128)], kv.at[own, kv_rows, 128:256], sk, sem, device).start()

    def send_rows(src, dst, sem, width, part, g, device):
        at = columns(device[0], width)
        remote(src.at[part * 32 : (part + 1) * 32, at], dst.at[rows_of(g), :], sk, sem, device).start()

    near = 1 - 2 * p.zl + 4
    for kx in range(4):
        send_kv(p.plane(near, kx), kv1.at[1])
        if kx:
            send_kv(p.plane(0, kx), kv1.at[0])
    for kx in range(4):
        send_rows(q, qbuf, q1, 256, 0, 2, p.plane(1, kx))
        send_rows(q, qbuf, q1, 256, 1, 1, p.plane(3, kx))
        if kx:
            send_rows(q, qbuf, q1, 256, 0, 0, p.plane(0, kx))
            send_rows(q, qbuf, q1, 256, 1, 3, p.plane(0, kx))

    def block(dz, kk, other=False):
        core = 1 - p.core if other else p.core
        return p.chip_at(dz, kk) * 2 + core

    def piece(dz, kk, part):
        return kv.at[block(dz, kk), part * 256 : (part + 1) * 256, 0:256]

    def send_piece(dz, kk, part, sem, device):
        remote(piece(dz, kk, part), piece(dz, kk, part), sk, sem, device).start()

    def wait_piece(dz, kk, part, sem):
        remote(piece(dz, kk, part), piece(dz, kk, part), sk, sem, p.up).wait_recv()

    def share(dz, kk, sem):
        ref = kv.at[block(dz, kk), :, 0:256]
        remote(ref, ref, sk, sem, p.partner).start()

    def wait_shared(dz, kk, sem):
        ref = kv.at[block(dz, kk, True), :, 0:256]
        remote(ref, ref, sk, sem, p.partner).wait_recv()

    def send_both(dz):
        i = 3 * dz
        send_piece(dz, 0, 0, ysem.at[0, i], p.up)
        send_piece(dz, 0, 1, ysem.at[1, i + 1], p.down)
        send_piece(dz, 0, 1, ysem.at[0, i + 1], p.up)
        send_piece(dz, 0, 0, ysem.at[1, i], p.down)

    def forward(dz):
        i = 3 * dz
        wait_piece(dz, 3, 0, ysem.at[0, i])
        send_piece(dz, 3, 0, ysem.at[0, i + 2], p.up)
        wait_piece(dz, 1, 1, ysem.at[1, i + 1])
        send_piece(dz, 1, 1, ysem.at[1, i + 2], p.down)

    def near_done(dz):
        i = 3 * dz
        wait_piece(dz, 3, 1, ysem.at[0, i + 1])
        share(dz, 3, csem.at[4 * dz + 3])
        wait_piece(dz, 1, 0, ysem.at[1, i])
        share(dz, 1, csem.at[4 * dz + 1])

    def far_done(dz):
        i = 3 * dz
        wait_piece(dz, 2, 0, ysem.at[0, i + 2])
        wait_piece(dz, 2, 1, ysem.at[1, i + 2])
        share(dz, 2, csem.at[4 * dz + 2])

    def own_rows(part):
        return kv.at[own, pl.ds(pl.multiple_of(part * 256, 256), 256), 0:256]

    for order, (part, count) in enumerate(((p.zl, 192), (1 - p.zl, 256))):
        ref = kv.at[own, 0:count, 0:256]
        remote(ref, ref, sk, kv1.at[order], p.up).wait_recv()
        ref = own_rows(part)
        remote(ref, ref, sk, ysem.at[0, part], p.up).start()
        remote(ref, ref, sk, ysem.at[1, part], p.down).start()
        remote(ref, ref, sk, zrecv.at[part], p.across).start()
    share(0, 0, csem.at[0])
    for kx in range(4):
        send_rows(hid_in, hid, h1, 512, 0, 2, p.plane(1, kx))
        send_rows(hid_in, hid, h1, 512, 1, 1, p.plane(3, kx))
        if kx:
            send_rows(hid_in, hid, h1, 512, 0, 0, p.plane(0, kx))
            send_rows(hid_in, hid, h1, 512, 1, 3, p.plane(0, kx))

    ref = qbuf.at[0:448]
    remote(ref, ref, sk, q1, p.up).wait_recv()
    same = 1 + p.zl
    for r in range(2):
        cols = slice(r * 128, (r + 1) * 128)
        qs[r * 384 : r * 384 + 128] = qbuf[0:128, cols]
        qs[r * 384 + 128 : r * 384 + 256] = qbuf[pl.ds(pl.multiple_of(same * 128, 128), 128), cols]
        qs[r * 384 + 256 : r * 384 + 384] = qbuf[384:512, cols]
        qs[768 + r * 128 : 896 + r * 128] = qbuf[pl.ds(pl.multiple_of((3 - same) * 128, 128), 128), cols]
    oa[...] = jnp.zeros_like(oa)
    peak[...] = jnp.full_like(peak, negative_fill)

    def absorb(start, count, sub, chip, row_pos):
        keys = kv[pl.ds(chip * 2, 2), :, 0:128].reshape(1024, 128)
        values = kv[pl.ds(chip * 2, 2), :, 128:384].reshape(1024, 256)
        tiles = [slice(start + at, start + at + sub) for at in range(0, count, sub)]
        asked = [qs[rows] for rows in tiles]
        olds = [peak[rows] for rows in tiles]
        sums = [oa[rows] for rows in tiles]

        def score(t):
            s = lax.dot_general(asked[t], keys, (((1,), (1,)), ((), ())), preferred_element_type=F32)
            if row_pos is not None:
                i = t * sub + lax.broadcasted_iota(jnp.int32, (sub, 1), 0)
                key_pos = chip * 1024 + lax.broadcasted_iota(jnp.int32, (sub, 1024), 1)
                s = jnp.where(key_pos <= row_pos(i), s, negative_fill)
            return [s[:, at : at + 128] for at in range(0, 1024, 128)]

        news, ends = [], []
        coming = score(0)
        for t, old in enumerate(olds):
            s = coming
            top = s[0]
            for piece in s[1:]:
                top = jnp.maximum(top, piece)
            if t + 1 < len(tiles):
                coming = score(t + 1)
            new = jnp.maximum(old, jnp.max(top, axis=1, keepdims=True))
            w = jnp.concatenate([jnp.exp2((piece - new) * SCALE).astype(BF16) for piece in s], axis=1)
            shrink = jnp.exp2((old - new) * SCALE)
            part = jnp.dot(w, values, preferred_element_type=F32)
            news.append(new)
            ends.append(sums[t] * jnp.concatenate([shrink, shrink], axis=1) + part)
        for rows, new, end in zip(tiles, news, ends):
            peak[rows] = new
            oa[rows] = end

    def spread(i):
        return ((i & 96) << 1) + (i & 31)

    def pos_a(i):
        seg = lax.rem(i >> 7, 3)
        shift = jnp.where(seg == 1, (1 - p.zl) * 288, p.zl * 256 + (seg >> 1) * 32)
        return own * 512 + spread(i & 127) + shift

    chip_b = (1 - p.zh) * 4 + p.y

    def pos_b(i):
        return (chip_b * 2 + p.core) * 512 + spread(i & 127) + (1 - p.zl) * 256 + p.zl * 32

    def absorb_a(chip, masked):
        absorb(0, 768, 256, chip, pos_a if masked else None)

    def absorb_b(chip, masked):
        absorb(768, 256, 128, chip, pos_b if masked else None)

    def seen(chip):
        @pl.when(chip < p.chip)
        def _():
            absorb_a(chip, False)

        @pl.when(chip < chip_b)
        def _():
            absorb_b(chip, False)

    wait_shared(0, 0, csem.at[0])
    absorb_a(p.chip, True)

    @pl.when(p.chip < chip_b)
    def _():
        absorb_b(p.chip, False)

    forward(0)
    near_done(0)
    for part in range(2):
        wait_piece(1, 0, part, zrecv.at[part])
    send_both(1)
    share(1, 0, csem.at[4])
    half = pl.ds(pl.multiple_of(p.core * 128, 128), 128)
    for kx in range(4):
        if kx:
            device = p.plane(0, kx)
            remote(
                wo_hbm.at[half, columns(device[0], 512)], wo.at[p.head, p.core], sk, w1, device
            ).start()
        for part in range(2):
            device = p.plane(1 + 2 * part, kx)
            rows = pl.ds(pl.multiple_of(p.core * 128 + part * 64, 64), 64)
            remote(
                wo_hbm.at[rows, columns(device[0], 512)],
                wo.at[p.head, p.core, part * 64 : (part + 1) * 64], sk, w1, device,
            ).start()
    wait_shared(0, 3, csem.at[3])
    wait_shared(0, 1, csem.at[1])

    def near_step(t, _):
        seen(p.chip_at(0, 3 - 2 * t))
        return 0

    lax.fori_loop(0, 2, near_step, 0)
    far_done(0)
    forward(1)
    wait_shared(1, 0, csem.at[4])
    chip = p.chip_at(1, 0)

    @pl.when(chip < p.chip)
    def _():
        absorb_a(chip, False)

    absorb_b(chip, True)
    near_done(1)
    wait_shared(0, 2, csem.at[2])
    wait_shared(1, 3, csem.at[7])
    wait_shared(1, 1, csem.at[5])

    def late_step(t, _):
        @pl.when(t == 3)
        def _():
            far_done(1)
            wait_shared(1, 2, csem.at[6])

        seen(p.chip_at(jnp.minimum(t, 1), 2 + t - 3 * (t // 2)))
        return 0

    lax.fori_loop(0, 4, late_step, 0)

    wown.wait()
    ref = wo.at[0:7, 0]
    remote(ref, ref, sk, w1, p.up).wait_recv()
    ref = wo.at[:, p.core]
    remote(ref, ref, sk, w2, p.partner).start()

    for r in range(2):
        a = (oa[r * 384 : (r + 1) * 384, 0:128] / oa[r * 384 : (r + 1) * 384, 128:256]).astype(BF16)
        abuf[p.head, r, 0, 0:128] = a[0:128]
        abuf[p.head, r, p.zl, pl.ds(pl.multiple_of((1 - p.zl) * 128, 128), 128)] = a[128:256]
        abuf[p.head, r, 1, 128:256] = a[256:384]
        b = (oa[768 + r * 128 : 896 + r * 128, 0:128] / oa[768 + r * 128 : 896 + r * 128, 128:256]).astype(BF16)
        abuf[p.head, r, 1 - p.zl, pl.ds(pl.multiple_of(p.zl * 128, 128), 128)] = b

    ref = hid.at[0:448]
    remote(ref, ref, sk, h1, p.up).wait_recv()
    ref = wo.at[:, 1 - p.core]
    remote(ref, ref, sk, w2, p.partner).wait_recv()

    for ref in (
        qbuf.at[0:448], hid.at[0:448], kv.at[own, 0:448, 0:256], kv.at[0:15, :, 0:256], wo.at[0:7, 0], wo.at[:, p.core],
    ):
        pltpu.make_async_copy(ref, ref, sk).wait()


NS1 = 2
NS2 = 4
NC = 8
CW = 512
FFL = 896


def block_kernel(
    q, k, v, hid_in, gain, wo_hbm, gate_hbm, up_hbm, down_hbm, out,
    kv, qbuf, qs, oa, peak,
    abuf, rbuf, hid, wo, wgu, wd, oacc, acc, xg, sq, inner,
    zs, zr, keep, m1s, m1r, m2s, m2r,
    wsem, sk, kv1, q1, h1, w1, w2, ysem, zrecv, csem,
    s1, r1, s2, r2, s3, zsem, m1sem, m2sem,
):
    p = Place()
    barrier = pltpu.get_barrier_semaphore()
    peers = [p.plane(0, kx) for kx in (1, 2, 3)]
    peers += [p.plane(step, kx) for step in (1, 3) for kx in range(4)]
    peers += [p.up, p.down, p.across, p.partner]
    for device in peers:
        pl.semaphore_signal(barrier, inc=1, device_id=device, device_id_type=MESH)

    order = [p.here(0), p.other(0), p.here(3), p.here(1), p.here(2), p.other(3), p.other(1), p.other(2)]
    half = pl.ds(pl.multiple_of(p.core * 128, 128), 128)
    wo_copy = pltpu.make_async_copy(
        wo_hbm.at[half, columns(p.head, 512)], wo.at[p.head, p.core], wsem.at[16]
    )
    wd_copy = pltpu.make_async_copy(down_hbm, wd, wsem.at[17])

    def gate_copy(h):
        rows = pl.ds(pl.multiple_of(h * 512, 512), 512)
        return pltpu.make_async_copy(gate_hbm.at[rows], wgu.at[rows, 0:FFL], wsem.at[h])

    def up_copy(h):
        rows = pl.ds(pl.multiple_of(h * 512, 512), 512)
        return pltpu.make_async_copy(up_hbm.at[rows], wgu.at[rows, FFL : 2 * FFL], wsem.at[8 + h])

    wo_copy.start()
    for h in order:
        gate_copy(h).start()
        up_copy(h).start()
    wd_copy.start()

    me = p.here(0)
    c1 = 256 // NS1
    kv[:, :, 256:384] = jnp.ones((16, 512, 128), BF16)
    kv_rows = pl.ds(pl.multiple_of(p.head * 64, 64), 64)
    kv[p.blk, kv_rows, 0:128] = k[:, columns(p.head, 128)]
    kv[p.blk, kv_rows, 128:256] = v[:, columns(p.head, 128)]
    for part in range(2):
        rows = pl.ds(pl.multiple_of(part * 384 + p.x * 32, 32), 32)
        qbuf[rows, :] = q[part * 32 : (part + 1) * 32, columns(p.head, 256)]
        hid[rows, :] = hid_in[part * 32 : (part + 1) * 32, columns(p.head, 512)]
    pl.semaphore_wait(barrier, len(peers))
    attend_blocks(
        p, q, k, v, hid_in, wo_hbm, kv, qbuf, hid, wo, qs, oa, peak, abuf,
        sk, kv1, q1, h1, w1, w2, ysem, zrecv, csem, wo_copy,
    )

    def project(h, first):
        a = jnp.concatenate([abuf[h, s].reshape(512, c1) for s in range(NS1)], axis=1)
        w = wo[h].reshape(256, 512)
        for n in range(2):
            cols = slice(n * 256, (n + 1) * 256)
            part = jnp.dot(a, w[:, cols], preferred_element_type=F32)
            if first:
                oacc[:, cols] = hid[:, cols].astype(F32) + part
            else:
                oacc[:, cols] += part

    gather_rows(p, abuf, s1, r1, NS1, project)

    c2 = 512 // NS2
    for s in range(NS2):
        for half in range(2):
            rbuf[me, s, half] = oacc[half * 256 : (half + 1) * 256, s * c2 : (s + 1) * c2].astype(BF16)

    def expand(h, first):
        gate_copy(h).wait()
        up_copy(h).wait()
        total = None
        for s in range(NS2):
            r = rbuf[h, s].reshape(512, c2).astype(F32)
            g = gain[pl.ds(h * NS2 + s, 1), :]
            xg[:, s * c2 : (s + 1) * c2] = (r * g).astype(BF16)
            total = r * r if total is None else total + r * r
        if first:
            sq[...] = total
        else:
            sq[...] += total
        rows = pl.ds(pl.multiple_of(h * 512, 512), 512)
        for m in range(0, 512, 256):
            part = jnp.dot(xg[m : m + 256], wgu[rows, :], preferred_element_type=F32)
            if first:
                acc[m : m + 256] = part
            else:
                acc[m : m + 256] += part

    gather_rows(p, rbuf, s2, r2, NS2, expand)

    scale = lax.rsqrt(jnp.sum(sq[...], axis=1, keepdims=True) * (1.0 / 4096.0) + 1e-5)
    sq[...] = jnp.broadcast_to(scale, (512, 128))

    def activate(j, _):
        at = pl.multiple_of(j * 128, 128)
        u = acc[:, pl.ds(at, 128)] * sq[...]
        v = acc[:, pl.ds(pl.multiple_of(at + FFL, 128), 128)] * sq[...]
        inner[:, pl.ds(at, 128)] = (u / (1.0 + jnp.exp(-u)) * v).astype(BF16)
        return 0

    lax.fori_loop(0, 7, activate, 0)

    def z_copy(c, side):
        device = p.above if side == 0 else p.below
        return remote(zs.at[c, side], zr.at[c, 1 - side], s3, zsem.at[1 - side, c], device)

    def z_wait(c, side):
        remote(zr.at[c, side], zr.at[c, side], s3, zsem.at[side, c], p.right).wait_recv()

    def reduce_down(c, _):
        cols = pl.ds(pl.multiple_of(c * CW, CW), CW)
        low = jnp.dot(inner[0:256], wd[:, cols], preferred_element_type=F32)
        high = jnp.dot(inner[256:512], wd[:, cols], preferred_element_type=F32)
        keep[c, 0] = low[0:128]
        zs[c, 0] = low[128:256].astype(BF16)
        zs[c, 1] = high[0:128].astype(BF16)
        keep[c, 1] = high[128:256]
        z_copy(c, 0).start()
        z_copy(c, 1).start()
        return 0

    wd_copy.wait()
    lax.fori_loop(0, NC, reduce_down, 0)

    def slot(k):
        return pl.ds(pl.multiple_of(p.xs[k] * 32, 32), 32)

    def m1_copy(c, side):
        device = p.right if side == 0 else p.left
        return remote(m1s.at[c, side], m1r.at[c, side], s3, m1sem.at[side, c], device)

    def m2_copy(c, side):
        device = p.right if side == 0 else p.left
        return remote(m2s.at[c, side], m2r.at[c, side], s3, m2sem.at[side, c], device)

    def finish(t, _):
        @pl.when(t < NC)
        def _():
            c = t
            for side in range(2):
                z_wait(c, side)
                keep[c, side] += zr[c, side].astype(F32)
                m1s[c, side] = keep[c, side, slot(2), :].astype(BF16)
                m1_copy(c, side).start()

        @pl.when((t >= 1) & (t < NC + 1))
        def _():
            c = t - 1
            for side in range(2):
                m1_copy(c, side).wait_recv()
                k = 1 if side == 0 else 3
                for part in range(2):
                    q = keep[c, part, slot(k), :]
                    if part == side:
                        q = q + m1r[c, side].astype(F32)
                    m2s[c, side, part] = q.astype(BF16)
                m2_copy(c, side).start()

        @pl.when(t >= 2)
        def _():
            c = t - 2
            for side in range(2):
                m2_copy(c, side).wait_recv()
            for part in range(2):
                q = keep[c, part, slot(0), :] + m2r[c, 0, part].astype(F32) + m2r[c, 1, part].astype(F32)
                rows = pl.ds(pl.multiple_of(part * 128 + p.x * 32, 32), 32)
                for s in range(NS2):
                    r = rbuf[c, s, part, rows, :].astype(F32)
                    cols = pl.ds(pl.multiple_of(c * CW + s * c2, c2), c2)
                    out[part * 32 : (part + 1) * 32, cols] = (r + q[:, s * c2 : (s + 1) * c2]).astype(BF16)

        return 0

    lax.fori_loop(0, NC + 2, finish, 0)
    pltpu.make_async_copy(zs, zs, s3).wait()
    pltpu.make_async_copy(m1s, m1s, s3).wait()
    pltpu.make_async_copy(m2s, m2s, s3).wait()


def layer(q, k, v, hidden, gain, wo, gate, up, down):
    vmem = pl.BlockSpec(memory_space=pltpu.VMEM)
    hbm = pl.BlockSpec(memory_space=pl.ANY)
    dma = pltpu.SemaphoreType.DMA
    return pl.pallas_call(
        block_kernel,
        out_shape=jax.ShapeDtypeStruct((64, 4096), BF16),
        in_specs=[vmem, vmem, vmem, vmem, vmem, hbm, hbm, hbm, hbm],
        out_specs=vmem,
        scratch_shapes=[
            pltpu.VMEM((16, 512, 384), BF16),
            pltpu.VMEM((512, 256), BF16),
            pltpu.VMEM((1024, 128), BF16),
            pltpu.VMEM((1024, 256), F32),
            pltpu.VMEM((1024, 128), F32),
            pltpu.VMEM((8, NS1, 2, 256, 256 // NS1), BF16),
            pltpu.VMEM((8, NS2, 2, 256, 512 // NS2), BF16),
            pltpu.VMEM((512, 512), BF16),
            pltpu.VMEM((8, 2, 128, 512), BF16),
            pltpu.VMEM((4096, 2 * FFL), BF16),
            pltpu.VMEM((FFL, 4096), BF16),
            pltpu.VMEM((512, 512), F32),
            pltpu.VMEM((512, 2 * FFL), F32),
            pltpu.VMEM((512, 512), BF16),
            pltpu.VMEM((512, 128), F32),
            pltpu.VMEM((512, FFL), BF16),
            pltpu.VMEM((NC, 2, 128, CW), BF16),
            pltpu.VMEM((NC, 2, 128, CW), BF16),
            pltpu.VMEM((NC, 2, 128, CW), F32),
            pltpu.VMEM((NC, 2, 32, CW), BF16),
            pltpu.VMEM((NC, 2, 32, CW), BF16),
            pltpu.VMEM((NC, 2, 2, 32, CW), BF16),
            pltpu.VMEM((NC, 2, 2, 32, CW), BF16),
            dma((18,)),
            dma,
            dma((2,)),
            dma,
            dma,
            dma,
            dma,
            dma((2, 6)),
            dma((2,)),
            dma((8,)),
            dma,
            dma((14, NS1)),
            dma,
            dma((14, NS2)),
            dma,
            dma((2, NC)),
            dma((2, NC)),
            dma((2, NC)),
        ],
        compiler_params=pltpu.CompilerParams(
            collective_id=1, has_side_effects=True, vmem_limit_bytes=62 * 1024 * 1024
        ),
        cost_estimate=pl.CostEstimate(flops=16_500_000_000, bytes_accessed=24_000_000, transcendentals=0),
        name="layer",
    )(q, k, v, hidden, gain, wo, gate, up, down)


def local(
    hidden_in,
    queries,
    key_states,
    value_states,
    out_weight,
    norm_gain,
    gate_weight,
    up_weight,
    down_weight,
):
    return layer(
        queries, key_states, value_states, hidden_in, norm_gain.reshape(32, 128),
        out_weight, gate_weight, up_weight, down_weight,
    )


def solution(mesh):
    return jax.shard_map(
        local,
        mesh=mesh,
        in_specs=(
            P(("blk", "head"), None),
            P(("blk", "head"), None),
            P(("blk", "head"), None),
            P(("blk", "head"), None),
            P("head", None),
            P(),
            P(None, "head"),
            P(None, "head"),
            P("head", None),
        ),
        out_specs=P(("blk", "head"), None),
        check_vma=False,
    )
```

```python
import jax
import jax.numpy as jnp
from jax import lax
from jax.experimental import pallas as pl
from jax.experimental.pallas import tpu as pltpu
from jax.sharding import PartitionSpec as P

HEAD_DIM = 128
MESH = pl.DeviceIdType.MESH
F32 = jnp.float32
BF16 = jnp.bfloat16

negative_fill = -1e30


class Place:
    def __init__(self):
        self.head = lax.axis_index("head")
        self.blk = lax.axis_index("blk")
        self.x = lax.rem(self.head, 4)
        self.zl = self.head // 4
        self.zh = self.blk // 8
        self.yc = lax.rem(self.blk, 8)
        self.z = self.zh * 2 + self.zl
        self.xs = [lax.rem(self.x + k, 4) for k in range(4)]
        self.right = self.at_x(self.xs[1])
        self.left = self.at_x(self.xs[3])
        self.above = self.at_z(1)
        self.below = self.at_z(3)

        self.y = self.yc // 2
        self.core = lax.rem(self.blk, 2)
        self.chip = self.blk // 2
        self.up = self.at_y(1)
        self.down = self.at_y(3)
        self.partner = (self.head, self.blk + 1 - 2 * self.core)
        self.across = (self.head, (1 - self.zh) * 8 + self.yc)

    def at_y(self, step):
        return (self.head, self.zh * 8 + lax.rem(self.y + step, 4) * 2 + self.core)

    def plane(self, step, k):
        z = lax.rem(self.z + step, 4)
        return (lax.rem(z, 2) * 4 + self.xs[k], (z // 2) * 8 + self.yc)

    def chip_at(self, dz, k):
        return lax.rem(self.zh + dz, 2) * 4 + lax.rem(self.y + k, 4)

    def at_x(self, x):
        return (self.zl * 4 + x, self.blk)

    def at_z(self, step):
        z = lax.rem(self.z + step, 4)
        return (lax.rem(z, 2) * 4 + self.x, (z // 2) * 8 + self.yc)

    def here(self, k):
        return self.zl * 4 + self.xs[k]

    def other(self, k):
        return (1 - self.zl) * 4 + self.xs[k]


def remote(src, dst, send_sem, recv_sem, device):
    return pltpu.make_async_remote_copy(
        src_ref=src, dst_ref=dst, send_sem=send_sem, recv_sem=recv_sem,
        device_id=device, device_id_type=MESH,
    )


def gather_rows(p, buf, batch, send_sem, recv, steps, compute):
    def send(h, s, half, to_half, kind, device):
        src, dst = buf.at[h, s, batch, half], buf.at[h, s, batch, to_half]
        remote(src, dst, send_sem, recv.at[kind, s, batch], device).start()

    def wait(h, s, half, kind):
        ref = buf.at[h, s, batch, half]
        remote(ref, ref, send_sem, recv.at[kind, s, batch], p.right).wait_recv()

    me, left, right, far = p.here(0), p.here(3), p.here(1), p.here(2)
    for s in range(steps):
        send(me, s, 0, 0, 0, p.right)
        send(me, s, 1, 1, 4, p.left)
        send(me, s, 0, 1, 6, p.above)
        send(me, s, 1, 0, 10, p.below)
    yield
    for s in range(steps):
        send(me, s, 1, 1, 1, p.right)
        send(me, s, 0, 0, 3, p.left)
    yield
    compute(me, True)
    yield
    for s in range(steps):
        wait(left, s, 0, 0)
        send(left, s, 0, 0, 2, p.right)
        send(left, s, 0, 1, 7, p.above)
        wait(right, s, 1, 4)
        send(right, s, 1, 1, 5, p.left)
        send(right, s, 1, 0, 12, p.below)
    yield
    for s in range(steps):
        wait(p.other(0), s, 1, 6)
        wait(p.other(0), s, 0, 10)
    compute(p.other(0), False)
    yield
    for s in range(steps):
        wait(left, s, 1, 1)
        send(left, s, 1, 0, 11, p.below)
        wait(right, s, 0, 3)
        send(right, s, 0, 1, 8, p.above)
    yield
    compute(left, False)
    compute(right, False)
    yield
    for s in range(steps):
        wait(far, s, 0, 2)
        send(far, s, 0, 1, 9, p.above)
        wait(far, s, 1, 5)
        send(far, s, 1, 0, 13, p.below)
    yield
    compute(far, False)
    for k, up, down in ((3, 7, 11), (1, 8, 12), (2, 9, 13)):
        yield
        for s in range(steps):
            wait(p.other(k), s, 1, up)
            wait(p.other(k), s, 0, down)
        compute(p.other(k), False)


def advance(stages, count):
    for _ in range(count):
        next(stages, None)


def columns(h, width):
    return pl.ds(pl.multiple_of(h * width, width), width)


SCALE = HEAD_DIM ** (-0.5) * 1.4426950408889634


def batch_rows(group, b):
    return jnp.concatenate([group[at + b * 16 : at + b * 16 + 16] for at in range(0, 128, 32)], axis=0)


def attend_blocks(
    p, q, k, v, hid_in, wo_hbm, kv, qbuf, hid, wo, qs, oa, peak, abuf,
    sk, kv1, q1, h1, w1, w2, ysem, zrecv, csem, wown,
):
    own = p.blk
    mine = pl.ds(pl.multiple_of(p.x * 32, 32), 32)

    def rows_of(g):
        return pl.ds(pl.multiple_of(g * 128 + p.x * 32, 32), 32)

    kv_rows = pl.ds(pl.multiple_of(p.head * 64, 64), 64)

    def send_kv(device, sem):
        h = device[0]
        remote(k.at[:, columns(h, 128)], kv.at[own, kv_rows, 0:128], sk, sem, device).start()
        remote(v.at[:, columns(h, 128)], kv.at[own, kv_rows, 128:256], sk, sem, device).start()

    def send_rows(src, dst, sem, width, part, g, device):
        at = columns(device[0], width)
        remote(src.at[part * 32 : (part + 1) * 32, at], dst.at[rows_of(g), :], sk, sem, device).start()

    near = 1 - 2 * p.zl + 4
    for kx in range(4):
        send_kv(p.plane(near, kx), kv1.at[1])
        if kx:
            send_kv(p.plane(0, kx), kv1.at[0])
    for kx in range(4):
        send_rows(q, qbuf, q1, 256, 0, 2, p.plane(1, kx))
        send_rows(q, qbuf, q1, 256, 1, 1, p.plane(3, kx))
        if kx:
            send_rows(q, qbuf, q1, 256, 0, 0, p.plane(0, kx))
            send_rows(q, qbuf, q1, 256, 1, 3, p.plane(0, kx))

    def block(dz, kk, other=False):
        core = 1 - p.core if other else p.core
        return p.chip_at(dz, kk) * 2 + core

    def piece(dz, kk, part):
        return kv.at[block(dz, kk), part * 256 : (part + 1) * 256, 0:256]

    def send_piece(dz, kk, part, sem, device):
        remote(piece(dz, kk, part), piece(dz, kk, part), sk, sem, device).start()

    def wait_piece(dz, kk, part, sem):
        remote(piece(dz, kk, part), piece(dz, kk, part), sk, sem, p.up).wait_recv()

    def share(dz, kk, sem):
        ref = kv.at[block(dz, kk), :, 0:256]
        remote(ref, ref, sk, sem, p.partner).start()

    def wait_shared(dz, kk, sem):
        ref = kv.at[block(dz, kk, True), :, 0:256]
        remote(ref, ref, sk, sem, p.partner).wait_recv()

    def send_both(dz):
        i = 3 * dz
        send_piece(dz, 0, 0, ysem.at[0, i], p.up)
        send_piece(dz, 0, 1, ysem.at[1, i + 1], p.down)
        send_piece(dz, 0, 1, ysem.at[0, i + 1], p.up)
        send_piece(dz, 0, 0, ysem.at[1, i], p.down)

    def forward(dz):
        i = 3 * dz
        wait_piece(dz, 3, 0, ysem.at[0, i])
        send_piece(dz, 3, 0, ysem.at[0, i + 2], p.up)
        wait_piece(dz, 1, 1, ysem.at[1, i + 1])
        send_piece(dz, 1, 1, ysem.at[1, i + 2], p.down)

    def near_done(dz):
        i = 3 * dz
        wait_piece(dz, 3, 1, ysem.at[0, i + 1])
        share(dz, 3, csem.at[4 * dz + 3])
        wait_piece(dz, 1, 0, ysem.at[1, i])
        share(dz, 1, csem.at[4 * dz + 1])

    def far_done(dz):
        i = 3 * dz
        wait_piece(dz, 2, 0, ysem.at[0, i + 2])
        wait_piece(dz, 2, 1, ysem.at[1, i + 2])
        share(dz, 2, csem.at[4 * dz + 2])

    def own_rows(part):
        return kv.at[own, pl.ds(pl.multiple_of(part * 256, 256), 256), 0:256]

    for order, (part, count) in enumerate(((p.zl, 192), (1 - p.zl, 256))):
        ref = kv.at[own, 0:count, 0:256]
        remote(ref, ref, sk, kv1.at[order], p.up).wait_recv()
        ref = own_rows(part)
        remote(ref, ref, sk, ysem.at[0, part], p.up).start()
        remote(ref, ref, sk, ysem.at[1, part], p.down).start()
        remote(ref, ref, sk, zrecv.at[part], p.across).start()
    share(0, 0, csem.at[0])
    for kx in range(4):
        send_rows(hid_in, hid, h1, 512, 0, 2, p.plane(1, kx))
        send_rows(hid_in, hid, h1, 512, 1, 1, p.plane(3, kx))
        if kx:
            send_rows(hid_in, hid, h1, 512, 0, 0, p.plane(0, kx))
            send_rows(hid_in, hid, h1, 512, 1, 3, p.plane(0, kx))

    ref = qbuf.at[0:448]
    remote(ref, ref, sk, q1, p.up).wait_recv()
    same = 1 + p.zl
    for r in range(2):
        cols = slice(r * 128, (r + 1) * 128)
        qs[r * 384 : r * 384 + 128] = qbuf[0:128, cols]
        qs[r * 384 + 128 : r * 384 + 256] = qbuf[pl.ds(pl.multiple_of(same * 128, 128), 128), cols]
        qs[r * 384 + 256 : r * 384 + 384] = qbuf[384:512, cols]
        qs[768 + r * 128 : 896 + r * 128] = qbuf[pl.ds(pl.multiple_of((3 - same) * 128, 128), 128), cols]
    oa[...] = jnp.zeros_like(oa)
    peak[...] = jnp.full_like(peak, negative_fill)

    def absorb(start, count, sub, chip, row_pos):
        keys = kv[pl.ds(chip * 2, 2), :, 0:128].reshape(1024, 128)
        values = kv[pl.ds(chip * 2, 2), :, 128:384].reshape(1024, 256)
        tiles = [slice(start + at, start + at + sub) for at in range(0, count, sub)]
        asked = [qs[rows] for rows in tiles]
        olds = [peak[rows] for rows in tiles]
        sums = [oa[rows] for rows in tiles]

        def score(t):
            s = lax.dot_general(asked[t], keys, (((1,), (1,)), ((), ())), preferred_element_type=F32)
            if row_pos is not None:
                i = t * sub + lax.broadcasted_iota(jnp.int32, (sub, 1), 0)
                key_pos = chip * 1024 + lax.broadcasted_iota(jnp.int32, (sub, 1024), 1)
                s = jnp.where(key_pos <= row_pos(i), s, negative_fill)
            return [s[:, at : at + 128] for at in range(0, 1024, 128)]

        news, ends = [], []
        coming = score(0)
        for t, old in enumerate(olds):
            s = coming
            top = s[0]
            for piece in s[1:]:
                top = jnp.maximum(top, piece)
            if t + 1 < len(tiles):
                coming = score(t + 1)
            new = jnp.maximum(old, jnp.max(top, axis=1, keepdims=True))
            w = jnp.concatenate([jnp.exp2((piece - new) * SCALE).astype(BF16) for piece in s], axis=1)
            shrink = jnp.exp2((old - new) * SCALE)
            part = jnp.dot(w, values, preferred_element_type=F32)
            news.append(new)
            ends.append(sums[t] * jnp.concatenate([shrink, shrink], axis=1) + part)
        for rows, new, end in zip(tiles, news, ends):
            peak[rows] = new
            oa[rows] = end

    def spread(i):
        return ((i & 96) << 1) + (i & 31)

    def pos_a(i):
        seg = lax.rem(i >> 7, 3)
        shift = jnp.where(seg == 1, (1 - p.zl) * 288, p.zl * 256 + (seg >> 1) * 32)
        return own * 512 + spread(i & 127) + shift

    chip_b = (1 - p.zh) * 4 + p.y

    def pos_b(i):
        return (chip_b * 2 + p.core) * 512 + spread(i & 127) + (1 - p.zl) * 256 + p.zl * 32

    def absorb_a(chip, masked):
        absorb(0, 768, 256, chip, pos_a if masked else None)

    def absorb_b(chip, masked):
        absorb(768, 256, 128, chip, pos_b if masked else None)

    def seen(chip):
        @pl.when(chip < p.chip)
        def _():
            absorb_a(chip, False)

        @pl.when(chip < chip_b)
        def _():
            absorb_b(chip, False)

    wait_shared(0, 0, csem.at[0])
    absorb_a(p.chip, True)

    @pl.when(p.chip < chip_b)
    def _():
        absorb_b(p.chip, False)

    forward(0)
    near_done(0)
    for part in range(2):
        wait_piece(1, 0, part, zrecv.at[part])
    send_both(1)
    share(1, 0, csem.at[4])
    half = pl.ds(pl.multiple_of(p.core * 128, 128), 128)
    for kx in range(4):
        if kx:
            device = p.plane(0, kx)
            remote(
                wo_hbm.at[half, columns(device[0], 512)], wo.at[p.head, p.core], sk, w1, device
            ).start()
        for part in range(2):
            device = p.plane(1 + 2 * part, kx)
            rows = pl.ds(pl.multiple_of(p.core * 128 + part * 64, 64), 64)
            remote(
                wo_hbm.at[rows, columns(device[0], 512)],
                wo.at[p.head, p.core, part * 64 : (part + 1) * 64], sk, w1, device,
            ).start()
    wait_shared(0, 3, csem.at[3])
    wait_shared(0, 1, csem.at[1])

    def near_step(t, _):
        seen(p.chip_at(0, 3 - 2 * t))
        return 0

    lax.fori_loop(0, 2, near_step, 0)
    far_done(0)
    forward(1)
    wait_shared(1, 0, csem.at[4])
    chip = p.chip_at(1, 0)

    @pl.when(chip < p.chip)
    def _():
        absorb_a(chip, False)

    absorb_b(chip, True)
    near_done(1)
    wait_shared(0, 2, csem.at[2])
    wait_shared(1, 3, csem.at[7])
    wait_shared(1, 1, csem.at[5])

    def late_step(t, _):
        @pl.when(t == 3)
        def _():
            wown.wait()
            ref = wo.at[0:7, 0]
            remote(ref, ref, sk, w1, p.up).wait_recv()
            ref = wo.at[:, p.core]
            remote(ref, ref, sk, w2, p.partner).start()
            far_done(1)
            wait_shared(1, 2, csem.at[6])

        seen(p.chip_at(jnp.minimum(t, 1), 2 + t - 3 * (t // 2)))
        return 0

    lax.fori_loop(0, 4, late_step, 0)

    for r in range(2):
        cols = slice(r * 128, (r + 1) * 128)
        a = (oa[r * 384 : (r + 1) * 384, 0:128] / oa[r * 384 : (r + 1) * 384, 128:256]).astype(BF16)
        o = (oa[768 + r * 128 : 896 + r * 128, 0:128] / oa[768 + r * 128 : 896 + r * 128, 128:256]).astype(BF16)
        for b in range(2):
            abuf[p.head, 0, b, 0, 0:64, cols] = batch_rows(a[0:128], b)
            abuf[p.head, 0, b, p.zl, pl.ds(pl.multiple_of((1 - p.zl) * 64, 64), 64), cols] = batch_rows(a[128:256], b)
            abuf[p.head, 0, b, 1, 64:128, cols] = batch_rows(a[256:384], b)
            abuf[p.head, 0, b, 1 - p.zl, pl.ds(pl.multiple_of(p.zl * 64, 64), 64), cols] = batch_rows(o, b)

    ref = hid.at[0:448]
    remote(ref, ref, sk, h1, p.up).wait_recv()
    ref = wo.at[:, 1 - p.core]
    remote(ref, ref, sk, w2, p.partner).wait_recv()

    for ref in (
        qbuf.at[0:448], hid.at[0:448], kv.at[own, 0:448, 0:256], kv.at[0:15, :, 0:256], wo.at[0:7, 0], wo.at[:, p.core],
    ):
        pltpu.make_async_copy(ref, ref, sk).wait()


NS1 = 1
NS2 = 2
NC = 8
CW = 512
FFL = 896


def block_kernel(
    q_hbm, k_hbm, v_hbm, hid_hbm, gain_hbm, wo_hbm, gate_hbm, up_hbm, down_hbm, out,
    q, k, v, hid_in, gain, kv, qbuf, qs, oa, peak,
    abuf, rbuf, hid, wo, wgu, wd, oacc, acc, xg, sq, inner,
    zs, zr, keep, m1s, m1r, m2s, m2r,
    insem, wsem, sk, kv1, q1, h1, w1, w2, ysem, zrecv, csem,
    s1, r1, s2, r2, s3, zsem, m1sem, m2sem,
):
    p = Place()
    barrier = pltpu.get_barrier_semaphore()
    peers = [p.plane(0, kx) for kx in (1, 2, 3)]
    peers += [p.plane(step, kx) for step in (1, 3) for kx in range(4)]
    peers += [p.up, p.down, p.across, p.partner]
    for device in peers:
        pl.semaphore_signal(barrier, inc=1, device_id=device, device_id_type=MESH)
    loads = [
        pltpu.make_async_copy(src, dst, insem.at[i])
        for i, (src, dst) in enumerate(((k_hbm, k), (v_hbm, v), (q_hbm, q), (hid_hbm, hid_in), (gain_hbm, gain)))
    ]
    for load in loads:
        load.start()

    order = [p.here(0), p.other(0), p.here(3), p.here(1), p.here(2), p.other(3), p.other(1), p.other(2)]
    half = pl.ds(pl.multiple_of(p.core * 128, 128), 128)
    wo_copy = pltpu.make_async_copy(
        wo_hbm.at[half, columns(p.head, 512)], wo.at[p.head, p.core], wsem.at[16]
    )
    wd_copy = pltpu.make_async_copy(down_hbm, wd, wsem.at[17])

    def gate_copy(h):
        rows = pl.ds(pl.multiple_of(h * 512, 512), 512)
        return pltpu.make_async_copy(gate_hbm.at[rows], wgu.at[rows, 0:FFL], wsem.at[h])

    def up_copy(h):
        rows = pl.ds(pl.multiple_of(h * 512, 512), 512)
        return pltpu.make_async_copy(up_hbm.at[rows], wgu.at[rows, FFL : 2 * FFL], wsem.at[8 + h])

    wo_copy.start()
    for h in order:
        gate_copy(h).start()
        up_copy(h).start()
    wd_copy.start()

    me = p.here(0)
    kv[:, :, 256:384] = jnp.ones((16, 512, 128), BF16)
    kv_rows = pl.ds(pl.multiple_of(p.head * 64, 64), 64)
    for load in loads:
        load.wait()
    kv[p.blk, kv_rows, 0:128] = k[:, columns(p.head, 128)]
    kv[p.blk, kv_rows, 128:256] = v[:, columns(p.head, 128)]
    for part in range(2):
        rows = pl.ds(pl.multiple_of(part * 384 + p.x * 32, 32), 32)
        qbuf[rows, :] = q[part * 32 : (part + 1) * 32, columns(p.head, 256)]
        hid[rows, :] = hid_in[part * 32 : (part + 1) * 32, columns(p.head, 512)]
    pl.semaphore_wait(barrier, len(peers))
    attend_blocks(
        p, q, k, v, hid_in, wo_hbm, kv, qbuf, hid, wo, qs, oa, peak, abuf,
        sk, kv1, q1, h1, w1, w2, ysem, zrecv, csem, wo_copy,
    )

    c2 = 512 // NS2

    def project(b):
        rows = slice(b * 256, (b + 1) * 256)

        def add(h, first):
            part = jnp.dot(abuf[h, 0, b].reshape(256, 256), wo[h].reshape(256, 512), preferred_element_type=F32)
            if first:
                held = jnp.concatenate([batch_rows(hid[g * 128 : (g + 1) * 128], b) for g in range(4)], axis=0)
                oacc[rows] = held.astype(F32) + part
            else:
                oacc[rows] += part

        return add

    def residual(b):
        for s in range(NS2):
            for half in range(2):
                at = b * 256 + half * 128
                rbuf[me, s, b, half] = oacc[at : at + 128, s * c2 : (s + 1) * c2].astype(BF16)

    def expand(b):
        out_rows = slice(b * 256, (b + 1) * 256)

        def add(h, first):
            if b == 0:
                gate_copy(h).wait()
                up_copy(h).wait()
            total = None
            for s in range(NS2):
                r = rbuf[h, s, b].reshape(256, c2).astype(F32)
                for j in range(c2 // 128):
                    piece = r[:, j * 128 : (j + 1) * 128]
                    g = gain[pl.ds(h * 4 + s * (c2 // 128) + j, 1), :]
                    at = s * c2 + j * 128
                    xg[b, :, at : at + 128] = (piece * g).astype(BF16)
                    total = piece * piece if total is None else total + piece * piece
            rows = pl.ds(pl.multiple_of(h * 512, 512), 512)
            part = jnp.dot(xg[b], wgu[rows, :], preferred_element_type=F32)
            if first:
                sq[out_rows] = total
                acc[out_rows] = part
            else:
                sq[out_rows] += total
                acc[out_rows] += part

        return add

    def activate(b):
        rows = slice(b * 256, (b + 1) * 256)
        scale = lax.rsqrt(jnp.sum(sq[rows], axis=1, keepdims=True) * (1.0 / 4096.0) + 1e-5)
        sq[rows] = jnp.broadcast_to(scale, (256, 128))

        def tile(j, _):
            at = pl.multiple_of(j * 128, 128)
            u = acc[rows, pl.ds(at, 128)] * sq[rows]
            v = acc[rows, pl.ds(pl.multiple_of(at + FFL, 128), 128)] * sq[rows]
            inner[rows, pl.ds(at, 128)] = (u / (1.0 + jnp.exp(-u)) * v).astype(BF16)
            return 0

        lax.fori_loop(0, 7, tile, 0)

    def reduce_down(b):
        def one(c, _):
            cols = pl.ds(pl.multiple_of(c * CW, CW), CW)
            part = jnp.dot(inner[b * 256 : (b + 1) * 256], wd[:, cols], preferred_element_type=F32)
            keep[b, c, 0] = part[0:64]
            zs[b, c, 0] = part[64:128].astype(BF16)
            zs[b, c, 1] = part[128:192].astype(BF16)
            keep[b, c, 1] = part[192:256]
            remote(zs.at[b, c, 0], zr.at[b, c, 1], s3, zsem.at[b, 1, c], p.above).start()
            remote(zs.at[b, c, 1], zr.at[b, c, 0], s3, zsem.at[b, 0, c], p.below).start()
            return 0

        lax.fori_loop(0, NC, one, 0)

    def slot(k):
        return pl.ds(pl.multiple_of(p.xs[k] * 16, 16), 16)

    def m1_copy(b, c, side):
        device = p.right if side == 0 else p.left
        return remote(m1s.at[b, c, side], m1r.at[b, c, side], s3, m1sem.at[b, side, c], device)

    def m2_copy(b, c, side):
        device = p.right if side == 0 else p.left
        return remote(m2s.at[b, c, side], m2r.at[b, c, side], s3, m2sem.at[b, side, c], device)

    def finish(b):
        def one(t, _):
            @pl.when(t < NC)
            def _():
                c = t
                for side in range(2):
                    ref = zr.at[b, c, side]
                    remote(ref, ref, s3, zsem.at[b, side, c], p.right).wait_recv()
                    keep[b, c, side] += zr[b, c, side].astype(F32)
                    m1s[b, c, side] = keep[b, c, side, slot(2), :].astype(BF16)
                    m1_copy(b, c, side).start()

            @pl.when((t >= 1) & (t < NC + 1))
            def _():
                c = t - 1
                for side in range(2):
                    m1_copy(b, c, side).wait_recv()
                    k = 1 if side == 0 else 3
                    for part in range(2):
                        q = keep[b, c, part, slot(k), :]
                        if part == side:
                            q = q + m1r[b, c, side].astype(F32)
                        m2s[b, c, side, part] = q.astype(BF16)
                    m2_copy(b, c, side).start()

            @pl.when(t >= 2)
            def _():
                c = t - 2
                for side in range(2):
                    m2_copy(b, c, side).wait_recv()
                for part in range(2):
                    q = keep[b, c, part, slot(0), :] + m2r[b, c, 0, part].astype(F32) + m2r[b, c, 1, part].astype(F32)
                    rows = pl.ds(pl.multiple_of(part * 64 + p.x * 16, 16), 16)
                    for s in range(NS2):
                        r = rbuf[c, s, b, part, rows, :].astype(F32)
                        cols = pl.ds(pl.multiple_of(c * CW + s * c2, c2), c2)
                        at = part * 32 + b * 16
                        out[at : at + 16, cols] = (r + q[:, s * c2 : (s + 1) * c2]).astype(BF16)

            return 0

        lax.fori_loop(0, NC + 2, one, 0)

    ga = [gather_rows(p, abuf, b, s1, r1, NS1, project(b)) for b in range(2)]
    gr = [gather_rows(p, rbuf, b, s2, r2, NS2, expand(b)) for b in range(2)]
    advance(ga[0], 2)
    advance(ga[1], 1)
    advance(ga[0], 2)
    advance(ga[1], 2)
    advance(ga[0], 3)
    advance(ga[1], 1)
    advance(ga[0], 1)
    advance(ga[1], 4)
    advance(ga[0], 4)
    residual(0)
    advance(gr[0], 3)
    advance(ga[1], 4)
    residual(1)
    advance(gr[0], 1)
    advance(gr[1], 1)
    advance(gr[0], 3)
    advance(gr[1], 2)
    advance(gr[0], 1)
    advance(gr[1], 1)
    advance(gr[0], 2)
    advance(gr[1], 2)
    advance(gr[0], 2)
    activate(0)
    advance(gr[1], 2)
    wd_copy.wait()
    reduce_down(0)
    advance(gr[1], 4)
    activate(1)
    reduce_down(1)
    finish(0)
    finish(1)
    pltpu.make_async_copy(abuf.at[0:7], abuf.at[0:7], s1).wait()
    pltpu.make_async_copy(rbuf.at[0:7], rbuf.at[0:7], s2).wait()
    for ref in (zs, m1s, m2s):
        pltpu.make_async_copy(ref, ref, s3).wait()


def layer(q, k, v, hidden, gain, wo, gate, up, down):
    vmem = pl.BlockSpec(memory_space=pltpu.VMEM)
    hbm = pl.BlockSpec(memory_space=pl.ANY)
    dma = pltpu.SemaphoreType.DMA
    return pl.pallas_call(
        block_kernel,
        out_shape=pltpu.VMEM((64, 4096), BF16),
        in_specs=[hbm] * 9,
        out_specs=vmem,
        scratch_shapes=[
            pltpu.VMEM((64, 2048), BF16),
            pltpu.VMEM((64, 1024), BF16),
            pltpu.VMEM((64, 1024), BF16),
            pltpu.VMEM((64, 4096), BF16),
            pltpu.VMEM((32, 128), F32),
            pltpu.VMEM((16, 512, 384), BF16),
            pltpu.VMEM((512, 256), BF16),
            pltpu.VMEM((1024, 128), BF16),
            pltpu.VMEM((1024, 256), F32),
            pltpu.VMEM((1024, 128), F32),
            pltpu.VMEM((8, NS1, 2, 2, 128, 256 // NS1), BF16),
            pltpu.VMEM((8, NS2, 2, 2, 128, 512 // NS2), BF16),
            pltpu.VMEM((512, 512), BF16),
            pltpu.VMEM((8, 2, 128, 512), BF16),
            pltpu.VMEM((4096, 2 * FFL), BF16),
            pltpu.VMEM((FFL, 4096), BF16),
            pltpu.VMEM((512, 512), F32),
            pltpu.VMEM((512, 2 * FFL), F32),
            pltpu.VMEM((2, 256, 512), BF16),
            pltpu.VMEM((512, 128), F32),
            pltpu.VMEM((512, FFL), BF16),
            pltpu.VMEM((2, NC, 2, 64, CW), BF16),
            pltpu.VMEM((2, NC, 2, 64, CW), BF16),
            pltpu.VMEM((2, NC, 2, 64, CW), F32),
            pltpu.VMEM((2, NC, 2, 16, CW), BF16),
            pltpu.VMEM((2, NC, 2, 16, CW), BF16),
            pltpu.VMEM((2, NC, 2, 2, 16, CW), BF16),
            pltpu.VMEM((2, NC, 2, 2, 16, CW), BF16),
            dma((5,)),
            dma((18,)),
            dma,
            dma((2,)),
            dma,
            dma,
            dma,
            dma,
            dma((2, 6)),
            dma((2,)),
            dma((8,)),
            dma,
            dma((14, NS1, 2)),
            dma,
            dma((14, NS2, 2)),
            dma,
            dma((2, 2, NC)),
            dma((2, 2, NC)),
            dma((2, 2, NC)),
        ],
        compiler_params=pltpu.CompilerParams(
            collective_id=1, has_side_effects=True, vmem_limit_bytes=62 * 1024 * 1024
        ),
        cost_estimate=pl.CostEstimate(flops=16_500_000_000, bytes_accessed=24_000_000, transcendentals=0),
        name="layer",
    )(q, k, v, hidden, gain, wo, gate, up, down)


def local(
    hidden_in,
    queries,
    key_states,
    value_states,
    out_weight,
    norm_gain,
    gate_weight,
    up_weight,
    down_weight,
):
    return layer(
        queries, key_states, value_states, hidden_in, norm_gain.reshape(32, 128),
        out_weight, gate_weight, up_weight, down_weight,
    )


def solution(mesh):
    return jax.shard_map(
        local,
        mesh=mesh,
        in_specs=(
            P(("blk", "head"), None),
            P(("blk", "head"), None),
            P(("blk", "head"), None),
            P(("blk", "head"), None),
            P("head", None),
            P(),
            P(None, "head"),
            P(None, "head"),
            P("head", None),
        ),
        out_specs=P(("blk", "head"), None),
        check_vma=False,
    )
```

```python
import jax
import jax.numpy as jnp
from jax import lax
from jax.experimental import pallas as pl
from jax.experimental.pallas import tpu as pltpu
from jax.sharding import PartitionSpec as P

HEAD_DIM = 128
MESH = pl.DeviceIdType.MESH
F32 = jnp.float32
BF16 = jnp.bfloat16

negative_fill = -1e30


class Place:
    def __init__(self):
        self.head = lax.axis_index("head")
        self.blk = lax.axis_index("blk")
        self.x = lax.rem(self.head, 4)
        self.zl = self.head // 4
        self.zh = self.blk // 8
        self.yc = lax.rem(self.blk, 8)
        self.z = self.zh * 2 + self.zl
        self.xs = [lax.rem(self.x + k, 4) for k in range(4)]
        self.right = self.at_x(self.xs[1])
        self.left = self.at_x(self.xs[3])
        self.above = self.at_z(1)
        self.below = self.at_z(3)

        self.y = self.yc // 2
        self.core = lax.rem(self.blk, 2)
        self.chip = self.blk // 2
        self.up = self.at_y(1)
        self.down = self.at_y(3)
        self.partner = (self.head, self.blk + 1 - 2 * self.core)
        self.across = (self.head, (1 - self.zh) * 8 + self.yc)

    def at_y(self, step):
        return (self.head, self.zh * 8 + lax.rem(self.y + step, 4) * 2 + self.core)

    def plane(self, step, k):
        z = lax.rem(self.z + step, 4)
        return (lax.rem(z, 2) * 4 + self.xs[k], (z // 2) * 8 + self.yc)

    def chip_at(self, dz, k):
        return lax.rem(self.zh + dz, 2) * 4 + lax.rem(self.y + k, 4)

    def at_x(self, x):
        return (self.zl * 4 + x, self.blk)

    def at_z(self, step):
        z = lax.rem(self.z + step, 4)
        return (lax.rem(z, 2) * 4 + self.x, (z // 2) * 8 + self.yc)

    def here(self, k):
        return self.zl * 4 + self.xs[k]

    def other(self, k):
        return (1 - self.zl) * 4 + self.xs[k]


def remote(src, dst, send_sem, recv_sem, device):
    return pltpu.make_async_remote_copy(
        src_ref=src, dst_ref=dst, send_sem=send_sem, recv_sem=recv_sem,
        device_id=device, device_id_type=MESH,
    )


def gather_rows(p, buf, batch, send_sem, recv, steps, compute, across_first=()):
    def send(h, s, half, to_half, kind, device):
        src, dst = buf.at[h, s, batch, half], buf.at[h, s, batch, to_half]
        remote(src, dst, send_sem, recv.at[kind, s, batch], device).start()

    def wait(h, s, half, kind):
        ref = buf.at[h, s, batch, half]
        remote(ref, ref, send_sem, recv.at[kind, s, batch], p.right).wait_recv()

    me, left, right, far = p.here(0), p.here(3), p.here(1), p.here(2)
    twin, twin_left, twin_right, twin_far = p.other(0), p.other(3), p.other(1), p.other(2)
    along_first = [s for s in range(steps) if s not in across_first]
    for s in range(steps):
        send(me, s, 0, 0, 0, p.right)
        send(me, s, 1, 1, 4, p.left)
        send(me, s, 0, 1, 6, p.above)
        send(me, s, 1, 0, 10, p.below)
    yield
    compute(me, True)
    yield
    for s in range(steps):
        wait(left, s, 0, 0)
        send(left, s, 0, 0, 2, p.right)
        wait(right, s, 1, 4)
        send(right, s, 1, 1, 5, p.left)
        if s in along_first:
            send(left, s, 0, 1, 7, p.above)
            send(right, s, 1, 0, 12, p.below)
    yield
    for s in range(steps):
        send(me, s, 1, 1, 1, p.right)
        send(me, s, 0, 0, 3, p.left)
    yield
    for s in range(steps):
        wait(twin, s, 1, 6)
        wait(twin, s, 0, 10)
        if s in across_first:
            send(twin, s, 0, 0, 11, p.right)
            send(twin, s, 1, 1, 8, p.left)
            send(twin, s, 1, 1, 7, p.right)
            send(twin, s, 0, 0, 12, p.left)
    compute(twin, False)
    yield
    for s in range(steps):
        wait(far, s, 0, 2)
        wait(far, s, 1, 5)
        if s in along_first:
            send(far, s, 0, 1, 9, p.above)
            send(far, s, 1, 0, 13, p.below)
    yield
    for s in range(steps):
        wait(left, s, 1, 1)
        wait(right, s, 0, 3)
        if s in along_first:
            send(left, s, 1, 0, 11, p.below)
            send(right, s, 0, 1, 8, p.above)
    for s in across_first:
        wait(twin_left, s, 0, 11)
        send(twin_left, s, 0, 0, 13, p.right)
        wait(twin_right, s, 1, 8)
        send(twin_right, s, 1, 1, 9, p.left)
    yield
    compute(left, False)
    compute(right, False)
    compute(far, False)
    yield
    for s in range(steps):
        wait(twin_left, s, 1, 7)
        if s in along_first:
            wait(twin_left, s, 0, 11)
    compute(twin_left, False)
    yield
    for s in range(steps):
        wait(twin_right, s, 0, 12)
        if s in along_first:
            wait(twin_right, s, 1, 8)
    compute(twin_right, False)
    yield
    for s in range(steps):
        wait(twin_far, s, 1, 9)
        wait(twin_far, s, 0, 13)
    compute(twin_far, False)


def advance(stages, count):
    for _ in range(count):
        next(stages, None)


def columns(h, width):
    return pl.ds(pl.multiple_of(h * width, width), width)


SCALE = HEAD_DIM ** (-0.5) * 1.4426950408889634


def batch_rows(group, b):
    return jnp.concatenate([group[at + b * 16 : at + b * 16 + 16] for at in range(0, 128, 32)], axis=0)


def attend_blocks(
    p, q, k, v, hid_in, wo_hbm, kv, qbuf, hid, wo, qs, oa, peak, abuf,
    sk, kv1, q1, h1, w1, w2, ysem, zrecv, csem, wown,
):
    own = p.blk
    mine = pl.ds(pl.multiple_of(p.x * 32, 32), 32)

    def rows_of(g):
        return pl.ds(pl.multiple_of(g * 128 + p.x * 32, 32), 32)

    kv_rows = pl.ds(pl.multiple_of(p.head * 64, 64), 64)

    def send_kv(device, sem):
        h = device[0]
        remote(k.at[:, columns(h, 128)], kv.at[own, kv_rows, 0:128], sk, sem, device).start()
        remote(v.at[:, columns(h, 128)], kv.at[own, kv_rows, 128:256], sk, sem, device).start()

    def send_rows(src, dst, sem, width, part, g, device):
        at = columns(device[0], width)
        remote(src.at[part * 32 : (part + 1) * 32, at], dst.at[rows_of(g), :], sk, sem, device).start()

    near = 1 - 2 * p.zl + 4
    for kx in range(4):
        send_kv(p.plane(near, kx), kv1.at[1])
        if kx:
            send_kv(p.plane(0, kx), kv1.at[0])
    for kx in range(4):
        send_rows(q, qbuf, q1, 256, 0, 2, p.plane(1, kx))
        send_rows(q, qbuf, q1, 256, 1, 1, p.plane(3, kx))
        if kx:
            send_rows(q, qbuf, q1, 256, 0, 0, p.plane(0, kx))
            send_rows(q, qbuf, q1, 256, 1, 3, p.plane(0, kx))

    def block(dz, kk, other=False):
        core = 1 - p.core if other else p.core
        return p.chip_at(dz, kk) * 2 + core

    def piece(dz, kk, part):
        return kv.at[block(dz, kk), part * 256 : (part + 1) * 256, 0:256]

    def send_piece(dz, kk, part, sem, device):
        remote(piece(dz, kk, part), piece(dz, kk, part), sk, sem, device).start()

    def wait_piece(dz, kk, part, sem):
        remote(piece(dz, kk, part), piece(dz, kk, part), sk, sem, p.up).wait_recv()

    def share(dz, kk, sem):
        ref = kv.at[block(dz, kk), :, 0:256]
        remote(ref, ref, sk, sem, p.partner).start()

    def wait_shared(dz, kk, sem):
        ref = kv.at[block(dz, kk, True), :, 0:256]
        remote(ref, ref, sk, sem, p.partner).wait_recv()

    def forward(dz):
        i = 3 * dz
        wait_piece(dz, 3, 0, ysem.at[0, i])
        send_piece(dz, 3, 0, ysem.at[0, i + 2], p.up)
        wait_piece(dz, 1, 1, ysem.at[1, i + 1])
        send_piece(dz, 1, 1, ysem.at[1, i + 2], p.down)

    def near_done(dz):
        i = 3 * dz
        wait_piece(dz, 3, 1, ysem.at[0, i + 1])
        share(dz, 3, csem.at[4 * dz + 3])
        wait_piece(dz, 1, 0, ysem.at[1, i])
        share(dz, 1, csem.at[4 * dz + 1])

    def far_done(dz):
        i = 3 * dz
        wait_piece(dz, 2, 0, ysem.at[0, i + 2])
        wait_piece(dz, 2, 1, ysem.at[1, i + 2])
        share(dz, 2, csem.at[4 * dz + 2])

    def own_rows(part):
        return kv.at[own, pl.ds(pl.multiple_of(part * 256, 256), 256), 0:256]

    for order, (part, count) in enumerate(((p.zl, 192), (1 - p.zl, 256))):
        ref = kv.at[own, 0:count, 0:256]
        remote(ref, ref, sk, kv1.at[order], p.up).wait_recv()
        ref = own_rows(part)
        remote(ref, ref, sk, ysem.at[0, part], p.up).start()
        remote(ref, ref, sk, ysem.at[1, part], p.down).start()
        remote(ref, ref, sk, zrecv.at[part], p.across).start()
    share(0, 0, csem.at[0])
    for kx in range(4):
        send_rows(hid_in, hid, h1, 512, 0, 2, p.plane(1, kx))
        send_rows(hid_in, hid, h1, 512, 1, 1, p.plane(3, kx))
        if kx:
            send_rows(hid_in, hid, h1, 512, 0, 0, p.plane(0, kx))
            send_rows(hid_in, hid, h1, 512, 1, 3, p.plane(0, kx))

    ref = qbuf.at[0:448]
    remote(ref, ref, sk, q1, p.up).wait_recv()
    same = 1 + p.zl
    for r in range(2):
        cols = slice(r * 128, (r + 1) * 128)
        qs[r * 384 : r * 384 + 128] = qbuf[0:128, cols]
        qs[r * 384 + 128 : r * 384 + 256] = qbuf[pl.ds(pl.multiple_of(same * 128, 128), 128), cols]
        qs[r * 384 + 256 : r * 384 + 384] = qbuf[384:512, cols]
        qs[768 + r * 128 : 896 + r * 128] = qbuf[pl.ds(pl.multiple_of((3 - same) * 128, 128), 128), cols]
    oa[...] = jnp.zeros_like(oa)
    peak[...] = jnp.full_like(peak, negative_fill)

    def absorb(start, count, sub, chip, row_pos):
        keys = kv[pl.ds(chip * 2, 2), :, 0:128].reshape(1024, 128)
        values = kv[pl.ds(chip * 2, 2), :, 128:384].reshape(1024, 256)
        tiles = [slice(start + at, start + at + sub) for at in range(0, count, sub)]
        asked = [qs[rows] for rows in tiles]
        olds = [peak[rows] for rows in tiles]
        sums = [oa[rows] for rows in tiles]

        def score(t):
            s = lax.dot_general(asked[t], keys, (((1,), (1,)), ((), ())), preferred_element_type=F32)
            if row_pos is not None:
                i = t * sub + lax.broadcasted_iota(jnp.int32, (sub, 1), 0)
                key_pos = chip * 1024 + lax.broadcasted_iota(jnp.int32, (sub, 1024), 1)
                s = jnp.where(key_pos <= row_pos(i), s, negative_fill)
            return [s[:, at : at + 128] for at in range(0, 1024, 128)]

        news, ends = [], []
        coming = score(0)
        for t, old in enumerate(olds):
            s = coming
            top = s[0]
            for piece in s[1:]:
                top = jnp.maximum(top, piece)
            if t + 1 < len(tiles):
                coming = score(t + 1)
            new = jnp.maximum(old, jnp.max(top, axis=1, keepdims=True))
            w = jnp.concatenate([jnp.exp2((piece - new) * SCALE).astype(BF16) for piece in s], axis=1)
            shrink = jnp.exp2((old - new) * SCALE)
            part = jnp.dot(w, values, preferred_element_type=F32)
            news.append(new)
            ends.append(sums[t] * jnp.concatenate([shrink, shrink], axis=1) + part)
        for rows, new, end in zip(tiles, news, ends):
            peak[rows] = new
            oa[rows] = end

    def spread(i):
        return ((i & 96) << 1) + (i & 31)

    def pos_a(i):
        seg = lax.rem(i >> 7, 3)
        shift = jnp.where(seg == 1, (1 - p.zl) * 288, p.zl * 256 + (seg >> 1) * 32)
        return own * 512 + spread(i & 127) + shift

    chip_b = (1 - p.zh) * 4 + p.y

    def pos_b(i):
        return (chip_b * 2 + p.core) * 512 + spread(i & 127) + (1 - p.zl) * 256 + p.zl * 32

    def absorb_a(chip, masked):
        absorb(0, 768, 256, chip, pos_a if masked else None)

    def absorb_b(chip, masked):
        absorb(768, 256, 128, chip, pos_b if masked else None)

    def seen(chip):
        @pl.when(chip < p.chip)
        def _():
            absorb_a(chip, False)

        @pl.when(chip < chip_b)
        def _():
            absorb_b(chip, False)

    wait_shared(0, 0, csem.at[0])
    absorb_a(p.chip, True)

    @pl.when(p.chip < chip_b)
    def _():
        absorb_b(p.chip, False)

    forward(0)
    for part in (p.zl, 1 - p.zl):
        ref = kv.at[block(1, 0), pl.ds(pl.multiple_of(part * 256, 256), 256), 0:256]
        remote(ref, ref, sk, zrecv.at[part], p.up).wait_recv()
        remote(ref, ref, sk, ysem.at[0, 3 + part], p.up).start()
        remote(ref, ref, sk, ysem.at[1, 3 + part], p.down).start()
    near_done(0)
    share(1, 0, csem.at[4])
    half = pl.ds(pl.multiple_of(p.core * 128, 128), 128)
    for kx in range(4):
        if kx:
            device = p.plane(0, kx)
            remote(
                wo_hbm.at[half, columns(device[0], 512)], wo.at[p.head, p.core], sk, w1, device
            ).start()
        for part in range(2):
            device = p.plane(1 + 2 * part, kx)
            rows = pl.ds(pl.multiple_of(p.core * 128 + part * 64, 64), 64)
            remote(
                wo_hbm.at[rows, columns(device[0], 512)],
                wo.at[p.head, p.core, part * 64 : (part + 1) * 64], sk, w1, device,
            ).start()
    wait_shared(0, 3, csem.at[3])
    wait_shared(0, 1, csem.at[1])

    def near_step(t, _):
        seen(p.chip_at(0, 3 - 2 * t))
        return 0

    lax.fori_loop(0, 2, near_step, 0)
    far_done(0)
    forward(1)
    wait_shared(1, 0, csem.at[4])
    chip = p.chip_at(1, 0)

    @pl.when(chip < p.chip)
    def _():
        absorb_a(chip, False)

    absorb_b(chip, True)
    near_done(1)
    wait_shared(0, 2, csem.at[2])
    wait_shared(1, 3, csem.at[7])
    wait_shared(1, 1, csem.at[5])

    def late_step(t, _):
        @pl.when(t == 3)
        def _():
            wown.wait()
            ref = wo.at[0:7, 0]
            remote(ref, ref, sk, w1, p.up).wait_recv()
            ref = wo.at[:, p.core]
            remote(ref, ref, sk, w2, p.partner).start()
            far_done(1)
            wait_shared(1, 2, csem.at[6])

        seen(p.chip_at(jnp.minimum(t, 1), 2 + t - 3 * (t // 2)))
        return 0

    lax.fori_loop(0, 4, late_step, 0)

    for r in range(2):
        cols = slice(r * 128, (r + 1) * 128)
        a = (oa[r * 384 : (r + 1) * 384, 0:128] / oa[r * 384 : (r + 1) * 384, 128:256]).astype(BF16)
        o = (oa[768 + r * 128 : 896 + r * 128, 0:128] / oa[768 + r * 128 : 896 + r * 128, 128:256]).astype(BF16)
        for b in range(2):
            abuf[p.head, 0, b, 0, 0:64, cols] = batch_rows(a[0:128], b)
            abuf[p.head, 0, b, p.zl, pl.ds(pl.multiple_of((1 - p.zl) * 64, 64), 64), cols] = batch_rows(a[128:256], b)
            abuf[p.head, 0, b, 1, 64:128, cols] = batch_rows(a[256:384], b)
            abuf[p.head, 0, b, 1 - p.zl, pl.ds(pl.multiple_of(p.zl * 64, 64), 64), cols] = batch_rows(o, b)

    ref = hid.at[0:448]
    remote(ref, ref, sk, h1, p.up).wait_recv()
    ref = wo.at[:, 1 - p.core]
    remote(ref, ref, sk, w2, p.partner).wait_recv()

    for ref in (
        qbuf.at[0:448], hid.at[0:448], kv.at[own, 0:448, 0:256], kv.at[0:15, :, 0:256], wo.at[0:7, 0], wo.at[:, p.core],
    ):
        pltpu.make_async_copy(ref, ref, sk).wait()


NS1 = 1
NS2 = 2
NC = 8
LAG = 5
ACROSS_FIRST = ((), ())
CW = 512
FFL = 896


def block_kernel(
    q_hbm, k_hbm, v_hbm, hid_hbm, gain_hbm, wo_hbm, gate_hbm, up_hbm, down_hbm, out,
    q, k, v, hid_in, gain, kv, qbuf, qs, oa, peak,
    abuf, rbuf, hid, wo, wgu, wd, oacc, acc, xg, sq, inner,
    zs, zr, keep, m1s, m1r, m2s, m2r,
    insem, wsem, sk, kv1, q1, h1, w1, w2, ysem, zrecv, csem,
    s1, r1, s2, r2, s3, zsem, m1sem, m2sem,
):
    p = Place()
    barrier = pltpu.get_barrier_semaphore()
    peers = [p.plane(0, kx) for kx in (1, 2, 3)]
    peers += [p.plane(step, kx) for step in (1, 3) for kx in range(4)]
    peers += [p.up, p.down, p.across, p.partner]
    for device in peers:
        pl.semaphore_signal(barrier, inc=1, device_id=device, device_id_type=MESH)
    loads = [
        pltpu.make_async_copy(src, dst, insem.at[i])
        for i, (src, dst) in enumerate(((k_hbm, k), (v_hbm, v), (q_hbm, q), (hid_hbm, hid_in), (gain_hbm, gain)))
    ]
    for load in loads:
        load.start()

    order = [p.here(0), p.other(0), p.here(3), p.here(1), p.here(2), p.other(3), p.other(1), p.other(2)]
    half = pl.ds(pl.multiple_of(p.core * 128, 128), 128)
    wo_copy = pltpu.make_async_copy(
        wo_hbm.at[half, columns(p.head, 512)], wo.at[p.head, p.core], wsem.at[16]
    )
    wd_copy = pltpu.make_async_copy(down_hbm, wd, wsem.at[17])

    def gate_copy(h):
        rows = pl.ds(pl.multiple_of(h * 512, 512), 512)
        return pltpu.make_async_copy(gate_hbm.at[rows], wgu.at[rows, 0:FFL], wsem.at[h])

    def up_copy(h):
        rows = pl.ds(pl.multiple_of(h * 512, 512), 512)
        return pltpu.make_async_copy(up_hbm.at[rows], wgu.at[rows, FFL : 2 * FFL], wsem.at[8 + h])

    wo_copy.start()
    for h in order:
        gate_copy(h).start()
        up_copy(h).start()
    wd_copy.start()

    me = p.here(0)
    kv[:, :, 256:384] = jnp.ones((16, 512, 128), BF16)
    kv_rows = pl.ds(pl.multiple_of(p.head * 64, 64), 64)
    for load in loads:
        load.wait()
    kv[p.blk, kv_rows, 0:128] = k[:, columns(p.head, 128)]
    kv[p.blk, kv_rows, 128:256] = v[:, columns(p.head, 128)]
    for part in range(2):
        rows = pl.ds(pl.multiple_of(part * 384 + p.x * 32, 32), 32)
        qbuf[rows, :] = q[part * 32 : (part + 1) * 32, columns(p.head, 256)]
        hid[rows, :] = hid_in[part * 32 : (part + 1) * 32, columns(p.head, 512)]
    pl.semaphore_wait(barrier, len(peers))
    attend_blocks(
        p, q, k, v, hid_in, wo_hbm, kv, qbuf, hid, wo, qs, oa, peak, abuf,
        sk, kv1, q1, h1, w1, w2, ysem, zrecv, csem, wo_copy,
    )

    c2 = 512 // NS2

    def project(b):
        rows = slice(b * 256, (b + 1) * 256)

        def add(h, first):
            part = jnp.dot(abuf[h, 0, b].reshape(256, 256), wo[h].reshape(256, 512), preferred_element_type=F32)
            if first:
                held = jnp.concatenate([batch_rows(hid[g * 128 : (g + 1) * 128], b) for g in range(4)], axis=0)
                oacc[rows] = held.astype(F32) + part
            else:
                oacc[rows] += part

        return add

    def residual(b):
        for s in range(NS2):
            for half in range(2):
                at = b * 256 + half * 128
                rbuf[me, s, b, half] = oacc[at : at + 128, s * c2 : (s + 1) * c2].astype(BF16)

    def expand(b):
        out_rows = slice(b * 256, (b + 1) * 256)

        def add(h, first):
            if b == 0:
                gate_copy(h).wait()
                up_copy(h).wait()
            total = None
            for s in range(NS2):
                r = rbuf[h, s, b].reshape(256, c2).astype(F32)
                for j in range(c2 // 128):
                    piece = r[:, j * 128 : (j + 1) * 128]
                    g = gain[pl.ds(h * 4 + s * (c2 // 128) + j, 1), :]
                    at = s * c2 + j * 128
                    xg[b, :, at : at + 128] = (piece * g).astype(BF16)
                    total = piece * piece if total is None else total + piece * piece
            rows = pl.ds(pl.multiple_of(h * 512, 512), 512)
            part = jnp.dot(xg[b], wgu[rows, :], preferred_element_type=F32)
            if first:
                sq[out_rows] = total
                acc[out_rows] = part
            else:
                sq[out_rows] += total
                acc[out_rows] += part

        return add

    def activate(b):
        rows = slice(b * 256, (b + 1) * 256)
        scale = lax.rsqrt(jnp.sum(sq[rows], axis=1, keepdims=True) * (1.0 / 4096.0) + 1e-5)
        sq[rows] = jnp.broadcast_to(scale, (256, 128))

        def tile(j, _):
            at = pl.multiple_of(j * 128, 128)
            u = acc[rows, pl.ds(at, 128)] * sq[rows]
            v = acc[rows, pl.ds(pl.multiple_of(at + FFL, 128), 128)] * sq[rows]
            inner[rows, pl.ds(at, 128)] = (u / (1.0 + jnp.exp(-u)) * v).astype(BF16)
            return 0

        lax.fori_loop(0, 7, tile, 0)

    def reduce_down(b):
        def one(c, _):
            cols = pl.ds(pl.multiple_of(c * CW, CW), CW)
            part = jnp.dot(inner[b * 256 : (b + 1) * 256], wd[:, cols], preferred_element_type=F32)
            n = b * NC + c
            keep[n, 0] = part[0:64]
            zs[n, 0] = part[64:128].astype(BF16)
            zs[n, 1] = part[128:192].astype(BF16)
            keep[n, 1] = part[192:256]
            remote(zs.at[n, 0], zr.at[n, 1], s3, zsem.at[1, n], p.above).start()
            remote(zs.at[n, 1], zr.at[n, 0], s3, zsem.at[0, n], p.below).start()
            return 0

        lax.fori_loop(0, NC, one, 0)

    def slot(k):
        return pl.ds(pl.multiple_of(p.xs[k] * 16, 16), 16)

    def m1_copy(n, side):
        device = p.right if side == 0 else p.left
        return remote(m1s.at[n, side], m1r.at[n, side], s3, m1sem.at[side, n], device)

    def m2_copy(n, side):
        device = p.right if side == 0 else p.left
        return remote(m2s.at[n, side], m2r.at[n, side], s3, m2sem.at[side, n], device)

    def finish():
        def one(t, _):
            @pl.when(t < 2 * NC)
            def _():
                n = t
                for side in range(2):
                    ref = zr.at[n, side]
                    remote(ref, ref, s3, zsem.at[side, n], p.right).wait_recv()
                    keep[n, side] += zr[n, side].astype(F32)
                    m1s[n, side] = keep[n, side, slot(2), :].astype(BF16)
                    m1_copy(n, side).start()

            @pl.when((t >= LAG) & (t < 2 * NC + LAG))
            def _():
                n = t - LAG
                for side in range(2):
                    m1_copy(n, side).wait_recv()
                    k = 1 if side == 0 else 3
                    for part in range(2):
                        q = keep[n, part, slot(k), :]
                        if part == side:
                            q = q + m1r[n, side].astype(F32)
                        m2s[n, side, part] = q.astype(BF16)
                    m2_copy(n, side).start()

            @pl.when(t >= 2 * LAG)
            def _():
                n = t - 2 * LAG
                b, c = n // NC, lax.rem(n, NC)
                for side in range(2):
                    m2_copy(n, side).wait_recv()
                for part in range(2):
                    q = keep[n, part, slot(0), :] + m2r[n, 0, part].astype(F32) + m2r[n, 1, part].astype(F32)
                    rows = pl.ds(pl.multiple_of(part * 64 + p.x * 16, 16), 16)
                    for s in range(NS2):
                        r = rbuf[c, s, b, part, rows, :].astype(F32)
                        cols = pl.ds(pl.multiple_of(c * CW + s * c2, c2), c2)
                        to = pl.ds(pl.multiple_of(part * 32 + b * 16, 16), 16)
                        out[to, cols] = (r + q[:, s * c2 : (s + 1) * c2]).astype(BF16)

            return 0

        lax.fori_loop(0, 2 * NC + 2 * LAG, one, 0)

    ga = [gather_rows(p, abuf, b, s1, r1, NS1, project(b)) for b in range(2)]
    gr = [gather_rows(p, rbuf, b, s2, r2, NS2, expand(b), ACROSS_FIRST[b]) for b in range(2)]
    advance(ga[0], 1)
    advance(ga[1], 1)
    advance(ga[0], 1)
    advance(ga[1], 1)
    advance(ga[0], 1)
    advance(ga[1], 1)
    advance(ga[0], 1)
    advance(ga[1], 1)
    advance(ga[0], 1)
    advance(ga[1], 1)
    advance(ga[0], 1)
    advance(ga[1], 1)
    advance(ga[0], 1)
    advance(ga[1], 1)
    advance(ga[0], 4)
    residual(0)
    advance(gr[0], 2)
    advance(ga[1], 4)
    residual(1)
    advance(gr[0], 5)
    advance(gr[1], 1)
    advance(gr[0], 1)
    advance(gr[1], 3)
    advance(gr[0], 3)
    activate(0)
    wd_copy.wait()
    advance(gr[1], 3)
    reduce_down(0)
    advance(gr[1], 4)
    activate(1)
    reduce_down(1)
    finish()
    pltpu.make_async_copy(abuf.at[0:7], abuf.at[0:7], s1).wait()
    pltpu.make_async_copy(rbuf.at[0:7], rbuf.at[0:7], s2).wait()
    for ref in (zs, m1s, m2s):
        pltpu.make_async_copy(ref, ref, s3).wait()


def layer(q, k, v, hidden, gain, wo, gate, up, down):
    vmem = pl.BlockSpec(memory_space=pltpu.VMEM)
    hbm = pl.BlockSpec(memory_space=pl.ANY)
    dma = pltpu.SemaphoreType.DMA
    return pl.pallas_call(
        block_kernel,
        out_shape=pltpu.VMEM((64, 4096), BF16),
        in_specs=[hbm] * 9,
        out_specs=vmem,
        scratch_shapes=[
            pltpu.VMEM((64, 2048), BF16),
            pltpu.VMEM((64, 1024), BF16),
            pltpu.VMEM((64, 1024), BF16),
            pltpu.VMEM((64, 4096), BF16),
            pltpu.VMEM((32, 128), F32),
            pltpu.VMEM((16, 512, 384), BF16),
            pltpu.VMEM((512, 256), BF16),
            pltpu.VMEM((1024, 128), BF16),
            pltpu.VMEM((1024, 256), F32),
            pltpu.VMEM((1024, 128), F32),
            pltpu.VMEM((8, NS1, 2, 2, 128, 256 // NS1), BF16),
            pltpu.VMEM((8, NS2, 2, 2, 128, 512 // NS2), BF16),
            pltpu.VMEM((512, 512), BF16),
            pltpu.VMEM((8, 2, 128, 512), BF16),
            pltpu.VMEM((4096, 2 * FFL), BF16),
            pltpu.VMEM((FFL, 4096), BF16),
            pltpu.VMEM((512, 512), F32),
            pltpu.VMEM((512, 2 * FFL), F32),
            pltpu.VMEM((2, 256, 512), BF16),
            pltpu.VMEM((512, 128), F32),
            pltpu.VMEM((512, FFL), BF16),
            pltpu.VMEM((2 * NC, 2, 64, CW), BF16),
            pltpu.VMEM((2 * NC, 2, 64, CW), BF16),
            pltpu.VMEM((2 * NC, 2, 64, CW), F32),
            pltpu.VMEM((2 * NC, 2, 16, CW), BF16),
            pltpu.VMEM((2 * NC, 2, 16, CW), BF16),
            pltpu.VMEM((2 * NC, 2, 2, 16, CW), BF16),
            pltpu.VMEM((2 * NC, 2, 2, 16, CW), BF16),
            dma((5,)),
            dma((18,)),
            dma,
            dma((2,)),
            dma,
            dma,
            dma,
            dma,
            dma((2, 6)),
            dma((2,)),
            dma((8,)),
            dma,
            dma((14, NS1, 2)),
            dma,
            dma((14, NS2, 2)),
            dma,
            dma((2, 2 * NC)),
            dma((2, 2 * NC)),
            dma((2, 2 * NC)),
        ],
        compiler_params=pltpu.CompilerParams(
            collective_id=1, has_side_effects=True, vmem_limit_bytes=62 * 1024 * 1024
        ),
        cost_estimate=pl.CostEstimate(flops=16_500_000_000, bytes_accessed=24_000_000, transcendentals=0),
        name="layer",
    )(q, k, v, hidden, gain, wo, gate, up, down)


def local(
    hidden_in,
    queries,
    key_states,
    value_states,
    out_weight,
    norm_gain,
    gate_weight,
    up_weight,
    down_weight,
):
    return layer(
        queries, key_states, value_states, hidden_in, norm_gain.reshape(32, 128),
        out_weight, gate_weight, up_weight, down_weight,
    )


def solution(mesh):
    return jax.shard_map(
        local,
        mesh=mesh,
        in_specs=(
            P(("blk", "head"), None),
            P(("blk", "head"), None),
            P(("blk", "head"), None),
            P(("blk", "head"), None),
            P("head", None),
            P(),
            P(None, "head"),
            P(None, "head"),
            P("head", None),
        ),
        out_specs=P(("blk", "head"), None),
        check_vma=False,
    )
```

```python
import jax
import jax.numpy as jnp
from jax import lax
from jax.experimental import pallas as pl
from jax.experimental.pallas import tpu as pltpu
from jax.sharding import PartitionSpec as P

HEAD_DIM = 128
MESH = pl.DeviceIdType.MESH
F32 = jnp.float32
BF16 = jnp.bfloat16

negative_fill = -1e30


class Place:
    def __init__(self):
        self.head = lax.axis_index("head")
        self.blk = lax.axis_index("blk")
        self.x = lax.rem(self.head, 4)
        self.zl = self.head // 4
        self.zh = self.blk // 8
        self.yc = lax.rem(self.blk, 8)
        self.z = self.zh * 2 + self.zl
        self.xs = [lax.rem(self.x + k, 4) for k in range(4)]
        self.right = self.at_x(self.xs[1])
        self.left = self.at_x(self.xs[3])
        self.above = self.at_z(1)
        self.below = self.at_z(3)

        self.y = self.yc // 2
        self.core = lax.rem(self.blk, 2)
        self.chip = self.blk // 2
        self.up = self.at_y(1)
        self.down = self.at_y(3)
        self.partner = (self.head, self.blk + 1 - 2 * self.core)
        self.across = (self.head, (1 - self.zh) * 8 + self.yc)

    def at_y(self, step):
        return (self.head, self.zh * 8 + lax.rem(self.y + step, 4) * 2 + self.core)

    def plane(self, step, k):
        z = lax.rem(self.z + step, 4)
        return (lax.rem(z, 2) * 4 + self.xs[k], (z // 2) * 8 + self.yc)

    def chip_at(self, dz, k):
        return lax.rem(self.zh + dz, 2) * 4 + lax.rem(self.y + k, 4)

    def at_x(self, x):
        return (self.zl * 4 + x, self.blk)

    def at_z(self, step):
        z = lax.rem(self.z + step, 4)
        return (lax.rem(z, 2) * 4 + self.x, (z // 2) * 8 + self.yc)

    def here(self, k):
        return self.zl * 4 + self.xs[k]

    def other(self, k):
        return (1 - self.zl) * 4 + self.xs[k]


def remote(src, dst, send_sem, recv_sem, device):
    return pltpu.make_async_remote_copy(
        src_ref=src, dst_ref=dst, send_sem=send_sem, recv_sem=recv_sem,
        device_id=device, device_id_type=MESH,
    )


def gather_rows(p, buf, batch, send_sem, recv, steps, compute, across_first=()):
    def send(h, s, half, to_half, kind, device):
        src, dst = buf.at[h, s, batch, half], buf.at[h, s, batch, to_half]
        remote(src, dst, send_sem, recv.at[kind, s, batch], device).start()

    def wait(h, s, half, kind):
        ref = buf.at[h, s, batch, half]
        remote(ref, ref, send_sem, recv.at[kind, s, batch], p.right).wait_recv()

    me, left, right, far = p.here(0), p.here(3), p.here(1), p.here(2)
    twin, twin_left, twin_right, twin_far = p.other(0), p.other(3), p.other(1), p.other(2)
    along_first = [s for s in range(steps) if s not in across_first]
    for s in range(steps):
        send(me, s, 0, 0, 0, p.right)
        send(me, s, 1, 1, 4, p.left)
        send(me, s, 0, 1, 6, p.above)
        send(me, s, 1, 0, 10, p.below)
    yield
    compute(me, True)
    yield
    for s in range(steps):
        wait(left, s, 0, 0)
        send(left, s, 0, 0, 2, p.right)
        wait(right, s, 1, 4)
        send(right, s, 1, 1, 5, p.left)
        if s in along_first:
            send(left, s, 0, 1, 7, p.above)
            send(right, s, 1, 0, 12, p.below)
    yield
    for s in range(steps):
        send(me, s, 1, 1, 1, p.right)
        send(me, s, 0, 0, 3, p.left)
    yield
    for s in range(steps):
        wait(twin, s, 1, 6)
        wait(twin, s, 0, 10)
        if s in across_first:
            send(twin, s, 0, 0, 11, p.right)
            send(twin, s, 1, 1, 8, p.left)
            send(twin, s, 1, 1, 7, p.right)
            send(twin, s, 0, 0, 12, p.left)
    compute(twin, False)
    yield
    for s in range(steps):
        wait(far, s, 0, 2)
        wait(far, s, 1, 5)
        if s in along_first:
            send(far, s, 0, 1, 9, p.above)
            send(far, s, 1, 0, 13, p.below)
    yield
    for s in range(steps):
        wait(left, s, 1, 1)
        wait(right, s, 0, 3)
        if s in along_first:
            send(left, s, 1, 0, 11, p.below)
            send(right, s, 0, 1, 8, p.above)
    yield
    for s in across_first:
        wait(twin_left, s, 0, 11)
        send(twin_left, s, 0, 0, 13, p.right)
        wait(twin_right, s, 1, 8)
        send(twin_right, s, 1, 1, 9, p.left)
    yield
    compute(left, False)
    compute(right, False)
    compute(far, False)
    yield
    for s in range(steps):
        wait(twin_left, s, 1, 7)
        if s in along_first:
            wait(twin_left, s, 0, 11)
    compute(twin_left, False)
    yield
    for s in range(steps):
        wait(twin_right, s, 0, 12)
        if s in along_first:
            wait(twin_right, s, 1, 8)
    compute(twin_right, False)
    yield
    for s in range(steps):
        wait(twin_far, s, 1, 9)
        wait(twin_far, s, 0, 13)
    compute(twin_far, False)


def advance(stages, count):
    for _ in range(count):
        next(stages, None)


def columns(h, width):
    return pl.ds(pl.multiple_of(h * width, width), width)


SCALE = HEAD_DIM ** (-0.5) * 1.4426950408889634


def batch_rows(group, b):
    return jnp.concatenate([group[at + b * 16 : at + b * 16 + 16] for at in range(0, 128, 32)], axis=0)


def attend_blocks(
    p, q, k, v, hid_in, wo_hbm, kv, qbuf, hid, wo, qs, oa, peak, abuf,
    sk, kv1, q1, h1, w1, w2, ysem, zrecv, csem, wown,
):
    own = p.blk
    mine = pl.ds(pl.multiple_of(p.x * 32, 32), 32)

    def rows_of(g):
        return pl.ds(pl.multiple_of(g * 128 + p.x * 32, 32), 32)

    kv_rows = pl.ds(pl.multiple_of(p.head * 64, 64), 64)

    def send_kv(device, sem):
        h = device[0]
        remote(k.at[:, columns(h, 128)], kv.at[own, kv_rows, 0:128], sk, sem, device).start()
        remote(v.at[:, columns(h, 128)], kv.at[own, kv_rows, 128:256], sk, sem, device).start()

    def send_rows(src, dst, sem, width, part, g, device):
        at = columns(device[0], width)
        remote(src.at[part * 32 : (part + 1) * 32, at], dst.at[rows_of(g), :], sk, sem, device).start()

    near = 1 - 2 * p.zl + 4
    for kx in range(4):
        send_kv(p.plane(near, kx), kv1.at[1])
        if kx:
            send_kv(p.plane(0, kx), kv1.at[0])
    for kx in range(4):
        send_rows(q, qbuf, q1, 256, 0, 2, p.plane(1, kx))
        send_rows(q, qbuf, q1, 256, 1, 1, p.plane(3, kx))
        if kx:
            send_rows(q, qbuf, q1, 256, 0, 0, p.plane(0, kx))
            send_rows(q, qbuf, q1, 256, 1, 3, p.plane(0, kx))

    def block(dz, kk, other=False):
        core = 1 - p.core if other else p.core
        return p.chip_at(dz, kk) * 2 + core

    def piece(dz, kk, part):
        return kv.at[block(dz, kk), part * 256 : (part + 1) * 256, 0:256]

    def send_piece(dz, kk, part, sem, device):
        remote(piece(dz, kk, part), piece(dz, kk, part), sk, sem, device).start()

    def wait_piece(dz, kk, part, sem):
        remote(piece(dz, kk, part), piece(dz, kk, part), sk, sem, p.up).wait_recv()

    def share(dz, kk, sem):
        ref = kv.at[block(dz, kk), :, 0:256]
        remote(ref, ref, sk, sem, p.partner).start()

    def wait_shared(dz, kk, sem):
        ref = kv.at[block(dz, kk, True), :, 0:256]
        remote(ref, ref, sk, sem, p.partner).wait_recv()

    def forward(dz):
        i = 3 * dz
        wait_piece(dz, 3, 0, ysem.at[0, i])
        send_piece(dz, 3, 0, ysem.at[0, i + 2], p.up)
        wait_piece(dz, 1, 1, ysem.at[1, i + 1])
        send_piece(dz, 1, 1, ysem.at[1, i + 2], p.down)

    def near_done(dz):
        i = 3 * dz
        wait_piece(dz, 3, 1, ysem.at[0, i + 1])
        share(dz, 3, csem.at[4 * dz + 3])
        wait_piece(dz, 1, 0, ysem.at[1, i])
        share(dz, 1, csem.at[4 * dz + 1])

    def far_done(dz):
        i = 3 * dz
        wait_piece(dz, 2, 0, ysem.at[0, i + 2])
        wait_piece(dz, 2, 1, ysem.at[1, i + 2])
        share(dz, 2, csem.at[4 * dz + 2])

    def own_rows(part):
        return kv.at[own, pl.ds(pl.multiple_of(part * 256, 256), 256), 0:256]

    for order, (part, count) in enumerate(((p.zl, 192), (1 - p.zl, 256))):
        ref = kv.at[own, 0:count, 0:256]
        remote(ref, ref, sk, kv1.at[order], p.up).wait_recv()
        ref = own_rows(part)
        remote(ref, ref, sk, ysem.at[0, part], p.up).start()
        remote(ref, ref, sk, ysem.at[1, part], p.down).start()
        remote(ref, ref, sk, zrecv.at[part], p.across).start()
    share(0, 0, csem.at[0])
    for kx in range(4):
        send_rows(hid_in, hid, h1, 512, 0, 2, p.plane(1, kx))
        send_rows(hid_in, hid, h1, 512, 1, 1, p.plane(3, kx))
        if kx:
            send_rows(hid_in, hid, h1, 512, 0, 0, p.plane(0, kx))
            send_rows(hid_in, hid, h1, 512, 1, 3, p.plane(0, kx))

    ref = qbuf.at[0:448]
    remote(ref, ref, sk, q1, p.up).wait_recv()
    same = 1 + p.zl
    for r in range(2):
        cols = slice(r * 128, (r + 1) * 128)
        qs[r * 384 : r * 384 + 128] = qbuf[0:128, cols]
        qs[r * 384 + 128 : r * 384 + 256] = qbuf[pl.ds(pl.multiple_of(same * 128, 128), 128), cols]
        qs[r * 384 + 256 : r * 384 + 384] = qbuf[384:512, cols]
        qs[768 + r * 128 : 896 + r * 128] = qbuf[pl.ds(pl.multiple_of((3 - same) * 128, 128), 128), cols]
    oa[...] = jnp.zeros_like(oa)
    peak[...] = jnp.full_like(peak, negative_fill)

    def absorb(start, count, sub, chip, row_pos):
        keys = kv[pl.ds(chip * 2, 2), :, 0:128].reshape(1024, 128)
        values = kv[pl.ds(chip * 2, 2), :, 128:384].reshape(1024, 256)
        tiles = [slice(start + at, start + at + sub) for at in range(0, count, sub)]
        asked = [qs[rows] for rows in tiles]
        olds = [peak[rows] for rows in tiles]
        sums = [oa[rows] for rows in tiles]

        def score(t):
            s = lax.dot_general(asked[t], keys, (((1,), (1,)), ((), ())), preferred_element_type=F32)
            if row_pos is not None:
                i = t * sub + lax.broadcasted_iota(jnp.int32, (sub, 1), 0)
                key_pos = chip * 1024 + lax.broadcasted_iota(jnp.int32, (sub, 1024), 1)
                s = jnp.where(key_pos <= row_pos(i), s, negative_fill)
            return [s[:, at : at + 128] for at in range(0, 1024, 128)]

        news, ends = [], []
        coming = score(0)
        for t, old in enumerate(olds):
            s = coming
            top = s[0]
            for piece in s[1:]:
                top = jnp.maximum(top, piece)
            if t + 1 < len(tiles):
                coming = score(t + 1)
            new = jnp.maximum(old, jnp.max(top, axis=1, keepdims=True))
            w = jnp.concatenate([jnp.exp2((piece - new) * SCALE).astype(BF16) for piece in s], axis=1)
            shrink = jnp.exp2((old - new) * SCALE)
            part = jnp.dot(w, values, preferred_element_type=F32)
            news.append(new)
            ends.append(sums[t] * jnp.concatenate([shrink, shrink], axis=1) + part)
        for rows, new, end in zip(tiles, news, ends):
            peak[rows] = new
            oa[rows] = end

    def spread(i):
        return ((i & 96) << 1) + (i & 31)

    def pos_a(i):
        seg = lax.rem(i >> 7, 3)
        shift = jnp.where(seg == 1, (1 - p.zl) * 288, p.zl * 256 + (seg >> 1) * 32)
        return own * 512 + spread(i & 127) + shift

    chip_b = (1 - p.zh) * 4 + p.y

    def pos_b(i):
        return (chip_b * 2 + p.core) * 512 + spread(i & 127) + (1 - p.zl) * 256 + p.zl * 32

    def absorb_a(chip, masked):
        absorb(0, 768, 256, chip, pos_a if masked else None)

    def absorb_b(chip, masked):
        absorb(768, 256, 128, chip, pos_b if masked else None)

    def seen(chip):
        @pl.when(chip < p.chip)
        def _():
            absorb_a(chip, False)

        @pl.when(chip < chip_b)
        def _():
            absorb_b(chip, False)

    wait_shared(0, 0, csem.at[0])
    absorb_a(p.chip, True)

    @pl.when(p.chip < chip_b)
    def _():
        absorb_b(p.chip, False)

    forward(0)
    for part in (p.zl, 1 - p.zl):
        ref = kv.at[block(1, 0), pl.ds(pl.multiple_of(part * 256, 256), 256), 0:256]
        remote(ref, ref, sk, zrecv.at[part], p.up).wait_recv()
        remote(ref, ref, sk, ysem.at[0, 3 + part], p.up).start()
        remote(ref, ref, sk, ysem.at[1, 3 + part], p.down).start()
    near_done(0)
    share(1, 0, csem.at[4])
    half = pl.ds(pl.multiple_of(p.core * 128, 128), 128)
    for kx in range(4):
        if kx:
            device = p.plane(0, kx)
            remote(
                wo_hbm.at[half, columns(device[0], 512)], wo.at[p.head, p.core], sk, w1, device
            ).start()
        for part in range(2):
            device = p.plane(1 + 2 * part, kx)
            rows = pl.ds(pl.multiple_of(p.core * 128 + part * 64, 64), 64)
            remote(
                wo_hbm.at[rows, columns(device[0], 512)],
                wo.at[p.head, p.core, part * 64 : (part + 1) * 64], sk, w1, device,
            ).start()
    wait_shared(0, 3, csem.at[3])
    wait_shared(0, 1, csem.at[1])

    def near_step(t, _):
        @pl.when(t == 1)
        def _():
            forward(1)

        seen(p.chip_at(0, 3 - 2 * t))
        return 0

    lax.fori_loop(0, 2, near_step, 0)
    far_done(0)
    wait_shared(1, 0, csem.at[4])
    chip = p.chip_at(1, 0)

    @pl.when(chip < p.chip)
    def _():
        absorb_a(chip, False)

    absorb_b(chip, True)

    def late_step(t, _):
        @pl.when(t == 0)
        def _():
            wait_shared(0, 2, csem.at[2])

        @pl.when(t == 1)
        def _():
            near_done(1)
            wait_shared(1, 3, csem.at[7])

        @pl.when(t == 2)
        def _():
            far_done(1)
            wait_shared(1, 1, csem.at[5])

        @pl.when(t == 3)
        def _():
            wown.wait()
            ref = wo.at[0:7, 0]
            remote(ref, ref, sk, w1, p.up).wait_recv()
            ref = wo.at[:, p.core]
            remote(ref, ref, sk, w2, p.partner).start()
            wait_shared(1, 2, csem.at[6])

        seen(p.chip_at(jnp.minimum(t, 1), 2 + t - 3 * (t // 2)))
        return 0

    lax.fori_loop(0, 4, late_step, 0)

    for r in range(2):
        cols = slice(r * 128, (r + 1) * 128)
        a = (oa[r * 384 : (r + 1) * 384, 0:128] / oa[r * 384 : (r + 1) * 384, 128:256]).astype(BF16)
        o = (oa[768 + r * 128 : 896 + r * 128, 0:128] / oa[768 + r * 128 : 896 + r * 128, 128:256]).astype(BF16)
        for b in range(2):
            abuf[p.head, 0, b, 0, 0:64, cols] = batch_rows(a[0:128], b)
            abuf[p.head, 0, b, p.zl, pl.ds(pl.multiple_of((1 - p.zl) * 64, 64), 64), cols] = batch_rows(a[128:256], b)
            abuf[p.head, 0, b, 1, 64:128, cols] = batch_rows(a[256:384], b)
            abuf[p.head, 0, b, 1 - p.zl, pl.ds(pl.multiple_of(p.zl * 64, 64), 64), cols] = batch_rows(o, b)

    ref = hid.at[0:448]
    remote(ref, ref, sk, h1, p.up).wait_recv()
    ref = wo.at[:, 1 - p.core]
    remote(ref, ref, sk, w2, p.partner).wait_recv()

    for ref in (
        qbuf.at[0:448], hid.at[0:448], kv.at[own, 0:448, 0:256], kv.at[0:15, :, 0:256], wo.at[0:7, 0], wo.at[:, p.core],
    ):
        pltpu.make_async_copy(ref, ref, sk).wait()


NS1 = 1
NS2 = 2
NC = 8
LAG = 5
ACROSS_FIRST = ((), (1,))
CW = 512
FFL = 896


def block_kernel(
    q_hbm, k_hbm, v_hbm, hid_hbm, gain_hbm, wo_hbm, gate_hbm, up_hbm, down_hbm, out,
    q, k, v, hid_in, gain, kv, qbuf, qs, oa, peak,
    abuf, rbuf, hid, wo, wgu, wd, oacc, acc, xg, sq, inner,
    zs, zr, keep, m1s, m1r, m2s, m2r,
    insem, wsem, sk, kv1, q1, h1, w1, w2, ysem, zrecv, csem,
    s1, r1, s2, r2, s3, zsem, m1sem, m2sem,
):
    p = Place()
    barrier = pltpu.get_barrier_semaphore()
    peers = [p.plane(0, kx) for kx in (1, 2, 3)]
    peers += [p.plane(step, kx) for step in (1, 3) for kx in range(4)]
    peers += [p.up, p.down, p.across, p.partner]
    for device in peers:
        pl.semaphore_signal(barrier, inc=1, device_id=device, device_id_type=MESH)
    loads = [
        pltpu.make_async_copy(src, dst, insem.at[i])
        for i, (src, dst) in enumerate(((k_hbm, k), (v_hbm, v), (q_hbm, q), (hid_hbm, hid_in), (gain_hbm, gain)))
    ]
    for load in loads:
        load.start()

    order = [p.here(0), p.other(0), p.here(3), p.here(1), p.here(2), p.other(3), p.other(1), p.other(2)]
    half = pl.ds(pl.multiple_of(p.core * 128, 128), 128)
    wo_copy = pltpu.make_async_copy(
        wo_hbm.at[half, columns(p.head, 512)], wo.at[p.head, p.core], wsem.at[16]
    )
    wd_copy = pltpu.make_async_copy(down_hbm, wd, wsem.at[17])

    def gate_copy(h):
        rows = pl.ds(pl.multiple_of(h * 512, 512), 512)
        return pltpu.make_async_copy(gate_hbm.at[rows], wgu.at[rows, 0:FFL], wsem.at[h])

    def up_copy(h):
        rows = pl.ds(pl.multiple_of(h * 512, 512), 512)
        return pltpu.make_async_copy(up_hbm.at[rows], wgu.at[rows, FFL : 2 * FFL], wsem.at[8 + h])

    wo_copy.start()
    for h in order:
        gate_copy(h).start()
        up_copy(h).start()
    wd_copy.start()

    me = p.here(0)
    kv[:, :, 256:384] = jnp.ones((16, 512, 128), BF16)
    kv_rows = pl.ds(pl.multiple_of(p.head * 64, 64), 64)
    for load in loads:
        load.wait()
    kv[p.blk, kv_rows, 0:128] = k[:, columns(p.head, 128)]
    kv[p.blk, kv_rows, 128:256] = v[:, columns(p.head, 128)]
    for part in range(2):
        rows = pl.ds(pl.multiple_of(part * 384 + p.x * 32, 32), 32)
        qbuf[rows, :] = q[part * 32 : (part + 1) * 32, columns(p.head, 256)]
        hid[rows, :] = hid_in[part * 32 : (part + 1) * 32, columns(p.head, 512)]
    pl.semaphore_wait(barrier, len(peers))
    attend_blocks(
        p, q, k, v, hid_in, wo_hbm, kv, qbuf, hid, wo, qs, oa, peak, abuf,
        sk, kv1, q1, h1, w1, w2, ysem, zrecv, csem, wo_copy,
    )

    c2 = 512 // NS2

    def project(b):
        rows = slice(b * 256, (b + 1) * 256)

        def add(h, first):
            part = jnp.dot(abuf[h, 0, b].reshape(256, 256), wo[h].reshape(256, 512), preferred_element_type=F32)
            if first:
                held = jnp.concatenate([batch_rows(hid[g * 128 : (g + 1) * 128], b) for g in range(4)], axis=0)
                oacc[rows] = held.astype(F32) + part
            else:
                oacc[rows] += part

        return add

    def residual(b):
        for s in range(NS2):
            for half in range(2):
                at = b * 256 + half * 128
                rbuf[me, s, b, half] = oacc[at : at + 128, s * c2 : (s + 1) * c2].astype(BF16)

    def expand(b):
        out_rows = slice(b * 256, (b + 1) * 256)

        def add(h, first):
            if b == 0:
                gate_copy(h).wait()
                up_copy(h).wait()
            total = None
            for s in range(NS2):
                r = rbuf[h, s, b].reshape(256, c2).astype(F32)
                for j in range(c2 // 128):
                    piece = r[:, j * 128 : (j + 1) * 128]
                    g = gain[pl.ds(h * 4 + s * (c2 // 128) + j, 1), :]
                    at = s * c2 + j * 128
                    xg[b, :, at : at + 128] = (piece * g).astype(BF16)
                    total = piece * piece if total is None else total + piece * piece
            rows = pl.ds(pl.multiple_of(h * 512, 512), 512)
            part = jnp.dot(xg[b], wgu[rows, :], preferred_element_type=F32)
            if first:
                sq[out_rows] = total
                acc[out_rows] = part
            else:
                sq[out_rows] += total
                acc[out_rows] += part

        return add

    def activate(b):
        rows = slice(b * 256, (b + 1) * 256)
        scale = lax.rsqrt(jnp.sum(sq[rows], axis=1, keepdims=True) * (1.0 / 4096.0) + 1e-5)
        sq[rows] = jnp.broadcast_to(scale, (256, 128))

        def tile(j, _):
            at = pl.multiple_of(j * 128, 128)
            u = acc[rows, pl.ds(at, 128)] * sq[rows]
            v = acc[rows, pl.ds(pl.multiple_of(at + FFL, 128), 128)] * sq[rows]
            inner[rows, pl.ds(at, 128)] = (u / (1.0 + jnp.exp(-u)) * v).astype(BF16)
            return 0

        lax.fori_loop(0, 7, tile, 0)

    def reduce_down(b, start, stop):
        def one(c, _):
            cols = pl.ds(pl.multiple_of(c * CW, CW), CW)
            part = jnp.dot(inner[b * 256 : (b + 1) * 256], wd[:, cols], preferred_element_type=F32)
            n = b * NC + c
            keep[n, 0] = part[0:64]
            zs[n, 0] = part[64:128].astype(BF16)
            zs[n, 1] = part[128:192].astype(BF16)
            keep[n, 1] = part[192:256]
            remote(zs.at[n, 0], zr.at[n, 1], s3, zsem.at[1, n], p.above).start()
            remote(zs.at[n, 1], zr.at[n, 0], s3, zsem.at[0, n], p.below).start()
            return 0

        lax.fori_loop(start, stop, one, 0)

    def slot(k):
        return pl.ds(pl.multiple_of(p.xs[k] * 16, 16), 16)

    def m1_copy(n, side):
        device = p.right if side == 0 else p.left
        return remote(m1s.at[n, side], m1r.at[n, side], s3, m1sem.at[side, n], device)

    def m2_copy(n, side):
        device = p.right if side == 0 else p.left
        return remote(m2s.at[n, side], m2r.at[n, side], s3, m2sem.at[side, n], device)

    def finish():
        def one(t, _):
            @pl.when(t < 2 * NC)
            def _():
                n = t
                for side in range(2):
                    ref = zr.at[n, side]
                    remote(ref, ref, s3, zsem.at[side, n], p.right).wait_recv()
                    keep[n, side] += zr[n, side].astype(F32)
                    m1s[n, side] = keep[n, side, slot(2), :].astype(BF16)
                    m1_copy(n, side).start()

            @pl.when((t >= LAG) & (t < 2 * NC + LAG))
            def _():
                n = t - LAG
                for side in range(2):
                    m1_copy(n, side).wait_recv()
                    k = 1 if side == 0 else 3
                    for part in range(2):
                        q = keep[n, part, slot(k), :]
                        if part == side:
                            q = q + m1r[n, side].astype(F32)
                        m2s[n, side, part] = q.astype(BF16)
                    m2_copy(n, side).start()

            @pl.when(t >= 2 * LAG)
            def _():
                n = t - 2 * LAG
                b, c = n // NC, lax.rem(n, NC)
                for side in range(2):
                    m2_copy(n, side).wait_recv()
                for part in range(2):
                    q = keep[n, part, slot(0), :] + m2r[n, 0, part].astype(F32) + m2r[n, 1, part].astype(F32)
                    rows = pl.ds(pl.multiple_of(part * 64 + p.x * 16, 16), 16)
                    for s in range(NS2):
                        r = rbuf[c, s, b, part, rows, :].astype(F32)
                        cols = pl.ds(pl.multiple_of(c * CW + s * c2, c2), c2)
                        to = pl.ds(pl.multiple_of(part * 32 + b * 16, 16), 16)
                        out[to, cols] = (r + q[:, s * c2 : (s + 1) * c2]).astype(BF16)

            return 0

        lax.fori_loop(0, 2 * NC + 2 * LAG, one, 0)

    ga = [gather_rows(p, abuf, b, s1, r1, NS1, project(b)) for b in range(2)]
    gr = [gather_rows(p, rbuf, b, s2, r2, NS2, expand(b), ACROSS_FIRST[b]) for b in range(2)]
    advance(ga[0], 1)
    advance(ga[1], 1)
    advance(ga[0], 1)
    advance(ga[1], 1)
    advance(ga[0], 1)
    advance(ga[1], 1)
    advance(ga[0], 1)
    advance(ga[1], 1)
    advance(ga[0], 1)
    advance(ga[1], 1)
    advance(ga[0], 1)
    advance(ga[1], 1)
    advance(ga[0], 1)
    advance(ga[1], 1)
    advance(ga[0], 5)
    residual(0)
    advance(gr[0], 2)
    advance(ga[1], 5)
    residual(1)
    advance(gr[0], 5)
    advance(gr[1], 1)
    advance(gr[0], 2)
    advance(gr[1], 3)
    advance(gr[0], 3)
    activate(0)
    wd_copy.wait()
    advance(gr[1], 3)
    reduce_down(0, 0, 3)
    advance(gr[1], 1)
    reduce_down(0, 3, NC)
    advance(gr[1], 4)
    activate(1)
    reduce_down(1, 0, NC)
    finish()
    pltpu.make_async_copy(abuf.at[0:7], abuf.at[0:7], s1).wait()
    pltpu.make_async_copy(rbuf.at[0:7], rbuf.at[0:7], s2).wait()
    for ref in (zs, m1s, m2s):
        pltpu.make_async_copy(ref, ref, s3).wait()


def layer(q, k, v, hidden, gain, wo, gate, up, down):
    vmem = pl.BlockSpec(memory_space=pltpu.VMEM)
    hbm = pl.BlockSpec(memory_space=pl.ANY)
    dma = pltpu.SemaphoreType.DMA
    return pl.pallas_call(
        block_kernel,
        out_shape=pltpu.VMEM((64, 4096), BF16),
        in_specs=[hbm] * 9,
        out_specs=vmem,
        scratch_shapes=[
            pltpu.VMEM((64, 2048), BF16),
            pltpu.VMEM((64, 1024), BF16),
            pltpu.VMEM((64, 1024), BF16),
            pltpu.VMEM((64, 4096), BF16),
            pltpu.VMEM((32, 128), F32),
            pltpu.VMEM((16, 512, 384), BF16),
            pltpu.VMEM((512, 256), BF16),
            pltpu.VMEM((1024, 128), BF16),
            pltpu.VMEM((1024, 256), F32),
            pltpu.VMEM((1024, 128), F32),
            pltpu.VMEM((8, NS1, 2, 2, 128, 256 // NS1), BF16),
            pltpu.VMEM((8, NS2, 2, 2, 128, 512 // NS2), BF16),
            pltpu.VMEM((512, 512), BF16),
            pltpu.VMEM((8, 2, 128, 512), BF16),
            pltpu.VMEM((4096, 2 * FFL), BF16),
            pltpu.VMEM((FFL, 4096), BF16),
            pltpu.VMEM((512, 512), F32),
            pltpu.VMEM((512, 2 * FFL), F32),
            pltpu.VMEM((2, 256, 512), BF16),
            pltpu.VMEM((512, 128), F32),
            pltpu.VMEM((512, FFL), BF16),
            pltpu.VMEM((2 * NC, 2, 64, CW), BF16),
            pltpu.VMEM((2 * NC, 2, 64, CW), BF16),
            pltpu.VMEM((2 * NC, 2, 64, CW), F32),
            pltpu.VMEM((2 * NC, 2, 16, CW), BF16),
            pltpu.VMEM((2 * NC, 2, 16, CW), BF16),
            pltpu.VMEM((2 * NC, 2, 2, 16, CW), BF16),
            pltpu.VMEM((2 * NC, 2, 2, 16, CW), BF16),
            dma((5,)),
            dma((18,)),
            dma,
            dma((2,)),
            dma,
            dma,
            dma,
            dma,
            dma((2, 6)),
            dma((2,)),
            dma((8,)),
            dma,
            dma((14, NS1, 2)),
            dma,
            dma((14, NS2, 2)),
            dma,
            dma((2, 2 * NC)),
            dma((2, 2 * NC)),
            dma((2, 2 * NC)),
        ],
        compiler_params=pltpu.CompilerParams(
            collective_id=1, has_side_effects=True, vmem_limit_bytes=62 * 1024 * 1024
        ),
        cost_estimate=pl.CostEstimate(flops=16_500_000_000, bytes_accessed=24_000_000, transcendentals=0),
        name="layer",
    )(q, k, v, hidden, gain, wo, gate, up, down)


def local(
    hidden_in,
    queries,
    key_states,
    value_states,
    out_weight,
    norm_gain,
    gate_weight,
    up_weight,
    down_weight,
):
    return layer(
        queries, key_states, value_states, hidden_in, norm_gain.reshape(32, 128),
        out_weight, gate_weight, up_weight, down_weight,
    )


def solution(mesh):
    return jax.shard_map(
        local,
        mesh=mesh,
        in_specs=(
            P(("blk", "head"), None),
            P(("blk", "head"), None),
            P(("blk", "head"), None),
            P(("blk", "head"), None),
            P("head", None),
            P(),
            P(None, "head"),
            P(None, "head"),
            P("head", None),
        ),
        out_specs=P(("blk", "head"), None),
        check_vma=False,
    )
```

```python
import jax
import jax.numpy as jnp
from jax import lax
from jax.experimental import pallas as pl
from jax.experimental.pallas import tpu as pltpu
from jax.sharding import PartitionSpec as P

HEAD_DIM = 128
MESH = pl.DeviceIdType.MESH
F32 = jnp.float32
BF16 = jnp.bfloat16

negative_fill = -1e30


class Place:
    def __init__(self):
        self.head = lax.axis_index("head")
        self.blk = lax.axis_index("blk")
        self.x = lax.rem(self.head, 4)
        self.zl = self.head // 4
        self.zh = self.blk // 8
        self.yc = lax.rem(self.blk, 8)
        self.z = self.zh * 2 + self.zl
        self.xs = [lax.rem(self.x + k, 4) for k in range(4)]
        self.right = self.at_x(self.xs[1])
        self.left = self.at_x(self.xs[3])
        self.above = self.at_z(1)
        self.below = self.at_z(3)

        self.y = self.yc // 2
        self.core = lax.rem(self.blk, 2)
        self.chip = self.blk // 2
        self.up = self.at_y(1)
        self.down = self.at_y(3)
        self.partner = (self.head, self.blk + 1 - 2 * self.core)
        self.across = (self.head, (1 - self.zh) * 8 + self.yc)

    def at_y(self, step):
        return (self.head, self.zh * 8 + lax.rem(self.y + step, 4) * 2 + self.core)

    def plane(self, step, k):
        z = lax.rem(self.z + step, 4)
        return (lax.rem(z, 2) * 4 + self.xs[k], (z // 2) * 8 + self.yc)

    def chip_at(self, dz, k):
        return lax.rem(self.zh + dz, 2) * 4 + lax.rem(self.y + k, 4)

    def at_x(self, x):
        return (self.zl * 4 + x, self.blk)

    def at_z(self, step):
        z = lax.rem(self.z + step, 4)
        return (lax.rem(z, 2) * 4 + self.x, (z // 2) * 8 + self.yc)

    def here(self, k):
        return self.zl * 4 + self.xs[k]

    def other(self, k):
        return (1 - self.zl) * 4 + self.xs[k]


def remote(src, dst, send_sem, recv_sem, device):
    return pltpu.make_async_remote_copy(
        src_ref=src, dst_ref=dst, send_sem=send_sem, recv_sem=recv_sem,
        device_id=device, device_id_type=MESH,
    )


def gather_rows(p, buf, batch, send_sem, recv, steps, compute, across_first=()):
    def send(h, s, half, to_half, kind, device):
        src, dst = buf.at[h, s, batch, half], buf.at[h, s, batch, to_half]
        remote(src, dst, send_sem, recv.at[kind, s, batch], device).start()

    def wait(h, s, half, kind):
        ref = buf.at[h, s, batch, half]
        remote(ref, ref, send_sem, recv.at[kind, s, batch], p.right).wait_recv()

    me, left, right, far = p.here(0), p.here(3), p.here(1), p.here(2)
    twin, twin_left, twin_right, twin_far = p.other(0), p.other(3), p.other(1), p.other(2)
    along_first = [s for s in range(steps) if s not in across_first]
    for s in range(steps):
        send(me, s, 0, 0, 0, p.right)
        send(me, s, 1, 1, 4, p.left)
        send(me, s, 0, 1, 6, p.above)
        send(me, s, 1, 0, 10, p.below)
    yield
    compute(me, True)
    yield
    for s in range(steps):
        wait(left, s, 0, 0)
        send(left, s, 0, 0, 2, p.right)
        wait(right, s, 1, 4)
        send(right, s, 1, 1, 5, p.left)
        if s in along_first:
            send(left, s, 0, 1, 7, p.above)
            send(right, s, 1, 0, 12, p.below)
    yield
    for s in range(steps):
        send(me, s, 1, 1, 1, p.right)
        send(me, s, 0, 0, 3, p.left)
    yield
    for s in range(steps):
        wait(twin, s, 1, 6)
        wait(twin, s, 0, 10)
        if s in across_first:
            send(twin, s, 0, 0, 11, p.right)
            send(twin, s, 1, 1, 8, p.left)
            send(twin, s, 1, 1, 7, p.right)
            send(twin, s, 0, 0, 12, p.left)
    compute(twin, False)
    yield
    for s in range(steps):
        wait(far, s, 0, 2)
        wait(far, s, 1, 5)
        if s in along_first:
            send(far, s, 0, 1, 9, p.above)
            send(far, s, 1, 0, 13, p.below)
    yield
    for s in range(steps):
        wait(left, s, 1, 1)
        wait(right, s, 0, 3)
        if s in along_first:
            send(left, s, 1, 0, 11, p.below)
            send(right, s, 0, 1, 8, p.above)
    yield
    for s in across_first:
        wait(twin_left, s, 0, 11)
        send(twin_left, s, 0, 0, 13, p.right)
        wait(twin_right, s, 1, 8)
        send(twin_right, s, 1, 1, 9, p.left)
    yield
    compute(left, False)
    compute(right, False)
    compute(far, False)
    yield
    for s in range(steps):
        wait(twin_left, s, 1, 7)
        if s in along_first:
            wait(twin_left, s, 0, 11)
    compute(twin_left, False)
    yield
    for s in range(steps):
        wait(twin_right, s, 0, 12)
        if s in along_first:
            wait(twin_right, s, 1, 8)
    compute(twin_right, False)
    yield
    for s in range(steps):
        wait(twin_far, s, 1, 9)
        wait(twin_far, s, 0, 13)
    compute(twin_far, False)


def advance(stages, count):
    for _ in range(count):
        next(stages, None)


def columns(h, width):
    return pl.ds(pl.multiple_of(h * width, width), width)


SCALE = HEAD_DIM ** (-0.5) * 1.4426950408889634


def batch_rows(group, b):
    return jnp.concatenate([group[at + b * 16 : at + b * 16 + 16] for at in range(0, 128, 32)], axis=0)


def attend_blocks(
    p, q, k, v, hid_in, wo_hbm, kv, qbuf, hid, wo, qs, oa, peak, abuf,
    sk, kv1, q1, h1, w1, w2, ysem, zrecv, csem, wown,
):
    own = p.blk
    mine = pl.ds(pl.multiple_of(p.x * 32, 32), 32)

    def rows_of(g):
        return pl.ds(pl.multiple_of(g * 128 + p.x * 32, 32), 32)

    kv_rows = pl.ds(pl.multiple_of(p.head * 64, 64), 64)

    def send_kv(device, sem):
        h = device[0]
        remote(k.at[:, columns(h, 128)], kv.at[own, kv_rows, 0:128], sk, sem, device).start()
        remote(v.at[:, columns(h, 128)], kv.at[own, kv_rows, 128:256], sk, sem, device).start()

    def send_rows(src, dst, sem, width, part, g, device):
        at = columns(device[0], width)
        remote(src.at[part * 32 : (part + 1) * 32, at], dst.at[rows_of(g), :], sk, sem, device).start()

    near = 1 - 2 * p.zl + 4
    for kx in range(4):
        send_kv(p.plane(near, kx), kv1.at[1])
        if kx:
            send_kv(p.plane(0, kx), kv1.at[0])
    for kx in range(4):
        send_rows(q, qbuf, q1, 256, 0, 2, p.plane(1, kx))
        send_rows(q, qbuf, q1, 256, 1, 1, p.plane(3, kx))
        if kx:
            send_rows(q, qbuf, q1, 256, 0, 0, p.plane(0, kx))
            send_rows(q, qbuf, q1, 256, 1, 3, p.plane(0, kx))

    def block(dz, kk, other=False):
        core = 1 - p.core if other else p.core
        return p.chip_at(dz, kk) * 2 + core

    def piece(dz, kk, part):
        return kv.at[block(dz, kk), part * 256 : (part + 1) * 256, 0:256]

    def send_piece(dz, kk, part, sem, device):
        remote(piece(dz, kk, part), piece(dz, kk, part), sk, sem, device).start()

    def wait_piece(dz, kk, part, sem):
        remote(piece(dz, kk, part), piece(dz, kk, part), sk, sem, p.up).wait_recv()

    def share(dz, kk, sem):
        ref = kv.at[block(dz, kk), :, 0:256]
        remote(ref, ref, sk, sem, p.partner).start()

    def wait_shared(dz, kk, sem):
        ref = kv.at[block(dz, kk, True), :, 0:256]
        remote(ref, ref, sk, sem, p.partner).wait_recv()

    def forward(dz):
        i = 3 * dz
        wait_piece(dz, 3, 0, ysem.at[0, i])
        send_piece(dz, 3, 0, ysem.at[0, i + 2], p.up)
        wait_piece(dz, 1, 1, ysem.at[1, i + 1])
        send_piece(dz, 1, 1, ysem.at[1, i + 2], p.down)

    def near_done(dz):
        i = 3 * dz
        wait_piece(dz, 3, 1, ysem.at[0, i + 1])
        share(dz, 3, csem.at[4 * dz + 3])
        wait_piece(dz, 1, 0, ysem.at[1, i])
        share(dz, 1, csem.at[4 * dz + 1])

    def far_done(dz):
        i = 3 * dz
        wait_piece(dz, 2, 0, ysem.at[0, i + 2])
        wait_piece(dz, 2, 1, ysem.at[1, i + 2])
        share(dz, 2, csem.at[4 * dz + 2])

    def own_rows(part):
        return kv.at[own, pl.ds(pl.multiple_of(part * 256, 256), 256), 0:256]

    for order, (part, count) in enumerate(((p.zl, 192), (1 - p.zl, 256))):
        ref = kv.at[own, 0:count, 0:256]
        remote(ref, ref, sk, kv1.at[order], p.up).wait_recv()
        ref = own_rows(part)
        remote(ref, ref, sk, ysem.at[0, part], p.up).start()
        remote(ref, ref, sk, ysem.at[1, part], p.down).start()
        remote(ref, ref, sk, zrecv.at[part], p.across).start()
    share(0, 0, csem.at[0])
    for kx in range(4):
        send_rows(hid_in, hid, h1, 512, 0, 2, p.plane(1, kx))
        send_rows(hid_in, hid, h1, 512, 1, 1, p.plane(3, kx))
        if kx:
            send_rows(hid_in, hid, h1, 512, 0, 0, p.plane(0, kx))
            send_rows(hid_in, hid, h1, 512, 1, 3, p.plane(0, kx))

    ref = qbuf.at[0:448]
    remote(ref, ref, sk, q1, p.up).wait_recv()
    same = 1 + p.zl
    for r in range(2):
        cols = slice(r * 128, (r + 1) * 128)
        qs[r * 384 : r * 384 + 128] = qbuf[0:128, cols]
        qs[r * 384 + 128 : r * 384 + 256] = qbuf[pl.ds(pl.multiple_of(same * 128, 128), 128), cols]
        qs[r * 384 + 256 : r * 384 + 384] = qbuf[384:512, cols]
        qs[768 + r * 128 : 896 + r * 128] = qbuf[pl.ds(pl.multiple_of((3 - same) * 128, 128), 128), cols]
    oa[...] = jnp.zeros_like(oa)
    peak[...] = jnp.full_like(peak, negative_fill)

    def absorb(start, count, sub, chip, row_pos):
        keys = kv[pl.ds(chip * 2, 2), :, 0:128].reshape(1024, 128)
        values = kv[pl.ds(chip * 2, 2), :, 128:384].reshape(1024, 256)
        tiles = [slice(start + at, start + at + sub) for at in range(0, count, sub)]
        asked = [qs[rows] for rows in tiles]
        olds = [peak[rows] for rows in tiles]
        sums = [oa[rows] for rows in tiles]

        def score(t):
            s = lax.dot_general(asked[t], keys, (((1,), (1,)), ((), ())), preferred_element_type=F32)
            if row_pos is not None:
                i = t * sub + lax.broadcasted_iota(jnp.int32, (sub, 1), 0)
                key_pos = chip * 1024 + lax.broadcasted_iota(jnp.int32, (sub, 1024), 1)
                s = jnp.where(key_pos <= row_pos(i), s, negative_fill)
            return [s[:, at : at + 128] for at in range(0, 1024, 128)]

        news, ends = [], []
        coming = score(0)
        for t, old in enumerate(olds):
            s = coming
            top = s[0]
            for piece in s[1:]:
                top = jnp.maximum(top, piece)
            if t + 1 < len(tiles):
                coming = score(t + 1)
            new = jnp.maximum(old, jnp.max(top, axis=1, keepdims=True))
            w = jnp.concatenate([jnp.exp2((piece - new) * SCALE).astype(BF16) for piece in s], axis=1)
            shrink = jnp.exp2((old - new) * SCALE)
            part = jnp.dot(w, values, preferred_element_type=F32)
            news.append(new)
            ends.append(sums[t] * jnp.concatenate([shrink, shrink], axis=1) + part)
        for rows, new, end in zip(tiles, news, ends):
            peak[rows] = new
            oa[rows] = end

    def spread(i):
        return ((i & 96) << 1) + (i & 31)

    def pos_a(i):
        seg = lax.rem(i >> 7, 3)
        shift = jnp.where(seg == 1, (1 - p.zl) * 288, p.zl * 256 + (seg >> 1) * 32)
        return own * 512 + spread(i & 127) + shift

    chip_b = (1 - p.zh) * 4 + p.y

    def pos_b(i):
        return (chip_b * 2 + p.core) * 512 + spread(i & 127) + (1 - p.zl) * 256 + p.zl * 32

    def absorb_a(chip, masked):
        absorb(0, 768, 256, chip, pos_a if masked else None)

    def absorb_b(chip, masked):
        absorb(768, 256, 128, chip, pos_b if masked else None)

    def seen(chip):
        @pl.when(chip < p.chip)
        def _():
            absorb_a(chip, False)

        @pl.when(chip < chip_b)
        def _():
            absorb_b(chip, False)

    wait_shared(0, 0, csem.at[0])
    absorb_a(p.chip, True)

    @pl.when(p.chip < chip_b)
    def _():
        absorb_b(p.chip, False)

    forward(0)
    for part in (p.zl, 1 - p.zl):
        ref = kv.at[block(1, 0), pl.ds(pl.multiple_of(part * 256, 256), 256), 0:256]
        remote(ref, ref, sk, zrecv.at[part], p.up).wait_recv()
        remote(ref, ref, sk, ysem.at[0, 3 + part], p.up).start()
        remote(ref, ref, sk, ysem.at[1, 3 + part], p.down).start()
    near_done(0)
    share(1, 0, csem.at[4])
    half = pl.ds(pl.multiple_of(p.core * 128, 128), 128)
    for kx in range(4):
        if kx:
            device = p.plane(0, kx)
            remote(
                wo_hbm.at[half, columns(device[0], 512)], wo.at[p.head, p.core], sk, w1, device
            ).start()
        for part in range(2):
            device = p.plane(1 + 2 * part, kx)
            rows = pl.ds(pl.multiple_of(p.core * 128 + part * 64, 64), 64)
            remote(
                wo_hbm.at[rows, columns(device[0], 512)],
                wo.at[p.head, p.core, part * 64 : (part + 1) * 64], sk, w1, device,
            ).start()
    wait_shared(0, 3, csem.at[3])
    wait_shared(0, 1, csem.at[1])

    def near_step(t, _):
        @pl.when(t == 1)
        def _():
            forward(1)

        seen(p.chip_at(0, 3 - 2 * t))
        return 0

    lax.fori_loop(0, 2, near_step, 0)
    far_done(0)
    wait_shared(1, 0, csem.at[4])
    chip = p.chip_at(1, 0)

    @pl.when(chip < p.chip)
    def _():
        absorb_a(chip, False)

    absorb_b(chip, True)

    def late_step(t, _):
        @pl.when(t == 0)
        def _():
            wait_shared(0, 2, csem.at[2])

        @pl.when(t == 1)
        def _():
            near_done(1)
            wait_shared(1, 3, csem.at[7])

        @pl.when(t == 2)
        def _():
            far_done(1)
            wait_shared(1, 1, csem.at[5])

        @pl.when(t == 3)
        def _():
            wown.wait()
            ref = wo.at[0:7, 0]
            remote(ref, ref, sk, w1, p.up).wait_recv()
            ref = wo.at[:, p.core]
            remote(ref, ref, sk, w2, p.partner).start()
            wait_shared(1, 2, csem.at[6])

        seen(p.chip_at(jnp.minimum(t, 1), 2 + t - 3 * (t // 2)))
        return 0

    lax.fori_loop(0, 4, late_step, 0)

    for r in range(2):
        cols = slice(r * 128, (r + 1) * 128)
        a = (oa[r * 384 : (r + 1) * 384, 0:128] / oa[r * 384 : (r + 1) * 384, 128:256]).astype(BF16)
        o = (oa[768 + r * 128 : 896 + r * 128, 0:128] / oa[768 + r * 128 : 896 + r * 128, 128:256]).astype(BF16)
        for b in range(2):
            abuf[p.head, r, b, 0, 0:64, :] = batch_rows(a[0:128], b)
            abuf[p.head, r, b, p.zl, pl.ds(pl.multiple_of((1 - p.zl) * 64, 64), 64), :] = batch_rows(a[128:256], b)
            abuf[p.head, r, b, 1, 64:128, :] = batch_rows(a[256:384], b)
            abuf[p.head, r, b, 1 - p.zl, pl.ds(pl.multiple_of(p.zl * 64, 64), 64), :] = batch_rows(o, b)

    ref = hid.at[0:448]
    remote(ref, ref, sk, h1, p.up).wait_recv()
    ref = wo.at[:, 1 - p.core]
    remote(ref, ref, sk, w2, p.partner).wait_recv()

    for ref in (
        qbuf.at[0:448], hid.at[0:448], kv.at[own, 0:448, 0:256], kv.at[0:15, :, 0:256], wo.at[0:7, 0], wo.at[:, p.core],
    ):
        pltpu.make_async_copy(ref, ref, sk).wait()


NS1 = 2
NS2 = 2
NC = 8
LAG = 5
ACROSS_FIRST = ((), (1,))
CW = 512
FFL = 896


def block_kernel(
    q_hbm, k_hbm, v_hbm, hid_hbm, gain_hbm, wo_hbm, gate_hbm, up_hbm, down_hbm, out,
    q, k, v, hid_in, gain, kv, qbuf, qs, oa, peak,
    abuf, rbuf, hid, wo, wgu, wd, oacc, acc, xg, sq, inner,
    zs, zr, keep, m1s, m1r, m2s, m2r,
    insem, wsem, sk, kv1, q1, h1, w1, w2, ysem, zrecv, csem,
    s1, r1, s2, r2, s3, zsem, m1sem, m2sem,
):
    p = Place()
    barrier = pltpu.get_barrier_semaphore()
    peers = [p.plane(0, kx) for kx in (1, 2, 3)]
    peers += [p.plane(step, kx) for step in (1, 3) for kx in range(4)]
    peers += [p.up, p.down, p.across, p.partner]
    for device in peers:
        pl.semaphore_signal(barrier, inc=1, device_id=device, device_id_type=MESH)
    loads = [
        pltpu.make_async_copy(src, dst, insem.at[i])
        for i, (src, dst) in enumerate(((k_hbm, k), (v_hbm, v), (q_hbm, q), (hid_hbm, hid_in), (gain_hbm, gain)))
    ]
    for load in loads:
        load.start()

    order = [p.here(0), p.other(0), p.here(3), p.here(1), p.here(2), p.other(3), p.other(1), p.other(2)]
    half = pl.ds(pl.multiple_of(p.core * 128, 128), 128)
    wo_copy = pltpu.make_async_copy(
        wo_hbm.at[half, columns(p.head, 512)], wo.at[p.head, p.core], wsem.at[16]
    )
    wd_copy = pltpu.make_async_copy(down_hbm, wd, wsem.at[17])

    def gate_copy(h):
        rows = pl.ds(pl.multiple_of(h * 512, 512), 512)
        return pltpu.make_async_copy(gate_hbm.at[rows], wgu.at[rows, 0:FFL], wsem.at[h])

    def up_copy(h):
        rows = pl.ds(pl.multiple_of(h * 512, 512), 512)
        return pltpu.make_async_copy(up_hbm.at[rows], wgu.at[rows, FFL : 2 * FFL], wsem.at[8 + h])

    wo_copy.start()
    for h in order:
        gate_copy(h).start()
        up_copy(h).start()
    wd_copy.start()

    me = p.here(0)
    kv[:, :, 256:384] = jnp.ones((16, 512, 128), BF16)
    kv_rows = pl.ds(pl.multiple_of(p.head * 64, 64), 64)
    for load in loads:
        load.wait()
    kv[p.blk, kv_rows, 0:128] = k[:, columns(p.head, 128)]
    kv[p.blk, kv_rows, 128:256] = v[:, columns(p.head, 128)]
    for part in range(2):
        rows = pl.ds(pl.multiple_of(part * 384 + p.x * 32, 32), 32)
        qbuf[rows, :] = q[part * 32 : (part + 1) * 32, columns(p.head, 256)]
        hid[rows, :] = hid_in[part * 32 : (part + 1) * 32, columns(p.head, 512)]
    pl.semaphore_wait(barrier, len(peers))
    attend_blocks(
        p, q, k, v, hid_in, wo_hbm, kv, qbuf, hid, wo, qs, oa, peak, abuf,
        sk, kv1, q1, h1, w1, w2, ysem, zrecv, csem, wo_copy,
    )

    c2 = 512 // NS2

    def project(b):
        rows = slice(b * 256, (b + 1) * 256)

        def add(h, first):
            a = jnp.concatenate([abuf[h, s, b].reshape(256, 256 // NS1) for s in range(NS1)], axis=1)
            part = jnp.dot(a, wo[h].reshape(256, 512), preferred_element_type=F32)
            if first:
                held = jnp.concatenate([batch_rows(hid[g * 128 : (g + 1) * 128], b) for g in range(4)], axis=0)
                oacc[rows] = held.astype(F32) + part
            else:
                oacc[rows] += part

        return add

    def residual(b):
        for s in range(NS2):
            for half in range(2):
                at = b * 256 + half * 128
                rbuf[me, s, b, half] = oacc[at : at + 128, s * c2 : (s + 1) * c2].astype(BF16)

    def expand(b):
        out_rows = slice(b * 256, (b + 1) * 256)

        def add(h, first):
            if b == 0:
                gate_copy(h).wait()
                up_copy(h).wait()
            total = None
            for s in range(NS2):
                r = rbuf[h, s, b].reshape(256, c2).astype(F32)
                for j in range(c2 // 128):
                    piece = r[:, j * 128 : (j + 1) * 128]
                    g = gain[pl.ds(h * 4 + s * (c2 // 128) + j, 1), :]
                    at = s * c2 + j * 128
                    xg[b, :, at : at + 128] = (piece * g).astype(BF16)
                    total = piece * piece if total is None else total + piece * piece
            rows = pl.ds(pl.multiple_of(h * 512, 512), 512)
            part = jnp.dot(xg[b], wgu[rows, :], preferred_element_type=F32)
            if first:
                sq[out_rows] = total
                acc[out_rows] = part
            else:
                sq[out_rows] += total
                acc[out_rows] += part

        return add

    def activate(b):
        rows = slice(b * 256, (b + 1) * 256)
        scale = lax.rsqrt(jnp.sum(sq[rows], axis=1, keepdims=True) * (1.0 / 4096.0) + 1e-5)
        sq[rows] = jnp.broadcast_to(scale, (256, 128))

        def tile(j, _):
            at = pl.multiple_of(j * 128, 128)
            u = acc[rows, pl.ds(at, 128)] * sq[rows]
            v = acc[rows, pl.ds(pl.multiple_of(at + FFL, 128), 128)] * sq[rows]
            inner[rows, pl.ds(at, 128)] = (u / (1.0 + jnp.exp(-u)) * v).astype(BF16)
            return 0

        lax.fori_loop(0, 7, tile, 0)

    def reduce_down(b, start, stop):
        def one(c, _):
            cols = pl.ds(pl.multiple_of(c * CW, CW), CW)
            part = jnp.dot(inner[b * 256 : (b + 1) * 256], wd[:, cols], preferred_element_type=F32)
            n = b * NC + c
            keep[n, 0] = part[0:64]
            zs[n, 0] = part[64:128].astype(BF16)
            zs[n, 1] = part[128:192].astype(BF16)
            keep[n, 1] = part[192:256]
            remote(zs.at[n, 0], zr.at[n, 1], s3, zsem.at[1, n], p.above).start()
            remote(zs.at[n, 1], zr.at[n, 0], s3, zsem.at[0, n], p.below).start()
            return 0

        lax.fori_loop(start, stop, one, 0)

    def slot(k):
        return pl.ds(pl.multiple_of(p.xs[k] * 16, 16), 16)

    def m1_copy(n, side):
        device = p.right if side == 0 else p.left
        return remote(m1s.at[n, side], m1r.at[n, side], s3, m1sem.at[side, n], device)

    def m2_copy(n, side):
        device = p.right if side == 0 else p.left
        return remote(m2s.at[n, side], m2r.at[n, side], s3, m2sem.at[side, n], device)

    def finish():
        def one(t, _):
            @pl.when(t < 2 * NC)
            def _():
                n = t
                for side in range(2):
                    ref = zr.at[n, side]
                    remote(ref, ref, s3, zsem.at[side, n], p.right).wait_recv()
                    keep[n, side] += zr[n, side].astype(F32)
                    m1s[n, side] = keep[n, side, slot(2), :].astype(BF16)
                    m1_copy(n, side).start()

            @pl.when((t >= LAG) & (t < 2 * NC + LAG))
            def _():
                n = t - LAG
                for side in range(2):
                    m1_copy(n, side).wait_recv()
                    k = 1 if side == 0 else 3
                    for part in range(2):
                        q = keep[n, part, slot(k), :]
                        if part == side:
                            q = q + m1r[n, side].astype(F32)
                        m2s[n, side, part] = q.astype(BF16)
                    m2_copy(n, side).start()

            @pl.when(t >= 2 * LAG)
            def _():
                n = t - 2 * LAG
                b, c = n // NC, lax.rem(n, NC)
                for side in range(2):
                    m2_copy(n, side).wait_recv()
                for part in range(2):
                    q = keep[n, part, slot(0), :] + m2r[n, 0, part].astype(F32) + m2r[n, 1, part].astype(F32)
                    rows = pl.ds(pl.multiple_of(part * 64 + p.x * 16, 16), 16)
                    for s in range(NS2):
                        r = rbuf[c, s, b, part, rows, :].astype(F32)
                        cols = pl.ds(pl.multiple_of(c * CW + s * c2, c2), c2)
                        to = pl.ds(pl.multiple_of(part * 32 + b * 16, 16), 16)
                        out[to, cols] = (r + q[:, s * c2 : (s + 1) * c2]).astype(BF16)

            return 0

        lax.fori_loop(0, 2 * NC + 2 * LAG, one, 0)

    ga = [gather_rows(p, abuf, b, s1, r1, NS1, project(b)) for b in range(2)]
    gr = [gather_rows(p, rbuf, b, s2, r2, NS2, expand(b), ACROSS_FIRST[b]) for b in range(2)]
    advance(ga[0], 1)
    advance(ga[1], 1)
    advance(ga[0], 1)
    advance(ga[1], 1)
    advance(ga[0], 1)
    advance(ga[1], 1)
    advance(ga[0], 1)
    advance(ga[1], 1)
    advance(ga[0], 1)
    advance(ga[1], 1)
    advance(ga[0], 1)
    advance(ga[1], 1)
    advance(ga[0], 1)
    advance(ga[1], 1)
    advance(ga[0], 5)
    residual(0)
    advance(gr[0], 2)
    advance(ga[1], 5)
    residual(1)
    advance(gr[0], 5)
    advance(gr[1], 1)
    advance(gr[0], 2)
    advance(gr[1], 3)
    advance(gr[0], 3)
    activate(0)
    wd_copy.wait()
    advance(gr[1], 3)
    reduce_down(0, 0, 3)
    advance(gr[1], 1)
    reduce_down(0, 3, NC)
    advance(gr[1], 4)
    activate(1)
    reduce_down(1, 0, NC)
    finish()
    pltpu.make_async_copy(abuf.at[0:7], abuf.at[0:7], s1).wait()
    pltpu.make_async_copy(rbuf.at[0:7], rbuf.at[0:7], s2).wait()
    for ref in (zs, m1s, m2s):
        pltpu.make_async_copy(ref, ref, s3).wait()


def layer(q, k, v, hidden, gain, wo, gate, up, down):
    vmem = pl.BlockSpec(memory_space=pltpu.VMEM)
    hbm = pl.BlockSpec(memory_space=pl.ANY)
    dma = pltpu.SemaphoreType.DMA
    return pl.pallas_call(
        block_kernel,
        out_shape=pltpu.VMEM((64, 4096), BF16),
        in_specs=[hbm] * 9,
        out_specs=vmem,
        scratch_shapes=[
            pltpu.VMEM((64, 2048), BF16),
            pltpu.VMEM((64, 1024), BF16),
            pltpu.VMEM((64, 1024), BF16),
            pltpu.VMEM((64, 4096), BF16),
            pltpu.VMEM((32, 128), F32),
            pltpu.VMEM((16, 512, 384), BF16),
            pltpu.VMEM((512, 256), BF16),
            pltpu.VMEM((1024, 128), BF16),
            pltpu.VMEM((1024, 256), F32),
            pltpu.VMEM((1024, 128), F32),
            pltpu.VMEM((8, NS1, 2, 2, 128, 256 // NS1), BF16),
            pltpu.VMEM((8, NS2, 2, 2, 128, 512 // NS2), BF16),
            pltpu.VMEM((512, 512), BF16),
            pltpu.VMEM((8, 2, 128, 512), BF16),
            pltpu.VMEM((4096, 2 * FFL), BF16),
            pltpu.VMEM((FFL, 4096), BF16),
            pltpu.VMEM((512, 512), F32),
            pltpu.VMEM((512, 2 * FFL), F32),
            pltpu.VMEM((2, 256, 512), BF16),
            pltpu.VMEM((512, 128), F32),
            pltpu.VMEM((512, FFL), BF16),
            pltpu.VMEM((2 * NC, 2, 64, CW), BF16),
            pltpu.VMEM((2 * NC, 2, 64, CW), BF16),
            pltpu.VMEM((2 * NC, 2, 64, CW), F32),
            pltpu.VMEM((2 * NC, 2, 16, CW), BF16),
            pltpu.VMEM((2 * NC, 2, 16, CW), BF16),
            pltpu.VMEM((2 * NC, 2, 2, 16, CW), BF16),
            pltpu.VMEM((2 * NC, 2, 2, 16, CW), BF16),
            dma((5,)),
            dma((18,)),
            dma,
            dma((2,)),
            dma,
            dma,
            dma,
            dma,
            dma((2, 6)),
            dma((2,)),
            dma((8,)),
            dma,
            dma((14, NS1, 2)),
            dma,
            dma((14, NS2, 2)),
            dma,
            dma((2, 2 * NC)),
            dma((2, 2 * NC)),
            dma((2, 2 * NC)),
        ],
        compiler_params=pltpu.CompilerParams(
            collective_id=1, has_side_effects=True, vmem_limit_bytes=62 * 1024 * 1024
        ),
        cost_estimate=pl.CostEstimate(flops=16_500_000_000, bytes_accessed=24_000_000, transcendentals=0),
        name="layer",
    )(q, k, v, hidden, gain, wo, gate, up, down)


def local(
    hidden_in,
    queries,
    key_states,
    value_states,
    out_weight,
    norm_gain,
    gate_weight,
    up_weight,
    down_weight,
):
    return layer(
        queries, key_states, value_states, hidden_in, norm_gain.reshape(32, 128),
        out_weight, gate_weight, up_weight, down_weight,
    )


def solution(mesh):
    return jax.shard_map(
        local,
        mesh=mesh,
        in_specs=(
            P(("blk", "head"), None),
            P(("blk", "head"), None),
            P(("blk", "head"), None),
            P(("blk", "head"), None),
            P("head", None),
            P(),
            P(None, "head"),
            P(None, "head"),
            P("head", None),
        ),
        out_specs=P(("blk", "head"), None),
        check_vma=False,
    )
```
